32 devices in a mesh: dp: 8 (over z, x), tensor: 4 (over y, core).
Axes of the slice: x: 2, y: 2, z: 4, core: 2. Of those that a mesh axis runs over, the one named last changes fastest.
Arguments:
- tubes: bfloat16 [16, 1568, 1536], P('dp'), may hold values from -6 to 6
- tube_order: int32 [16, 1568], P('dp'), may hold values from 0 to 1567, each once within a row
- common_master: float32 [2666880], P('dp'), as said below
- common_first: float32 [2666880], P('dp'), may hold values from -4.7683716e-06 to 4.7683716e-06
- common_second: float32 [2666880], P('dp'), may hold values from 2.3706446e-13 to 7.2031123e-13
- split_master: float32 [4, 2065920], P('tensor', 'dp'), as said below
- split_first: float32 [4, 2065920], P('tensor', 'dp'), may hold values from -4.7683716e-06 to 4.7683716e-06
- split_second: float32 [4, 2065920], P('tensor', 'dp'), may hold values from 2.3706446e-13 to 7.2031123e-13
Outputs:
- loss_mean: float32 [1], replicated
- grad_norm: float32 [1], replicated
- common_new: float32 [2666880], P('dp')
- common_first_new: float32 [2666880], P('dp')
- common_second_new: float32 [2666880], P('dp')
- common_copy: bfloat16 [2666880], P('dp')
- split_new: float32 [4, 2065920], P('tensor', 'dp')
- split_first_new: float32 [4, 2065920], P('tensor', 'dp')
- split_second_new: float32 [4, 2065920], P('tensor', 'dp')
- split_copy: bfloat16 [4, 2065920], P('tensor', 'dp')
The draws below stay inside these ranges and needn't reach their ends.
Inputs may be any that keep to these rules, and one draw needn't show every extreme that they name: `tube_order`: each row is a permutation of the 1568 tubes; its first 157 entries are the visible tubes, the rest the masked ones. `common_master`: laid out as the first step states; padding entries are drawn as well. `split_master`: laid out as the first step states; padding entries are drawn as well.
All inputs are finite; a program needn't handle non-finite values.
Results may differ from the reference program's by a relative error of at most 0.011.
The reference program's roundings to bfloat16 on the way count: a program that leaves them out, or rounds other values in their place, can miss the bound.
Values may be sent and summed in bfloat16 or wider, within the bound.
A program may use at most 320 MiB of HBM per device.

```python
import math
import jax
import jax.numpy as jnp
from jax import lax

D = 768
HEAD = 64
FF = 3072
DD = 384
DEC_HEADS = 6
DFF = 1536
PATCH = 1536
TUBES = 1568
VIS = 157
QBLOCK = 784
STEP = 10
MASKED = 1411
CLIPS = 16
PC = 2666880
PT = 2065920
N_TENSOR = 4


def segment_values(key, segment_plan, total_size):
    pieces = []
    for segment_index in range(len(segment_plan)):
        amount, center, spread = segment_plan[segment_index]
        normal_draw = jax.random.truncated_normal(jax.random.fold_in(key, segment_index), -3.0, 3.0, (amount,), jnp.float32)
        pieces.append(center + spread * normal_draw)
    joined = jnp.concatenate(pieces)
    tail_draw = 0.02 * jax.random.normal(jax.random.fold_in(key, 999), (total_size - joined.shape[0],), jnp.float32)
    return jnp.concatenate([joined, tail_draw])


def draw_common_master(key, part):
    segment_plan = [(PATCH * D, 0.0, PATCH ** (-0.5)), (D, 0.0, 0.3)]
    for norm_index in range(3):
        segment_plan.append((D, 1.0, 0.15))
        segment_plan.append((D, 0.0, 0.2))
    segment_plan.append((2 * D, 0.0, 0.3))
    segment_plan.append((D * DD, 0.0, D ** (-0.5)))
    segment_plan.append((DD, 0.0, 1.0))
    for norm_index in range(3):
        segment_plan.append((DD, 1.0, 0.15))
        segment_plan.append((DD, 0.0, 0.2))
    segment_plan.append((2 * DD, 0.0, 0.3))
    segment_plan.append((DD * 3 * DD, 0.0, DD ** (-0.5)))
    segment_plan.append((2 * DD, 0.0, 0.05))
    segment_plan.append((DD * DD, 0.0, (TUBES / 3.0) ** 0.5 * DD ** (-0.5)))
    segment_plan.append((DD * PATCH, 0.0, DD ** (-0.5)))
    segment_plan.append((PATCH, 0.0, 0.3))
    return segment_values(jax.random.fold_in(key, 1), segment_plan, PC)


def draw_split_master(key, part):
    local_width = D // N_TENSOR
    hidden = FF // N_TENSOR
    dec_hidden = DFF // N_TENSOR
    segment_plan = [(D * 3 * local_width, 0.0, D ** (-0.5)), (2 * local_width, 0.0, 0.1), (local_width * D, 0.0, (VIS / 3.0) ** 0.5 * D ** (-0.5)), (D * hidden, 0.0, D ** (-0.5)), (hidden, 0.0, 0.3), (hidden * D, 0.0, FF ** (-0.5)), (DD * dec_hidden, 0.0, DD ** (-0.5)), (dec_hidden, 0.0, 0.3), (dec_hidden * DD, 0.0, DFF ** (-0.5))]
    rows_drawn = [segment_values(jax.random.fold_in(key, 100 + row_index), segment_plan, PT) for row_index in range(N_TENSOR)]
    return jnp.stack(rows_drawn)


def shard_levels(stream_key, shape, split, smallest, high):
    gain, own = 1.0, jax.random.fold_in(stream_key, 6)
    for dim, parts in split:
        steps = jnp.exp(jax.random.uniform(jax.random.fold_in(own, dim), (parts,), jnp.float32, smallest / len(split), high / len(split)))
        gain = gain * jnp.repeat(steps, shape[dim] // parts).reshape([-1 if axis == dim else 1 for axis in range(len(shape))])
    return gain


def gaussian(key, shape, scale, most, cuts=(), kind=jnp.bfloat16):
    gain = shard_levels(key, shape, cuts, -0.22, 0.18) if cuts else 1.0
    entries = jax.random.normal(key, shape, jnp.float32) * scale * gain
    return jnp.minimum(jnp.maximum(entries, -most), most).astype(kind)


def setup_inputs(seed: int = 0) -> dict:
    arg_keys = jax.random.split(jax.random.key(seed), 9)
    return {
        "tubes": gaussian(arg_keys[0], (CLIPS, TUBES, PATCH), 1.0, 6.0, ((0, 8),)),
        "tube_order": jax.vmap(lambda own: jax.random.permutation(own, TUBES))(jax.random.split(arg_keys[1], CLIPS)).reshape((CLIPS, TUBES)).astype(jnp.int32),
        "common_master": draw_common_master(jax.random.fold_in(arg_keys[8], 71), 0),
        "common_first": gaussian(arg_keys[3], (PC,), (0.111 * 1.5 / ((CLIPS * MASKED) * (PC + N_TENSOR * PT)) ** 0.5), 4.76837158203125e-06, ((0, 8),), jnp.float32),
        "common_second": jnp.clip(2.370644641962877e-13 + 4.83246770507581e-13 * jax.random.uniform(arg_keys[4], (PC,), jnp.float32) ** shard_levels(arg_keys[4], (PC,), ((0, 8),), -0.2, 0.2), 2.370644641962877e-13, 7.203112347038687e-13),
        "split_master": draw_split_master(jax.random.fold_in(arg_keys[8], 71), 0),
        "split_first": gaussian(arg_keys[6], (N_TENSOR, PT), (0.111 * 1.5 / ((CLIPS * MASKED) * (PC + N_TENSOR * PT)) ** 0.5), 4.76837158203125e-06, ((0, 4), (1, 8)), jnp.float32),
        "split_second": jnp.clip(2.370644641962877e-13 + 4.83246770507581e-13 * jax.random.uniform(arg_keys[7], (N_TENSOR, PT), jnp.float32) ** shard_levels(arg_keys[7], (N_TENSOR, PT), ((0, 4), (1, 8)), -0.2, 0.2), 2.370644641962877e-13, 7.203112347038687e-13),
    }


PRECISE = lax.Precision.HIGHEST
NORM_EPS = 1e-06
PIXEL_EPS = 1e-06
CLIP_RATIO = 1.5
BETA_FIRST = 0.9
BETA_SECOND = 0.95
LEARN_RATE = 0.05
DECAY_RATE = 0.05
ADAM_EPS = 1e-08

@jax.custom_vjp
def low(v):
    return lax.optimization_barrier(v.astype(jnp.bfloat16)).astype(jnp.float32)

@jax.custom_vjp
def low_back(v):
    return v

def low_keep(v):
    return (low(v), None)

def low_pass(kept, grad):
    return (grad,)

def back_keep(v):
    return (v, None)

def back_low(kept, grad):
    return (low(grad),)
low.defvjp(low_keep, low_pass)
low_back.defvjp(back_keep, back_low)

def common_layout():
    return [('embedding', (PATCH, D)), ('embedding_bias', (D,)), ('enc_norms', (6, D)), ('enc_biases', (2, D)), ('to_decoder', (D, DD)), ('mask_token', (DD,)), ('dec_norms', (6, DD)), ('dec_biases', (2, DD)), ('dec_qkv', (DD, 3 * DD)), ('dec_qkv_bias', (2, DD)), ('dec_proj', (DD, DD)), ('pixel_head', (DD, PATCH)), ('head_bias', (PATCH,))]

def split_layout(tensor_parts):
    local_width = D // tensor_parts
    hidden = FF // tensor_parts
    dec_hidden = DFF // tensor_parts
    return [('enc_qkv', (D, 3 * local_width)), ('enc_qkv_bias', (2, local_width)), ('enc_proj', (local_width, D)), ('enc_up', (D, hidden)), ('enc_up_bias', (hidden,)), ('enc_down', (hidden, D)), ('dec_up', (DD, dec_hidden)), ('dec_up_bias', (dec_hidden,)), ('dec_down', (dec_hidden, DD))]

def unpack(flat, layout):
    pieces = {}
    offset = 0
    for layout_entry in layout:
        amount = math.prod(layout_entry[1])
        pieces[layout_entry[0]] = flat[offset:offset + amount].reshape(layout_entry[1])
        offset += amount
    return pieces

def sine_table(length, table_width):
    position = jnp.arange(length, dtype=jnp.float32)[:, None]
    column = jnp.arange(table_width)
    exponent = (2 * (column // 2)).astype(jnp.float32) / table_width
    angles = position / jnp.power(10000.0, exponent)[None, :]
    return jnp.where((column % 2 == 0)[None, :], jnp.sin(angles), jnp.cos(angles))

def layer_norm(inputs, gain_row, shift_row):
    centered = inputs - lax.optimization_barrier(jnp.mean(inputs, axis=-1, keepdims=True))
    spread = lax.optimization_barrier(jnp.mean(centered * centered, axis=-1, keepdims=True))
    return centered * lax.rsqrt(spread + NORM_EPS) * gain_row + shift_row

def pixel_targets(pixels):
    centered = pixels - lax.optimization_barrier(jnp.mean(pixels, axis=-1, keepdims=True))
    spread = lax.optimization_barrier(jnp.mean(centered * centered, axis=-1, keepdims=True))
    return centered * lax.rsqrt(spread + PIXEL_EPS)

def attention(query_heads, key_heads, value_heads, blocks):
    batch_size, head_count, length, head_size = query_heads.shape
    row_count = length // blocks
    query_blocks = query_heads.reshape(batch_size, head_count, blocks, row_count, head_size).transpose(2, 0, 1, 3, 4)

    def one_block(query_block):
        scores = low_back(jnp.einsum('bhqe,bhke->bhqk', query_block, key_heads, precision=PRECISE) * head_size ** (-0.5))
        probs = low(jax.nn.softmax(scores, axis=-1))
        return jnp.einsum('bhqk,bhke->bhqe', probs, value_heads, precision=PRECISE)
    outputs = lax.map(jax.checkpoint(one_block), query_blocks)
    return outputs.transpose(1, 2, 0, 3, 4).reshape(batch_size, head_count, length, head_size)

def both_low(inputs):
    return low(low_back(inputs))

def stacked_heads(source):
    batch_size, tensor_parts, length, local_width = source.shape
    local_heads = local_width // HEAD
    grouped = source.reshape(batch_size, tensor_parts, length, local_heads, HEAD).transpose(0, 1, 3, 2, 4)
    return grouped.reshape(batch_size, tensor_parts * local_heads, length, HEAD)

def stacked_merge(source, tensor_parts):
    batch_size, head_count, length, head_size = source.shape
    grouped = source.reshape(batch_size, tensor_parts, head_count // tensor_parts, length, head_size).transpose(0, 1, 3, 2, 4)
    return grouped.reshape(batch_size, tensor_parts, length, head_count // tensor_parts * head_size)

def split_mlp(residual, gain_row, shift_row, up_weight, up_bias, down_weight, down_bias):
    normed = low(layer_norm(residual, gain_row, shift_row))
    raised = low_back(jnp.einsum('bsd,kdf->bksf', normed, up_weight, precision=PRECISE) + up_bias[None, :, None, :])
    active = low(jax.nn.gelu(raised, approximate=False))
    branch = low_back(jnp.einsum('bksf,kfd->bsd', active, down_weight, precision=PRECISE) + down_bias)
    return residual + branch

def encoder_layer(residual, common_w, split_w):
    norms = common_w['enc_norms']
    biases = common_w['enc_biases']
    normed = low(layer_norm(residual, norms[0], norms[1]))
    mixed_all = jnp.einsum('bsd,kdc->bksc', normed, split_w['enc_qkv'], precision=PRECISE)
    local_width = D // N_TENSOR
    qkv_bias = split_w['enc_qkv_bias']
    query_heads = both_low(stacked_heads(mixed_all[..., :local_width] + qkv_bias[:, 0][None, :, None, :]))
    key_heads = both_low(stacked_heads(mixed_all[..., local_width:2 * local_width]))
    value_heads = both_low(stacked_heads(mixed_all[..., 2 * local_width:] + qkv_bias[:, 1][None, :, None, :]))
    attended = both_low(attention(query_heads, key_heads, value_heads, 1))
    merged = stacked_merge(attended, N_TENSOR)
    branch = low_back(jnp.einsum('bksc,kcd->bsd', merged, split_w['enc_proj'], precision=PRECISE) + biases[0])
    residual = residual + branch
    return split_mlp(residual, norms[2], norms[3], split_w['enc_up'], split_w['enc_up_bias'], split_w['enc_down'], biases[1])

def decoder_layer(residual, common_w, split_w):
    norms = common_w['dec_norms']
    biases = common_w['dec_biases']
    batch_size, length, _ = residual.shape
    normed = low(layer_norm(residual, norms[0], norms[1]))
    mixed_all = jnp.einsum('bsd,dc->bsc', normed, common_w['dec_qkv'], precision=PRECISE)
    qkv_bias = common_w['dec_qkv_bias']

    def to_heads(source):
        return source.reshape(batch_size, length, DEC_HEADS, HEAD).transpose(0, 2, 1, 3)
    query_heads = both_low(to_heads(mixed_all[..., :DD] + qkv_bias[0]))
    key_heads = both_low(to_heads(mixed_all[..., DD:2 * DD]))
    value_heads = both_low(to_heads(mixed_all[..., 2 * DD:] + qkv_bias[1]))
    attended = both_low(attention(query_heads, key_heads, value_heads, TUBES // QBLOCK))
    merged = attended.transpose(0, 2, 1, 3).reshape(batch_size, length, DD)
    branch = low_back(jnp.einsum('bsc,cd->bsd', merged, common_w['dec_proj'], precision=PRECISE) + biases[0])
    residual = residual + branch
    return split_mlp(residual, norms[2], norms[3], split_w['dec_up'], split_w['dec_up_bias'], split_w['dec_down'], biases[1])

def clip_loss(common_w, split_w, pixels, order_row):
    seen_index = order_row[:VIS]
    hidden_index = order_row[VIS:]
    seen_pixels = pixels[seen_index][None]
    embedded = jnp.einsum('bsp,pd->bsd', seen_pixels, common_w['embedding'], precision=PRECISE) + common_w['embedding_bias'] + sine_table(TUBES, D)[seen_index][None]
    embedded = low_back(embedded)
    encoded = encoder_layer(embedded, common_w, split_w)
    norms = common_w['enc_norms']
    final_low = low(layer_norm(encoded, norms[4], norms[5]))
    lowered = low_back(jnp.einsum('bsd,de->bse', final_low, common_w['to_decoder'], precision=PRECISE))
    dec_pos = sine_table(TUBES, DD)
    visible_rows = lowered + dec_pos[seen_index][None]
    masked_rows = common_w['mask_token'][None, None, :] + dec_pos[hidden_index][None]
    decoder_in = jnp.concatenate([visible_rows, masked_rows], axis=1)
    decoded = decoder_layer(decoder_in, common_w, split_w)
    dec_norms = common_w['dec_norms']
    head_low = low(layer_norm(decoded[:, VIS:], dec_norms[4], dec_norms[5]))
    predicted = low_back(jnp.einsum('bsd,dp->bsp', head_low, common_w['pixel_head'], precision=PRECISE) + common_w['head_bias'])
    target = pixel_targets(pixels[hidden_index])[None]
    missing = predicted - target
    return jnp.sum(missing * missing)

def adamw(master, first, second, gradient):
    first_new = BETA_FIRST * first + (1.0 - BETA_FIRST) * gradient
    second_new = BETA_SECOND * second + (1.0 - BETA_SECOND) * gradient * gradient
    first_hat = first_new / (1.0 - BETA_FIRST ** STEP)
    second_hat = second_new / (1.0 - BETA_SECOND ** STEP)
    master_new = master - LEARN_RATE * (first_hat / (jnp.sqrt(second_hat) + ADAM_EPS) + DECAY_RATE * master)
    return (master_new, first_new, second_new, master_new.astype(jnp.bfloat16))

def reference(tubes, tube_order, common_master, common_first, common_second, split_master, split_first, split_second):
    pixels_all = tubes.astype(jnp.float32)

    def total_loss(common_flat, split_flat):
        common_w = unpack(low(common_flat), common_layout())
        lowered_split = low(split_flat)
        pieces = [unpack(lowered_split[part_index], split_layout(N_TENSOR)) for part_index in range(N_TENSOR)]
        split_w = {}
        for layout_entry in split_layout(N_TENSOR):
            split_w[layout_entry[0]] = jnp.stack([piece[layout_entry[0]] for piece in pieces])

        def per_clip(running, inputs):
            return (running + jax.checkpoint(clip_loss)(common_w, split_w, inputs[0], inputs[1]), None)
        result, _ = lax.scan(per_clip, jnp.zeros((), jnp.float32), (pixels_all, tube_order))
        return result
    loss_total, pull_back = jax.vjp(total_loss, common_master, split_master)
    pixel_count = CLIPS * MASKED * PATCH
    common_grad, split_grad = pull_back(jnp.ones((), jnp.float32) / pixel_count)
    grad_norm = jnp.sqrt(jnp.sum(common_grad * common_grad) + jnp.sum(split_grad * split_grad))
    clip_limit = CLIP_RATIO / math.sqrt(CLIPS * MASKED)
    factor = jnp.minimum(1.0, clip_limit / (grad_norm + 1e-06))
    common_new, common_first_new, common_second_new, common_copy = adamw(common_master, common_first, common_second, common_grad * factor)
    split_new, split_first_new, split_second_new, split_copy = adamw(split_master, split_first, split_second, split_grad * factor)
    loss_mean = loss_total / pixel_count
    return (loss_mean.reshape(1), grad_norm.reshape(1), common_new, common_first_new, common_second_new, common_copy, split_new, split_first_new, split_second_new, split_copy)
```

```python
import functools
import math
from types import SimpleNamespace as Namespace

import jax
import jax.numpy as jnp
import numpy as np
from jax import lax
from jax.experimental import pallas as pl
from jax.experimental.pallas import tpu as pltpu
from jax.sharding import PartitionSpec as P

DP = "dp"
TENSOR = "tensor"
D = 768
HEAD = 64
FF = 3072
DD = 384
DFF = 1536
PATCH = 1536
TUBES = 1568
VIS = 157
STEP = 10
LANES = 128
TILE = 16
BLOCK = TILE * LANES
FRONT = 24
MESH = pl.DeviceIdType.MESH
F32 = jnp.float32
BF16 = jnp.bfloat16


def round_up(value, step):
    return -(-value // step) * step


COMMON = dict(
    embedding=(PATCH, D), embedding_bias=(D,), enc_norms=(6, D), enc_biases=(2, D), to_decoder=(D, DD), mask_token=(DD,),
    dec_norms=(6, DD), dec_biases=(2, DD), dec_qkv=(DD, 3 * DD), dec_qkv_bias=(2, DD), dec_proj=(DD, DD), pixel_head=(DD, PATCH),
    head_bias=(PATCH,))
SPLIT = dict(
    enc_qkv=(D, 576), enc_qkv_bias=(2, 192), enc_proj=(192, D), enc_up=(D, 768), enc_up_bias=(768,), enc_down=(768, D),
    dec_up=(DD, 384), dec_up_bias=(384,), dec_down=(384, DD))


def row_table(layout):
    table, at = {}, 0
    for name, shape in layout.items():
        count = math.prod(shape) // LANES
        table[name] = (at, count)
        at += count
    return Namespace(**table)


CROW = row_table(COMMON)
SROW = row_table(SPLIT)
DEC_ROW = SROW.dec_up[0]
SPLIT_ROWS = SROW.dec_down[0] + SROW.dec_down[1]
COMMON_ROWS = CROW.head_bias[0] + CROW.head_bias[1]


class Plan:
    def __init__(self, parts, share, rows_step):
        self.parts, self.share = parts, share
        self.base = [i * share // BLOCK * TILE for i in range(parts)]
        self.rows = round_up(-(-(share + BLOCK - 1) // LANES), rows_step)

    def pieces(self, first, last):
        out = []
        for i in range(self.parts):
            start = self.base[i] + (TILE if i else 0)
            stop = self.base[i + 1] if i + 1 < self.parts else self.base[i] + self.rows
            low, high = max(start, first), min(stop, last)
            if i and first <= self.base[i] < last:
                out.append(("edge", i, self.base[i] - self.base[i - 1], self.base[i], TILE))
            if low < high:
                out.append(("body", i, low - self.base[i], low, high - low))
        return out

    def owners(self, first, last):
        return sorted({i for kind, i, *_ in self.pieces(first, last)} | {i - 1 for kind, i, *_ in self.pieces(first, last) if kind == "edge"})


def align_kernel(scalars, split_in, common_in, split_out, common_out):
    def move(source, target, lanes, rows_down, skip, step):
        def part(row, step):
            lane = lax.broadcasted_iota(jnp.int32, (step, LANES), 1)
            here = source[pl.ds(FRONT - rows_down + skip + row, step), :]
            before = source[pl.ds(FRONT - 1 - rows_down + skip + row, step), :]
            value = jnp.where(lane >= lanes, pltpu.roll(here, lanes, 1), pltpu.roll(before, lanes, 1))
            target[pl.ds(pl.multiple_of(row, TILE), step), :] = value.astype(BF16)

        def body(index, _):
            part(index * step, step)
            return 0

        whole = target.shape[0] // step
        lax.fori_loop(0, whole, body, 0)
        if target.shape[0] % step:
            part(whole * step, target.shape[0] % step)

    move(split_in, split_out, scalars[0], scalars[1], 0, 256)
    move(common_in, common_out, scalars[2], scalars[3], scalars[4], 256)


def aligned(master, plan):
    tail = (plan.rows + 8) * LANES - master.shape[-1]
    return jnp.pad(master, ((0, 0),) * (master.ndim - 1) + ((FRONT * LANES, tail),)).reshape(-1, LANES)


def align(common_master, split_master, cplan, splan):
    me, t = lax.axis_index(DP), lax.axis_index(TENSOR)
    soff = me * splan.share % BLOCK
    coff = me * cplan.share % BLOCK
    quarter = cplan.rows // 4
    scalars = jnp.stack([soff % LANES, soff // LANES, coff % LANES, coff // LANES, t * quarter]).astype(jnp.int32)
    return pl.pallas_call(
        align_kernel,
        out_shape=(jax.ShapeDtypeStruct((splan.rows, LANES), BF16), jax.ShapeDtypeStruct((quarter, LANES), BF16)),
        in_specs=[pl.BlockSpec(memory_space=pltpu.SMEM), pl.BlockSpec(memory_space=pltpu.VMEM), pl.BlockSpec(memory_space=pltpu.VMEM)],
        out_specs=[pl.BlockSpec(memory_space=pltpu.VMEM)] * 2,
        name="align",
    )(scalars, aligned(split_master, splan), aligned(common_master, cplan))


OUTS = Namespace(
    embedding=(PATCH, D), to_decoder=(D, DD), dec_qkv=(DD, 3 * DD), dec_proj=(DD, DD), pixel_head=(DD, PATCH),
    enc_qkv=(2, D, 576), enc_proj=(384, D), enc_up=(D, 1536), enc_down=(1536, D), dec_up=(DD, 1536), dec_down=(1536, DD))
OUT_NAMES = tuple(vars(OUTS))
CMATS = OUT_NAMES[:5]
SMALLS = ((CROW.embedding_bias[0], 54), (CROW.mask_token[0], 27), (CROW.dec_qkv_bias[0], 6), (CROW.head_bias[0], 12))


def copy_rows(pieces, frame, wide, first, chunk=64):
    for kind, part, row, at, count in pieces:
        if kind == "edge":
            wide[pl.ds(at - first, TILE), :] = frame(part)[pl.ds(0, TILE), :].astype(F32) + frame(part - 1)[pl.ds(row, TILE), :].astype(F32)
            continue
        source, whole = frame(part), count // chunk

        def body(index, _, source=source, row=row, at=at):
            wide[pl.ds(pl.multiple_of(at - first + index * chunk, TILE), chunk), :] = source[
                pl.ds(pl.multiple_of(row + index * chunk, TILE), chunk), :
            ].astype(F32)
            return 0

        if whole:
            lax.fori_loop(0, whole, body, 0)
        for rest in range(whole * chunk, count, TILE):
            wide[pl.ds(at - first + rest, TILE), :] = source[pl.ds(row + rest, TILE), :].astype(F32)


def matrix_out(wide, start, rows, width, target, row0, col0, step=64):
    per_row = width // LANES

    def body(index, _):
        at = index * step
        for j in range(per_row):
            value = wide[pl.ds(start + j + at * per_row, step, stride=per_row), :]
            target[pl.ds(pl.multiple_of(row0 + at, TILE), step), col0 + j * LANES : col0 + (j + 1) * LANES] = value.astype(BF16)
        return 0

    lax.fori_loop(0, rows // step, body, 0)


def qkv_out(wide, start, pair_buf, target):
    step = 32
    lane = lax.broadcasted_iota(jnp.int32, (step, LANES), 1)

    def body(index, _):
        at = start + index * step * 9
        for j in range(5):
            even = wide[pl.ds(at + j, step, stride=9), :]
            low = pltpu.roll(wide[pl.ds(at + 4 + j, step, stride=9), :], 64, 1)
            if j < 4:
                high = pltpu.roll(wide[pl.ds(at + 5 + j, step, stride=9), :], 64, 1)
                odd = jnp.where(lane < 64, low, high)
            else:
                odd = low
            pair_buf[j, pl.ds(0, step, stride=2), :] = even
            pair_buf[j, pl.ds(1, step, stride=2), :] = odd
            both = pair_buf[j].astype(BF16)
            rows = pl.ds(pl.multiple_of(index * 64, 64), 64)
            if j < 4:
                target[rows, j * LANES : (j + 1) * LANES] = both
            else:
                target[rows, 512:576] = both[:, :64]
        return 0

    lax.fori_loop(0, 12, body, 0)


def floor16(value):
    return value // TILE * TILE


def unpack_into(cplan, splan, common_frame, split_frame, dec_frame, stage, small_ref, bias_ref, dbias_ref, wide, pair_buf, done):
    def load(plan, frame, start, count):
        first, last = floor16(start), round_up(start + count, TILE)
        copy_rows(plan.pieces(first, last), frame, wide, first)
        return start - first

    for c in range(2):
        frame = functools.partial(split_frame, c)
        start, count = SROW.enc_qkv
        qkv_out(wide, load(splan, frame, start, count), pair_buf, stage.enc_qkv.at[c])
        if c:
            done(stage.enc_qkv)
        at = load(splan, frame, *SROW.enc_qkv_bias)
        bias_ref[c, 0:8, :] = wide[pl.ds(at, 8), :]
        at = load(splan, frame, *SROW.enc_proj)
        matrix_out(wide, at, 192, D, stage.enc_proj, c * 192, 0)
        if c:
            done(stage.enc_proj)
        at = load(splan, frame, *SROW.enc_up)
        matrix_out(wide, at, D, 768, stage.enc_up, 0, c * 768)
        if c:
            done(stage.enc_up)
        at = load(splan, frame, *SROW.enc_up_bias)
        bias_ref[c, 8:16, :] = wide[pl.ds(at, 8), :]
        at = load(splan, frame, *SROW.enc_down)
        matrix_out(wide, at, 768, D, stage.enc_down, c * 768, 0)
        if c:
            done(stage.enc_down)
    at = load(cplan, common_frame, *CROW.embedding)
    matrix_out(wide, at, PATCH, D, stage.embedding, 0, 0)
    done(stage.embedding)
    for name in CMATS[1:]:
        at = load(cplan, common_frame, *vars(CROW)[name])
        rows, width = vars(OUTS)[name]
        matrix_out(wide, at, rows, width, vars(stage)[name], 0, 0)
        done(vars(stage)[name])
    small_at = 0
    for start, count in SMALLS:
        at = load(cplan, common_frame, start, count)
        small_ref[pl.ds(small_at, round_up(count, 8)), :] = wide[pl.ds(at, round_up(count, 8)), :]
        small_at += round_up(count, 8)
    for slot in range(4):
        frame = functools.partial(split_frame, slot) if slot < 2 else functools.partial(dec_frame, slot - 2)
        at = load(splan, frame, DEC_ROW, SPLIT_ROWS - DEC_ROW)
        matrix_out(wide, at, DD, 384, stage.dec_up, 0, slot * 384)
        bias = at + SROW.dec_up_bias[0] - DEC_ROW
        dbias_ref[slot, :, :] = wide[pl.ds(bias, 8), :]
        matrix_out(wide, bias + 3, 384, DD, stage.dec_down, slot * 384, 0)
    done(stage.dec_up)
    done(stage.dec_down)


SMALL_ROWS = sum(round_up(count, 8) for _, count in SMALLS)
GATHERED = tuple(jax.ShapeDtypeStruct(vars(OUTS)[name], BF16) for name in OUT_NAMES) + (
    jax.ShapeDtypeStruct((SMALL_ROWS, LANES), F32), jax.ShapeDtypeStruct((2, 16, LANES), F32), jax.ShapeDtypeStruct((4, 8, LANES), F32))


def first_dec(splan):
    return splan.owners(floor16(DEC_ROW), round_up(SPLIT_ROWS, TILE))[0]


def unpack_scratch(cplan, splan):
    fd = first_dec(splan)
    return [
        pltpu.VMEM((2, splan.parts, splan.rows, LANES), BF16),
        pltpu.VMEM((2, splan.parts - fd, splan.rows, LANES), BF16),
        pltpu.VMEM((cplan.parts, 4, cplan.rows // 4, LANES), BF16),
        pltpu.VMEM((CROW.embedding[1] + 32, LANES), F32),
        pltpu.VMEM((5, 64, LANES), F32),
    ] + [pltpu.VMEM(vars(OUTS)[name], BF16) for name in OUT_NAMES] + [pltpu.SemaphoreType.DMA((len(OUT_NAMES),))]


def finish_unpack(cplan, splan, outs, smalls, sbuf, dbuf, cbuf, wide, pair_buf, stages, out_sem):
    fd = first_dec(splan)
    stage = Namespace(**dict(zip(OUT_NAMES, stages)))
    copies = []

    def done(whole):
        index = [ref is whole for ref in stages].index(True)
        copy = pltpu.make_async_copy(whole, outs[index], out_sem.at[index])
        copy.start()
        copies.append(copy)

    unpack_into(
        cplan, splan, lambda i: cbuf.at[i], lambda c, i: sbuf.at[c, i], lambda c, i: dbuf.at[c, i - fd],
        stage, smalls[0], smalls[1], smalls[2], wide, pair_buf, done)
    for copy in copies:
        copy.wait()


def gather_kernel(cplan, splan, s_own, c_own, *refs):
    nout = len(OUT_NAMES)
    outs, smalls = refs[:nout], refs[nout : nout + 3]
    sbuf, dbuf, cbuf, wide, pair_buf = refs[nout + 3 : nout + 8]
    stages, out_sem = refs[nout + 8 : 2 * nout + 8], refs[2 * nout + 8]
    send, recv, local = refs[2 * nout + 9 :]
    me, t = lax.axis_index(DP), lax.axis_index(TENSOR)
    z, x, y, c = me // 2, me % 2, t // 2, t % 2
    ty = (1 - y) * 2 + c
    fd = first_dec(splan)
    quarter = cplan.rows // 4

    def cblock(i, tt):
        return cbuf.at[i, pl.ds(pl.multiple_of(tt * quarter, TILE), quarter)]

    def sblock(i):
        return sbuf.at[c, i]

    zdev = [{DP: (z + k) % 4 * 2 + x, TENSOR: t} for k in range(4)]
    xdev, ydev, kdev = {DP: z * 2 + (1 - x), TENSOR: t}, {DP: me, TENSOR: ty}, {DP: me, TENSOR: y * 2 + (1 - c)}
    barrier = pltpu.get_barrier_semaphore()
    for device in zdev[1:] + [xdev, ydev, kdev]:
        pl.semaphore_signal(barrier, inc=1, device_id=device, device_id_type=MESH)
    own = [pltpu.make_async_copy(s_own, sblock(me), local.at[0]), pltpu.make_async_copy(c_own, cblock(me, t), local.at[1])]
    for copy in own:
        copy.start()
    pl.semaphore_wait(barrier, 6)
    for copy in own:
        copy.wait()

    def remote(source, target, slot, device):
        return pltpu.make_async_remote_copy(
            src_ref=source, dst_ref=target, send_sem=send.at[slot], recv_sem=recv.at[slot], device_id=device, device_id_type=MESH)

    def z_copy(common, down, hop, i):
        block = cblock(i, t) if common else sblock(i)
        return remote(block, block, common * 6 + down * 3 + hop - 1, zdev[3 if down else 1])

    def x_copy(common, i):
        block = cblock(i, t) if common else sblock(i)
        return remote(block, block, 12 + common * 4 + i // 2, xdev)

    def y_copy(i):
        return remote(cblock(i, t), cblock(i, t), 20 + i, ydev)

    def k_copy(i):
        return remote(sblock(i), sblock(i), 28 + i, kdev)

    def k_common(i):
        return remote(cblock(i, t), cblock(i, t), 36 + i, kdev)

    def k_far(i):
        return remote(cblock(i, ty), cblock(i, ty), 44 + i, kdev)

    def dec_rows(i):
        return pl.ds(max(0, DEC_FIRST - splan.base[i]), min(splan.rows, S_WIDE - splan.base[i]) - max(0, DEC_FIRST - splan.base[i]))

    def d_copy(i):
        return remote(sbuf.at[c, i, dec_rows(i)], dbuf.at[c, i - fd, dec_rows(i)], 52 + i - fd, ydev)

    def d_beside(i):
        return remote(dbuf.at[c, i - fd, dec_rows(i)], dbuf.at[c, i - fd, dec_rows(i)], 54 + i - fd, kdev)

    def send_z(common, down, hop):
        i = (z + (hop - 1 if down else 1 - hop)) * 2 + x
        able = jnp.logical_and(z > 0, z + hop - 1 <= 3) if down else jnp.logical_and(z < 3, z - hop + 1 >= 0)
        return i, able

    def pass_on(common, down, hop, action):
        i, able = send_z(common, down, hop)

        @pl.when(able)
        def _():
            action(z_copy(common, down, hop, i))

    def share_c(i):
        x_copy(1, i).start()
        y_copy(i).start()
        k_common(i).start()

    def share_s(i):
        x_copy(0, i).start()
        k_copy(i).start()
        dec_start(i)

    def dec_start(i):
        for known in range(fd, splan.parts):
            @pl.when(i == known)
            def _(known=known):
                d_copy(known).start()

    for common in (1, 0):
        for down in (0, 1):
            pass_on(common, down, 1, lambda copy: copy.start())
    share_c(me)
    share_s(me)
    for hop in (1, 2, 3):
        for common in (1, 0):
            for down in (0, 1):
                i = (z + (hop if down else -hop)) * 2 + x
                here = z + hop <= 3 if down else z >= hop

                @pl.when(here)
                def _(common=common, down=down, hop=hop, i=i):
                    z_copy(common, down, hop, i).wait_recv()
                    if hop < 3:
                        pass_on(common, down, hop + 1, lambda copy: copy.start())
                    if common:
                        share_c(i)
                    else:
                        share_s(i)

    for zz in range(4):
        i = zz * 2 + (1 - x)
        x_copy(1, i).wait_recv()
        y_copy(i).start()
        k_common(i).start()
    for i in range(8):
        y_copy(i).wait_recv()
        k_far(i).start()
    for zz in range(4):
        i = zz * 2 + (1 - x)
        x_copy(0, i).wait_recv()
        k_copy(i).start()
        dec_start(i)
    for i in range(fd, splan.parts):
        d_copy(i).wait_recv()
        d_beside(i).start()
    for i in range(8):
        k_common(i).wait_recv()
        k_far(i).wait_recv()
        k_copy(i).wait_recv()
    for i in range(fd, splan.parts):
        d_beside(i).wait_recv()
    for hop in (1, 2, 3):
        for common in (1, 0):
            for down in (0, 1):
                pass_on(common, down, hop, lambda copy: copy.wait_send())
    for zz in range(4):
        for common in (1, 0):
            x_copy(common, zz * 2 + x).wait_send()
    for i in range(8):
        for copy in (y_copy(i), k_copy(i), k_common(i), k_far(i)):
            copy.wait_send()
    for i in range(fd, splan.parts):
        d_copy(i).wait_send()
        d_beside(i).wait_send()
    finish_unpack(cplan, splan, outs, smalls, sbuf, dbuf, cbuf, wide, pair_buf, stages, out_sem)


def local_unpack_kernel(cplan, splan, s_all, d_all, c_all, *refs):
    nout = len(OUT_NAMES)
    outs, smalls = refs[:nout], refs[nout : nout + 3]
    sbuf, dbuf, cbuf, wide, pair_buf = refs[nout + 3 : nout + 8]
    stages, out_sem = refs[nout + 8 : 2 * nout + 8], refs[2 * nout + 8]
    local = refs[2 * nout + 9]
    copies = [pltpu.make_async_copy(source, target, local.at[k]) for k, (source, target) in enumerate(((s_all, sbuf), (d_all, dbuf), (c_all, cbuf)))]
    for copy in copies:
        copy.start()
    for copy in copies:
        copy.wait()
    finish_unpack(cplan, splan, outs, smalls, sbuf, dbuf, cbuf, wide, pair_buf, stages, out_sem)


def gather_weights(common_master, split_master, cplan, splan):
    s_own, c_own = align(common_master, split_master, cplan, splan)
    any_spec = pl.BlockSpec(memory_space=pl.ANY)
    vmem = pl.BlockSpec(memory_space=pltpu.VMEM)
    scratch = unpack_scratch(cplan, splan)
    scratch[2] = pltpu.VMEM((cplan.parts, cplan.rows, LANES), BF16)
    fd = first_dec(splan)
    out_specs = [any_spec] * len(OUT_NAMES) + [vmem] * 3
    limit = 64000 * 1024
    if cplan.parts == 8 and splan.parts == 8:
        copies = 60
        results = pl.pallas_call(
            functools.partial(gather_kernel, cplan, splan),
            out_shape=GATHERED, in_specs=[vmem, vmem], out_specs=out_specs,
            scratch_shapes=scratch + [pltpu.SemaphoreType.DMA((copies,)), pltpu.SemaphoreType.DMA((copies,)), pltpu.SemaphoreType.DMA((2,))],
            compiler_params=pltpu.CompilerParams(collective_id=0, has_side_effects=True, vmem_limit_bytes=limit),
            name="gather",
        )(s_own, c_own)
    else:
        y = lax.axis_index(TENSOR) // 2
        s_all = lax.all_gather(lax.all_gather(s_own, DP), TENSOR).reshape(2, 2, splan.parts, splan.rows, LANES)
        c_all = jnp.moveaxis(lax.all_gather(lax.all_gather(c_own, DP), TENSOR), 0, 1).reshape(cplan.parts, cplan.rows, LANES)
        s_mine = lax.dynamic_index_in_dim(s_all, y, 0, False)
        d_other = lax.dynamic_index_in_dim(s_all, 1 - y, 0, False)[:, fd:]
        results = pl.pallas_call(
            functools.partial(local_unpack_kernel, cplan, splan),
            out_shape=GATHERED, in_specs=[any_spec] * 3, out_specs=out_specs,
            scratch_shapes=scratch + [pltpu.SemaphoreType.DMA((3,))],
            compiler_params=pltpu.CompilerParams(vmem_limit_bytes=limit),
            name="unpack",
        )(s_mine, d_other, c_all)
    weights = Namespace(**dict(zip(OUT_NAMES, results)))
    small, bias, dbias = results[len(OUT_NAMES) :]
    at = 0
    rows = []
    for _, count in SMALLS:
        rows.append(small[at : at + count])
        at += round_up(count, 8)
    a, b, qkv_rows, head_rows = rows
    weights.embedding_bias = a[:6].reshape(1, D)
    weights.enc_norms = a[6:42].reshape(6, D)
    weights.enc_biases = a[42:54].reshape(2, D)
    weights.mask_token = b[:3].reshape(1, DD)
    weights.dec_norms = b[3:21].reshape(6, DD)
    weights.dec_biases = b[21:27].reshape(2, DD)
    weights.dec_qkv_bias = qkv_rows.reshape(2, DD)
    weights.head_bias = head_rows.reshape(1, PATCH)
    weights.enc_qkv_bias = bias[:, :3].reshape(2, 2, 192)
    weights.enc_up_bias = bias[:, 8:14].reshape(1, 1536)
    weights.dec_up_bias = dbias[:, :3].reshape(1, 1536)
    return weights


DEC_FIRST = floor16(DEC_ROW)
S_WIDE = round_up(SPLIT_ROWS, TILE)
C_WIDE = round_up(COMMON_ROWS, TILE)
D_WIDE = S_WIDE - DEC_FIRST
SLOTS = 3


def buffer_rows(plan, wide):
    return max(wide, plan.base[-1] + plan.rows)


def narrow(wide, target, count, chunk=128):
    def body(index, _):
        at = pl.ds(pl.multiple_of(index * chunk, TILE), chunk)
        target[at, :] = wide[at, :].astype(BF16)
        return 0

    whole = count // chunk
    lax.fori_loop(0, whole, body, 0)
    if count % chunk:
        target[whole * chunk : count, :] = wide[whole * chunk : count, :].astype(BF16)


def clear(wide, first, last, chunk=64):
    def body(index, _):
        wide[pl.ds(first + index * chunk, chunk), :] = jnp.zeros((chunk, LANES), F32)
        return 0

    whole = (last - first) // chunk
    lax.fori_loop(0, whole, body, 0)
    rest = (last - first) % chunk
    if rest:
        wide[pl.ds(first + whole * chunk, rest), :] = jnp.zeros((rest, LANES), F32)


def matrix_in(wide, start, per_row, stage, rows, width, j0, step=64):
    def body(index, _):
        at = index * step
        for j in range(width // LANES):
            wide[pl.ds(start + j0 + j + at * per_row, step, stride=per_row), :] = stage[
                pl.ds(pl.multiple_of(at, 8), step), j * LANES : (j + 1) * LANES
            ]
        return 0

    lax.fori_loop(0, rows // step, body, 0)


def qkv_in(wide, start, pair_buf, stage):
    step = 32
    lane = lax.broadcasted_iota(jnp.int32, (step, LANES), 1)

    def body(index, _):
        at = start + index * step * 9
        even, odd = [], []
        base = pl.multiple_of(index * 64, 8)
        for j in range(5):
            lanes = slice(j * LANES, (j + 1) * LANES) if j < 4 else slice(512, 640)
            pair_buf[j] = stage[pl.ds(base, 64), lanes]
            even.append(pair_buf[j, pl.ds(0, step, stride=2), :])
            odd.append(pltpu.roll(pair_buf[j, pl.ds(1, step, stride=2), :], 64, 1))
        for j in range(4):
            wide[pl.ds(at + j, step, stride=9), :] = even[j]
        wide[pl.ds(at + 4, step, stride=9), :] = jnp.where(lane < 64, even[4], odd[0])
        for j in range(4):
            wide[pl.ds(at + 5 + j, step, stride=9), :] = jnp.where(lane < 64, odd[j], odd[j + 1])
        return 0

    lax.fori_loop(0, 12, body, 0)


def pack_all(y, grads, small, bias, dbias, wide, pair_buf, stage, stage_sem, gs, gd, gc):
    grad = Namespace(**dict(zip(OUT_NAMES, grads)))
    jobs = []

    def matrix(source, rows, width, per_row, start, j0=0):
        jobs.append(("m", source, rows, width, per_row, start, j0))

    def call(action):
        jobs.append(("f", action))

    def small_rows(source_rows, start):
        def action():
            wide[pl.ds(start, source_rows.shape[0]), :] = source_rows[...]

        call(action)

    half = CROW.embedding[1] // 2

    def clear_other():
        def body(index, _):
            wide[pl.ds((1 - y) * half + index * 64, 64), :] = jnp.zeros((64, LANES), F32)
            return 0

        lax.fori_loop(0, half // 64, body, 0)
        clear(wide, COMMON_ROWS, C_WIDE)

    call(clear_other)
    matrix(grad.embedding, 768, D, 6, y * half)
    at = 0
    for start, count in SMALLS:
        small_rows(small.at[pl.ds(at, count)], start)
        at += round_up(count, 8)
    for name in CMATS[1:]:
        rows, total = vars(OUTS)[name]
        for col in range(0, total, 768):
            width = min(768, total - col)
            matrix(vars(grad)[name].at[:, pl.ds(col, width)], rows, width, total // LANES, vars(CROW)[name][0], col // LANES)
    call(lambda: narrow(wide, gc, C_WIDE))
    for slot in range(4):
        first = 0 if slot < 2 else DEC_FIRST
        if slot < 2:
            jobs.append(("q", grad.enc_qkv.at[:, pl.ds(slot * 640, 640)], SROW.enc_qkv[0]))
            small_rows(bias.at[slot, pl.ds(0, 3)], SROW.enc_qkv_bias[0])
            matrix(grad.enc_proj.at[pl.ds(slot * 192, 192)], 192, D, 6, SROW.enc_proj[0])
            matrix(grad.enc_up.at[:, pl.ds(slot * 768, 768)], D, 768, 6, SROW.enc_up[0])
            small_rows(bias.at[slot, pl.ds(8, 6)], SROW.enc_up_bias[0])
            matrix(grad.enc_down.at[pl.ds(slot * 768, 768)], 768, D, 6, SROW.enc_down[0])
        else:
            call(lambda: clear(wide, 0, DEC_ROW - DEC_FIRST))
        matrix(grad.dec_up.at[:, pl.ds(slot * 384, 384)], DD, 384, 3, SROW.dec_up[0] - first)
        small_rows(dbias.at[slot, pl.ds(0, 3)], SROW.dec_up_bias[0] - first)
        matrix(grad.dec_down.at[pl.ds(slot * 384, 384)], 384, DD, 3, SROW.dec_down[0] - first)
        call(functools.partial(clear, wide, SPLIT_ROWS - first, S_WIDE - first))
        if slot < 2:
            call(functools.partial(narrow, wide, gs.at[slot], S_WIDE))
        else:
            call(functools.partial(narrow, wide, gd.at[slot - 2], D_WIDE))

    loads = [job for job in jobs if job[0] in "mq"]
    copies = []
    for index, job in enumerate(loads):
        rows, width = (job[2], job[3]) if job[0] == "m" else (D, 640)
        target = stage.at[index % SLOTS, pl.ds(0, rows), pl.ds(0, width)]
        copies.append(pltpu.make_async_copy(job[1], target, stage_sem.at[index % SLOTS]))
    for copy in copies[: SLOTS - 1]:
        copy.start()
    index = 0
    for job in jobs:
        if job[0] == "f":
            job[1]()
            continue
        if index + SLOTS - 1 < len(copies):
            copies[index + SLOTS - 1].start()
        copies[index].wait()
        here = stage.at[index % SLOTS]
        if job[0] == "m":
            matrix_in(wide, job[5], job[4], here, job[2], job[3], job[6])
        else:
            qkv_in(wide, job[2], pair_buf, here)
        index += 1


def add_rows(target, parts, count, chunk=None):
    chunk = chunk or max(c for c in (128, 64, 48, 32, 16) if count % c == 0)

    def body(index, _):
        at = index * chunk
        total = None
        for ref, start in parts:
            value = ref[pl.ds(pl.multiple_of(start + at, TILE), chunk), :].astype(F32)
            total = value if total is None else total + value
        target[pl.ds(pl.multiple_of(at, TILE), chunk), :] = total.astype(target.dtype)
        return 0

    lax.fori_loop(0, count // chunk, body, 0)


def unalign(source, target, share, offset):
    down, lanes = offset // LANES, offset % LANES
    step = 64
    lane = lax.broadcasted_iota(jnp.int32, (step, LANES), 1)
    row = lax.broadcasted_iota(jnp.int32, (step, LANES), 0)

    def body(index, total):
        at = index * step
        here = pltpu.roll(source[pl.ds(down + at, step), :], LANES - lanes, 1)
        after = pltpu.roll(source[pl.ds(down + at + 1, step), :], LANES - lanes, 1)
        value = jnp.where(lane < LANES - lanes, here, after)
        value = jnp.where((row + at) * LANES + lane < share, value, 0.0)
        target[pl.ds(pl.multiple_of(at, 8), step), :] = value
        square = (value * value).reshape(step // 8, 8, LANES)
        return total + jnp.sum(square, axis=0)

    return lax.fori_loop(0, target.shape[0] // step, body, jnp.zeros((8, LANES), F32))


def flat_rows(share):
    return round_up(-(-share // LANES), 64)


def reduce_kernel(cplan, splan, *refs):
    nin = len(OUT_NAMES)
    grads, (small, bias, dbias, loss) = refs[:nin], refs[nin : nin + 4]
    g_split, g_common, sums = refs[nin + 4 : nin + 7]
    (wide, pair_buf, stage, gs, gd, gc, ks, xs, rz, acc, kc, yc, xc, rc, acy, acx, kd, yd, cq, fin, finc, part, stage_sem, send, recv) = refs[nin + 7 :]
    me, t = lax.axis_index(DP), lax.axis_index(TENSOR)
    z, x, y, c = me // 2, me % 2, t // 2, t % 2
    rank = me * 4 + t
    srows, quarter = splan.rows, cplan.rows // 4
    zdev = [{DP: (z + k) % 4 * 2 + x, TENSOR: t} for k in range(4)]
    xdev, ydev, kdev = {DP: z * 2 + (1 - x), TENSOR: t}, {DP: me, TENSOR: (1 - y) * 2 + c}, {DP: me, TENSOR: y * 2 + (1 - c)}
    others = [(rank + k) % 32 for k in range(1, 32)]
    devices = [{DP: other // 4, TENSOR: other % 4} for other in others]
    barrier = pltpu.get_barrier_semaphore()
    for device in devices:
        pl.semaphore_signal(barrier, inc=1, device_id=device, device_id_type=MESH)

    pack_all(y, grads, small, bias, dbias, wide, pair_buf, stage, stage_sem, gs, gd, gc)
    pl.semaphore_wait(barrier, 31)

    count, sent = [0], []

    def ship(source, target, device):
        index = count[0]
        count[0] += 1
        copy = pltpu.make_async_remote_copy(
            src_ref=source, dst_ref=target, send_sem=send.at[index], recv_sem=recv.at[index], device_id=device, device_id_type=MESH)
        copy.start()
        sent.append(copy)
        return copy

    def s_at(i):
        return pl.multiple_of(i * splan.share // BLOCK * TILE, TILE)

    def c_at(i, tt):
        return pl.multiple_of(i * cplan.share // BLOCK * TILE + tt * quarter, TILE)

    def frame_of(k, xx):
        return (z + k) % 4 * 2 + xx

    order = [frame_of(k, 1 - x) for k in (1, 2, 3, 0)] + [frame_of(k, x) for k in (1, 2, 3, 0)]
    keys = [(k, 0) for k in (1, 2, 3, 0)] + [(k, 1) for k in (1, 2, 3, 0)]
    kds = ship(gd.at[1 - c], kd, kdev)
    kcs, kss = [], []
    for n, i in enumerate(order):
        kcs.append([ship(gc.at[pl.ds(c_at(i, 2 * yy + 1 - c), quarter)], kc.at[n, yy], kdev) for yy in range(2)])
    for n, i in enumerate(order):
        kss.append(ship(gs.at[1 - c, pl.ds(s_at(i), srows)], ks.at[n], kdev))
    kds.wait_recv()
    add_rows(kd, [(gd.at[c], 0), (kd, 0)], D_WIDE)
    yds = ship(kd, yd, ydev)
    ycs = []
    for n, i in enumerate(order):
        for yy in range(2):
            kcs[n][yy].wait_recv()
        add_rows(acy.at[n], [(gc, c_at(i, 2 * (1 - y) + c)), (kc.at[n, 1 - y], 0)], quarter)
        ycs.append(ship(acy.at[n], yc.at[n], ydev))
    yds.wait_recv()
    add_rows(gs.at[c, pl.ds(DEC_FIRST, D_WIDE)], [(gs.at[c, pl.ds(DEC_FIRST, D_WIDE)], 0), (yd, 0)], D_WIDE)
    xss, xcs = [], []
    for n in range(4):
        i = order[n]
        kss[n].wait_recv()
        add_rows(acc.at[n], [(gs.at[c], s_at(i)), (ks.at[n], 0)], srows)
        xss.append(ship(acc.at[n], xs.at[n], xdev))
        ycs[n].wait_recv()
        add_rows(acx.at[n], [(gc, c_at(i, t)), (kc.at[n, y], 0), (yc.at[n], 0)], quarter)
        xcs.append(ship(acx.at[n], xc.at[n], xdev))
    zss, zcs = [], []
    for n in range(4, 7):
        i, k = order[n], n - 3
        kss[n].wait_recv()
        xss[n - 4].wait_recv()
        add_rows(acc.at[n], [(gs.at[c], s_at(i)), (ks.at[n], 0), (xs.at[n - 4], 0)], srows)
        zss.append(ship(acc.at[n], rz.at[k - 1], zdev[k]))
        ycs[n].wait_recv()
        xcs[n - 4].wait_recv()
        add_rows(acx.at[n], [(gc, c_at(i, t)), (kc.at[n, y], 0), (yc.at[n], 0), (xc.at[n - 4], 0)], quarter)
        zcs.append(ship(acx.at[n], rc.at[k - 1], zdev[k]))
    kss[7].wait_recv()
    xss[3].wait_recv()
    ycs[7].wait_recv()
    xcs[3].wait_recv()
    for copy in zcs:
        copy.wait_recv()
    mine = pl.ds(pl.multiple_of(t * quarter, TILE), quarter)
    add_rows(cq.at[mine], [(gc, c_at(me, t)), (kc.at[7, y], 0), (yc.at[7], 0), (xc.at[3], 0)] + [(rc.at[k], 0) for k in range(3)], quarter)
    across = ship(cq.at[mine], cq.at[mine], ydev)
    beside = ship(cq.at[mine], cq.at[mine], kdev)
    across.wait_recv()
    far = pl.ds(pl.multiple_of(((1 - y) * 2 + c) * quarter, TILE), quarter)
    beside2 = ship(cq.at[far], cq.at[far], kdev)
    for copy in zss:
        copy.wait_recv()
    add_rows(fin, [(gs.at[c], s_at(me)), (ks.at[7], 0), (xs.at[3], 0)] + [(rz.at[k], 0) for k in range(3)], srows)
    squares = unalign(fin, g_split, splan.share, me * splan.share % BLOCK)
    beside.wait_recv()
    beside2.wait_recv()
    add_rows(finc, [(cq, 0)], cplan.rows)
    squares += unalign(finc, g_common, cplan.share, me * cplan.share % BLOCK) * 0.25
    part[rank, 0:8, :] = squares
    part[rank, 8:16, :] = loss[...]
    shared = [ship(part.at[rank], part.at[rank], device) for device in devices]
    for copy in shared:
        copy.wait_recv()

    def total(index, value):
        return value + part[index]

    sums[...] = lax.fori_loop(0, 32, total, jnp.zeros((16, LANES), F32))
    for copy in sent:
        copy.wait_send()


def pack_kernel(*refs):
    nin = len(OUT_NAMES)
    grads, (small, bias, dbias) = refs[:nin], refs[nin : nin + 3]
    gs_out, gd_out, gc_out = refs[nin + 3 : nin + 6]
    wide, pair_buf, stage, gs, gd, gc, stage_sem, out_sem = refs[nin + 6 :]
    pack_all(lax.axis_index(TENSOR) // 2, grads, small, bias, dbias, wide, pair_buf, stage, stage_sem, gs, gd, gc)
    copies = [pltpu.make_async_copy(a, b, out_sem.at[k]) for k, (a, b) in enumerate(((gs, gs_out), (gd, gd_out), (gc, gc_out)))]
    for copy in copies:
        copy.start()
    for copy in copies:
        copy.wait()


def unalign_kernel(share_s, share_c, scalars, s_in, c_in, s_out, c_out, sums):
    sums[...] = unalign(s_in, s_out, share_s, scalars[0]) + unalign(c_in, c_out, share_c, scalars[1]) * 0.25


def reduce_grads(grads, small, bias, dbias, loss, cplan, splan):
    any_spec, vmem = pl.BlockSpec(memory_space=pl.ANY), pl.BlockSpec(memory_space=pltpu.VMEM)
    srows, quarter = splan.rows, cplan.rows // 4
    gs_rows, gc_rows = buffer_rows(splan, S_WIDE), buffer_rows(cplan, C_WIDE)
    flat = (jax.ShapeDtypeStruct((flat_rows(splan.share), LANES), F32), jax.ShapeDtypeStruct((flat_rows(cplan.share), LANES), F32))
    packing = [
        pltpu.VMEM((C_WIDE, LANES), F32), pltpu.VMEM((5, 64, LANES), F32), pltpu.VMEM((SLOTS, 768, 768), F32),
        pltpu.VMEM((2, gs_rows, LANES), BF16), pltpu.VMEM((2, D_WIDE, LANES), BF16), pltpu.VMEM((gc_rows, LANES), BF16)]
    operands = [vars(grads)[name] for name in OUT_NAMES]
    limit = 67_000_000
    if cplan.parts == 8 and splan.parts == 8:
        def rows(*shape, kind=BF16):
            return pltpu.VMEM(shape + (LANES,), kind)

        copies = 1 + 16 + 8 + 1 + 8 + 8 + 6 + 3 + 31
        return pl.pallas_call(
            functools.partial(reduce_kernel, cplan, splan),
            out_shape=flat + (jax.ShapeDtypeStruct((16, LANES), F32),),
            in_specs=[any_spec] * len(operands) + [vmem] * 4, out_specs=[vmem] * 3,
            scratch_shapes=packing + [
                rows(8, srows), rows(4, srows), rows(3, srows), rows(8, srows), rows(8, 2, quarter), rows(8, quarter), rows(4, quarter),
                rows(3, quarter), rows(8, quarter), rows(8, quarter), rows(D_WIDE), rows(D_WIDE), rows(cplan.rows),
                rows(srows + 64, kind=F32), rows(cplan.rows + 64, kind=F32), rows(32, 16, kind=F32),
                pltpu.SemaphoreType.DMA((SLOTS,)), pltpu.SemaphoreType.DMA((copies,)), pltpu.SemaphoreType.DMA((copies,))],
            compiler_params=pltpu.CompilerParams(collective_id=1, has_side_effects=True, vmem_limit_bytes=limit),
            name="reduce",
        )(*operands, small, bias, dbias, loss)
    shapes = [jax.ShapeDtypeStruct((2, gs_rows, LANES), BF16), jax.ShapeDtypeStruct((2, D_WIDE, LANES), BF16), jax.ShapeDtypeStruct((gc_rows, LANES), BF16)]
    gs, gd, gc = pl.pallas_call(
        pack_kernel, out_shape=shapes, in_specs=[any_spec] * len(operands) + [vmem] * 3, out_specs=[any_spec] * 3,
        scratch_shapes=packing + [pltpu.SemaphoreType.DMA((SLOTS,)), pltpu.SemaphoreType.DMA((3,))],
        compiler_params=pltpu.CompilerParams(vmem_limit_bytes=limit), name="pack",
    )(*operands, small, bias, dbias)
    me, t = lax.axis_index(DP), lax.axis_index(TENSOR)
    c = t % 2

    def swap(value, bit):
        return lax.ppermute(value, TENSOR, [(i, i ^ bit) for i in range(4)])

    def mine(value):
        keep = lax.dynamic_index_in_dim(value, c, 0, False).astype(F32)
        return keep + swap(lax.dynamic_index_in_dim(value, 1 - c, 0, False), 1).astype(F32)

    far = swap(mine(gd).astype(BF16), 2)
    split_sum = mine(gs).at[DEC_FIRST : DEC_FIRST + D_WIDE].add(far.astype(F32))
    common_sum = lax.psum(gc, TENSOR).astype(F32)

    def scattered(value, plan):
        frames = jnp.stack([value[base : base + plan.rows] for base in plan.base])
        return lax.psum_scatter(frames.astype(BF16), DP, scatter_dimension=0, tiled=True)[0].astype(F32)

    s_frame, c_frame = scattered(split_sum, splan), scattered(common_sum, cplan)
    pad = ((0, 64), (0, 0))
    g_split, g_common, squares = pl.pallas_call(
        functools.partial(unalign_kernel, splan.share, cplan.share), out_shape=flat + (jax.ShapeDtypeStruct((8, LANES), F32),),
        in_specs=[pl.BlockSpec(memory_space=pltpu.SMEM), vmem, vmem], out_specs=[vmem] * 3, name="unalign",
    )(jnp.stack([me * splan.share % BLOCK, me * cplan.share % BLOCK]).astype(jnp.int32), jnp.pad(s_frame, pad), jnp.pad(c_frame, pad))
    return g_split, g_common, lax.psum(jnp.concatenate([squares, loss]), (DP, TENSOR))


QROWS = 208
QBLOCKS = 4
OWN = TUBES // 2
SCALE = HEAD ** (-0.5)


def nt(a, b):
    return lax.dot_general(a, b, (((1,), (1,)), ((), ())), preferred_element_type=F32)


def nn(a, b):
    return lax.dot_general(a, b, (((1,), (0,)), ((), ())), preferred_element_type=F32)


def head_masks(rows):
    lane = lax.broadcasted_iota(jnp.int32, (rows, LANES), 1)
    return lane < HEAD, lane >= HEAD


def attend_kernel(q_ref, k_ref, vt_ref, o_ref, lse_ref):
    q, k = q_ref[...], k_ref[...]
    pieces = []
    for head, mask in enumerate(head_masks(QROWS)):
        scores = nt(k, jnp.where(mask, q, jnp.zeros_like(q)))
        top = jnp.max(scores, axis=0, keepdims=True)
        shifted = jnp.exp((scores - top) * SCALE)
        total = jnp.sum(shifted, axis=0, keepdims=True)
        value = nn(vt_ref[head * HEAD : (head + 1) * HEAD, :], shifted.astype(BF16))
        pieces.append(value / total)
        lse_ref[0, 0, head : head + 1, :] = top * SCALE + jnp.log(total)
    o_ref[...] = jnp.concatenate(pieces, axis=0).T


def attend(q, k, vt):
    return pl.pallas_call(
        attend_kernel, grid=(3, QBLOCKS),
        out_shape=(jax.ShapeDtypeStruct((QROWS * QBLOCKS, DD), F32), jax.ShapeDtypeStruct((3, QBLOCKS, 8, QROWS), F32)),
        in_specs=[
            pl.BlockSpec((QROWS, LANES), lambda h, i: (i, h)), pl.BlockSpec((TUBES, LANES), lambda h, i: (0, h)),
            pl.BlockSpec((LANES, TUBES), lambda h, i: (h, 0))],
        out_specs=[pl.BlockSpec((QROWS, LANES), lambda h, i: (i, h)), pl.BlockSpec((1, 1, 8, QROWS), lambda h, i: (h, i, 0, 0))],
        name="attend",
    )(q, k, vt)


def attend_back_kernel(q_ref, k_ref, v_ref, kt_ref, do_ref, o_ref, lse_ref, dq_ref, dk_ref, dv_ref):
    @pl.when(pl.program_id(1) == 0)
    def _():
        dk_ref[...] = jnp.zeros_like(dk_ref)
        dv_ref[...] = jnp.zeros_like(dv_ref)

    q, do, k, v = q_ref[...], do_ref[...], k_ref[...], v_ref[...]
    along = (do.astype(F32) * o_ref[...]).T
    pieces, dk, dv = [], None, None
    for head, mask in enumerate(head_masks(QROWS)):
        qm, dom = jnp.where(mask, q, jnp.zeros_like(q)), jnp.where(mask, do, jnp.zeros_like(do))
        delta = jnp.sum(along[head * HEAD : (head + 1) * HEAD], axis=0, keepdims=True)
        probs = jnp.exp(nt(k, qm) * SCALE - lse_ref[0, 0, head : head + 1, :])
        value = nn(probs.astype(BF16), dom)
        dv = value if dv is None else dv + value
        ds = (probs * (nt(v, dom) - delta)).astype(BF16)
        key = nn(ds, qm)
        dk = key if dk is None else dk + key
        pieces.append(nn(kt_ref[head * HEAD : (head + 1) * HEAD, :], ds))
    dq_ref[...] = (jnp.concatenate(pieces, axis=0) * SCALE).T.astype(BF16)
    dk_ref[...] += dk * SCALE
    dv_ref[...] += dv


def attend_back(q, k, v, kt, do, o, lse):
    block = pl.BlockSpec((QROWS, LANES), lambda h, i: (i, h))
    whole = pl.BlockSpec((TUBES, LANES), lambda h, i: (0, h))
    return pl.pallas_call(
        attend_back_kernel, grid=(3, QBLOCKS),
        out_shape=(jax.ShapeDtypeStruct((QROWS * QBLOCKS, DD), BF16), jax.ShapeDtypeStruct((TUBES, DD), F32), jax.ShapeDtypeStruct((TUBES, DD), F32)),
        in_specs=[block, whole, whole, pl.BlockSpec((LANES, TUBES), lambda h, i: (h, 0)), block, block, pl.BlockSpec((1, 1, 8, QROWS), lambda h, i: (h, i, 0, 0))],
        out_specs=[block, whole, whole],
        name="attend_back",
    )(q, k, v, kt, do, o, lse)


NORM_EPS = 1e-06
PIXEL_EPS = 1e-06
CLIP_RATIO = 1.5
BETA_FIRST = 0.9
BETA_SECOND = 0.95
LEARN_RATE = 0.05
DECAY_RATE = 0.05
ADAM_EPS = 1e-08


def layer_norm(inputs, gain, shift):
    centered = inputs - jnp.mean(inputs, axis=-1, keepdims=True)
    spread = jnp.mean(centered * centered, axis=-1, keepdims=True)
    return centered * lax.rsqrt(spread + NORM_EPS) * gain + shift


def norm_back(inputs, gain, grad):
    centered = inputs - jnp.mean(inputs, axis=-1, keepdims=True)
    scale = lax.rsqrt(jnp.mean(centered * centered, axis=-1, keepdims=True) + NORM_EPS)
    unit = centered * scale
    inner = grad * gain
    back = scale * (inner - jnp.mean(inner, axis=-1, keepdims=True) - unit * jnp.mean(inner * unit, axis=-1, keepdims=True))
    return back, jnp.sum(grad * unit, axis=0), jnp.sum(grad, axis=0)


def tn(a, b):
    return lax.dot_general(a, b, (((0,), (0,)), ((), ())), preferred_element_type=F32)


def gelu(inputs):
    return jax.nn.gelu(inputs, approximate=False)


def gelu_slope(inputs):
    return 0.5 * (1.0 + lax.erf(inputs * math.sqrt(0.5))) + inputs * jnp.exp(-0.5 * inputs * inputs) * (1.0 / math.sqrt(2.0 * math.pi))


def sine_rows(position, width):
    column = jnp.arange(width)
    exponent = (2 * (column // 2)).astype(F32) / width
    angles = position.astype(F32)[:, None] / jnp.power(10000.0, exponent)[None, :]
    return jnp.where((column % 2 == 0)[None, :], jnp.sin(angles), jnp.cos(angles))


def sine_table(width, step=32):
    column = np.arange(width)
    rate = 10000.0 ** (-(2 * (column // 2)) / width)
    high, low = np.arange(0, TUBES, step)[:, None] * rate, np.arange(step)[:, None] * rate
    even = column % 2 == 0
    a = np.where(even, np.sin(high), np.cos(high)).astype(np.float32)
    b = np.where(even, np.cos(high), -np.sin(high)).astype(np.float32)
    c, s = np.cos(low).astype(np.float32), np.sin(low).astype(np.float32)
    table = a[:, None] * jnp.asarray(c)[None] + b[:, None] * jnp.asarray(s)[None]
    return table.reshape(TUBES, width)


def across(value):
    return lax.ppermute(value, TENSOR, [(i, i ^ 2) for i in range(4)])


def beside(value):
    return lax.ppermute(value, TENSOR, [(i, i ^ 1) for i in range(4)])


def y_total(partial):
    low = partial.astype(BF16)
    return low.astype(F32) + across(low).astype(F32)


def heads_of(mixed):
    parts = mixed.reshape(VIS, 2, 3, 3, HEAD)
    return [parts[:, :, k].transpose(1, 2, 0, 3).reshape(6, VIS, HEAD) for k in range(3)]


def heads_back(parts):
    stacked = jnp.stack([part.reshape(2, 3, VIS, HEAD) for part in parts], axis=1)
    return stacked.transpose(3, 0, 1, 2, 4).reshape(VIS, 1152)


def step_grads(pixels, order, w, scale_back):
    t = lax.axis_index(TENSOR)
    y, c = t // 2, t % 2
    first_y = (y == 0).astype(F32)
    seen = lax.dynamic_index_in_dim(order, c, 0, False)[:VIS]
    seen_y = lax.dynamic_index_in_dim(order, y, 0, False)[:VIS]
    rows = pixels.reshape(2 * TUBES, PATCH)
    seen_pixels = jnp.take(rows, c * TUBES + seen, axis=0)
    embedded = nn(seen_pixels, w.embedding) + w.embedding_bias + sine_rows(seen, D)
    norms, biases = w.enc_norms, w.enc_biases
    normed_a = layer_norm(embedded, norms[0], norms[1]).astype(BF16)
    qkv_w = jnp.concatenate([w.enc_qkv[0], w.enc_qkv[1]], axis=1)
    zero = jnp.zeros((192,), F32)
    qkv_b = jnp.concatenate([piece for k in range(2) for piece in (w.enc_qkv_bias[k, 0], zero, w.enc_qkv_bias[k, 1])])
    q, k, v = heads_of((nn(normed_a, qkv_w) + qkv_b).astype(BF16))
    scores = jnp.einsum("hqe,hke->hqk", q, k, preferred_element_type=F32) * SCALE
    probs = jax.nn.softmax(scores, axis=-1)
    probs_low = probs.astype(BF16)
    out = jnp.einsum("hqk,hke->hqe", probs_low, v, preferred_element_type=F32).astype(BF16)
    merged = out.transpose(1, 0, 2).reshape(VIS, 384)
    after = embedded + (y_total(nn(merged, w.enc_proj)) + biases[0])
    normed_m = layer_norm(after, norms[2], norms[3]).astype(BF16)
    raised = nn(normed_m, w.enc_up) + w.enc_up_bias
    active = gelu(raised).astype(BF16)
    encoded = after + (y_total(nn(active, w.enc_down)) + biases[1])
    final_low = layer_norm(encoded, norms[4], norms[5]).astype(BF16)
    moved = lax.ppermute(final_low, TENSOR, [(0, 1), (3, 2)])
    mine = jnp.where(y == c, final_low, moved)
    lowered = nn(mine, w.to_decoder)
    select = seen_y[None, :] == jnp.arange(TUBES, dtype=jnp.int32)[:, None]
    visible = jnp.any(select, axis=1, keepdims=True)
    placed = lax.dot_general(select.astype(F32), lowered, (((1,), (0,)), ((), ())), precision=lax.Precision.HIGHEST, preferred_element_type=F32)
    dec_in = placed + jnp.where(visible, 0.0, w.mask_token) + sine_table(DD)
    start = c * OWN

    def own(value):
        return lax.dynamic_slice_in_dim(value, start, OWN, 0)

    dnorms, dbiases = w.dec_norms, w.dec_biases
    normed_all = layer_norm(dec_in, dnorms[0], dnorms[1]).astype(BF16)
    normed_q = own(normed_all)
    dec_own = own(dec_in)
    query = (nn(normed_q, w.dec_qkv[:, :DD]) + w.dec_qkv_bias[0]).astype(BF16)
    key = nn(normed_all, w.dec_qkv[:, DD : 2 * DD]).astype(BF16)
    value = (nn(normed_all, w.dec_qkv[:, 2 * DD :]) + w.dec_qkv_bias[1]).astype(BF16)
    pad = ((0, QROWS * QBLOCKS - OWN), (0, 0))
    query = jnp.pad(query, pad)
    attended, lse = attend(query, key, value.T)
    attended_low = attended[:OWN].astype(BF16)
    mid = dec_own + (nn(attended_low, w.dec_proj) + dbiases[0])
    normed_d = layer_norm(mid, dnorms[2], dnorms[3]).astype(BF16)
    draised = nn(normed_d, w.dec_up) + w.dec_up_bias
    dactive = gelu(draised).astype(BF16)
    decoded = mid + (nn(dactive, w.dec_down) + dbiases[1])
    head_low = layer_norm(decoded, dnorms[4], dnorms[5]).astype(BF16)
    predicted = nn(head_low, w.pixel_head) + w.head_bias
    target = lax.dynamic_slice_in_dim(rows, y * TUBES + start, OWN, 0).astype(F32)
    target = target - jnp.mean(target, axis=-1, keepdims=True)
    target = target * lax.rsqrt(jnp.mean(target * target, axis=-1, keepdims=True) + PIXEL_EPS)
    hidden = 1.0 - own(visible.astype(F32))
    missing = (predicted - target) * hidden
    loss = jnp.sum((missing * missing).reshape(-1, 8, PATCH // LANES, LANES), axis=(0, 2))
    pred_grad = (2.0 * scale_back * missing).astype(BF16)
    grads, small = Namespace(), Namespace()
    grads.pixel_head = tn(head_low, pred_grad)
    small.head_bias = jnp.sum(pred_grad, axis=0, dtype=F32)
    decoded_grad, dg4, dg5 = norm_back(decoded, dnorms[4], nt(pred_grad, w.pixel_head))
    branch = decoded_grad.astype(BF16)
    grads.dec_down = tn(dactive, branch)
    db1 = jnp.sum(branch, axis=0, dtype=F32)
    draised_grad = (nt(branch, w.dec_down) * gelu_slope(draised)).astype(BF16)
    grads.dec_up = tn(normed_d, draised_grad)
    dec_up_bias = jnp.sum(draised_grad, axis=0, dtype=F32)
    back, dg2, dg3 = norm_back(mid, dnorms[2], nt(draised_grad, w.dec_up))
    mid_grad = decoded_grad + back
    branch = mid_grad.astype(BF16)
    grads.dec_proj = tn(attended_low, branch)
    db0 = jnp.sum(branch, axis=0, dtype=F32)
    attended_grad = jnp.pad(nt(branch, w.dec_proj).astype(BF16), pad)
    query_grad, key_grad, value_grad = attend_back(query, key, value, key.T, attended_grad, attended, lse)

    def shared(total):
        keep = lax.dynamic_slice_in_dim(total, start, OWN, 0)
        give = lax.dynamic_slice_in_dim(total, OWN - start, OWN, 0).astype(BF16)
        return (keep + beside(give).astype(F32)).astype(BF16)

    mixed = jnp.concatenate([query_grad[:OWN], shared(key_grad), shared(value_grad)], axis=1)
    grads.dec_qkv = tn(normed_q, mixed)
    dqb = jnp.sum(mixed, axis=0, dtype=F32)
    small.dec_qkv_bias = jnp.concatenate([dqb[:DD], dqb[2 * DD :]])
    back, dg0, dg1 = norm_back(dec_own, dnorms[0], nt(mixed, w.dec_qkv))
    in_grad = mid_grad + back
    small.mask_token = jnp.sum(in_grad * hidden, axis=0)
    part = tn(own(select).astype(BF16), in_grad.astype(BF16)).astype(BF16)
    near = lax.ppermute(part, TENSOR, [(1, 0), (2, 3)])
    joined = part + near
    far = lax.ppermute(joined, TENSOR, [(0, 2), (3, 1)])
    lowered_grad = jnp.where(y == c, joined, far)
    grads.to_decoder = tn(final_low, lowered_grad) * first_y
    encoded_grad, eg4, eg5 = norm_back(encoded, norms[4], nt(lowered_grad, w.to_decoder))
    branch = encoded_grad.astype(BF16)
    grads.enc_down = tn(active, branch)
    eb1 = jnp.sum(branch, axis=0, dtype=F32)
    raised_grad = (nt(branch, w.enc_down) * gelu_slope(raised)).astype(BF16)
    grads.enc_up = tn(normed_m, raised_grad)
    enc_up_bias = jnp.sum(raised_grad, axis=0, dtype=F32)
    back, eg2, eg3 = norm_back(after, norms[2], y_total(nt(raised_grad, w.enc_up)))
    after_grad = encoded_grad + back
    branch = after_grad.astype(BF16)
    grads.enc_proj = tn(merged, branch)
    eb0 = jnp.sum(branch, axis=0, dtype=F32)
    merged_grad = nt(branch, w.enc_proj).astype(BF16).reshape(VIS, 6, HEAD).transpose(1, 0, 2)
    v_grad = jnp.einsum("hqk,hqe->hke", probs_low, merged_grad, preferred_element_type=F32).astype(BF16)
    probs_grad = jnp.einsum("hqe,hke->hqk", merged_grad, v, preferred_element_type=F32)
    scores_low = (probs * (probs_grad - jnp.sum(probs_grad * probs, axis=-1, keepdims=True))).astype(BF16)
    q_grad = (jnp.einsum("hqk,hke->hqe", scores_low, k, preferred_element_type=F32) * SCALE).astype(BF16)
    k_grad = (jnp.einsum("hqk,hqe->hke", scores_low, q, preferred_element_type=F32) * SCALE).astype(BF16)
    emixed = heads_back([q_grad, k_grad, v_grad])
    wide_mixed = jnp.pad(emixed.reshape(VIS, 2, 576), ((0, 0), (0, 0), (0, 64))).reshape(VIS, 1280)
    grads.enc_qkv = tn(normed_a, wide_mixed)
    eqb = jnp.sum(emixed, axis=0, dtype=F32).reshape(2, 3, 192)
    back, eg0, eg1 = norm_back(embedded, norms[0], y_total(nt(emixed, qkv_w)))
    embedded_low = (after_grad + back).astype(BF16)
    grads.embedding = tn(lax.dynamic_slice_in_dim(seen_pixels, y * 768, 768, 1), embedded_low)
    embedding_bias = jnp.sum(embedded_low, axis=0, dtype=F32)
    small_a = jnp.concatenate([embedding_bias, eg0, eg1, eg2, eg3, eg4, eg5, eb0, eb1]) * first_y
    small_b = jnp.concatenate([small.mask_token, dg0, dg1, dg2, dg3, dg4, dg5, db0, db1])
    tiles = []
    for piece in (small_a, small_b, small.dec_qkv_bias, small.head_bias):
        count = piece.shape[0] // LANES
        tiles.append(jnp.pad(piece.reshape(count, LANES), ((0, -count % 8), (0, 0))))
    bias = jnp.concatenate(
        [jnp.pad(eqb[:, ::2].reshape(2, 3, LANES), ((0, 0), (0, 5), (0, 0))), jnp.pad(enc_up_bias.reshape(2, 6, LANES), ((0, 0), (0, 2), (0, 0)))], axis=1)
    dbias = jnp.pad(dec_up_bias.reshape(4, 3, LANES), ((0, 0), (0, 5), (0, 0)))
    return loss, grads, jnp.concatenate(tiles), bias, dbias


def adamw(master, first, second, gradient):
    first_new = BETA_FIRST * first + (1.0 - BETA_FIRST) * gradient
    second_new = BETA_SECOND * second + (1.0 - BETA_SECOND) * gradient * gradient
    first_hat = first_new / (1.0 - BETA_FIRST**STEP)
    second_hat = second_new / (1.0 - BETA_SECOND**STEP)
    master_new = master - LEARN_RATE * (first_hat / (jnp.sqrt(second_hat) + ADAM_EPS) + DECAY_RATE * master)
    return (master_new, first_new, second_new, master_new.astype(BF16))


def shards(tubes, tube_order, common_master, common_first, common_second, split_master, split_first, split_second):
    groups = lax.axis_size(DP)
    cplan = Plan(groups, common_master.shape[0], 64)
    splan = Plan(groups, split_master.shape[1], TILE)
    masked_total = tubes.shape[0] * groups * (TUBES - VIS)
    pixel_count = masked_total * PATCH
    w = gather_weights(common_master, split_master, cplan, splan)
    loss, grads, small, bias, dbias = step_grads(tubes, tube_order, w, 1.0 / pixel_count)
    g_split, g_common, sums = reduce_grads(grads, small, bias, dbias, loss, cplan, splan)
    loss_mean = jnp.sum(sums[8:]) / pixel_count
    grad_norm = jnp.sqrt(jnp.sum(sums[:8]))
    factor = jnp.minimum(1.0, CLIP_RATIO / math.sqrt(masked_total) / (grad_norm + 1e-06))
    common = adamw(common_master, common_first, common_second, g_common.reshape(-1)[: common_master.shape[0]] * factor)
    split = adamw(split_master, split_first, split_second, g_split.reshape(1, -1)[:, : split_master.shape[1]] * factor)
    return (loss_mean.reshape(1), grad_norm.reshape(1)) + common + split


def solution(mesh):
    in_specs = (P(DP, None, None), P(DP, None), P(DP), P(DP), P(DP), P(TENSOR, DP), P(TENSOR, DP), P(TENSOR, DP))
    out_specs = (P(), P()) + (P(DP),) * 4 + (P(TENSOR, DP),) * 4
    return jax.shard_map(shards, mesh=mesh, in_specs=in_specs, out_specs=out_specs, check_vma=False)
```

```python
import functools
import math
from types import SimpleNamespace as Namespace

import jax
import jax.numpy as jnp
import numpy as np
from jax import lax
from jax.experimental import pallas as pl
from jax.experimental.pallas import tpu as pltpu
from jax.sharding import PartitionSpec as P

DP = "dp"
TENSOR = "tensor"
D = 768
HEAD = 64
FF = 3072
DD = 384
DFF = 1536
PATCH = 1536
TUBES = 1568
VIS = 157
STEP = 10
LANES = 128
TILE = 16
BLOCK = TILE * LANES
FRONT = 24
MESH = pl.DeviceIdType.MESH
F32 = jnp.float32
BF16 = jnp.bfloat16


def round_up(value, step):
    return -(-value // step) * step


COMMON = dict(
    embedding=(PATCH, D), embedding_bias=(D,), enc_norms=(6, D), enc_biases=(2, D), to_decoder=(D, DD), mask_token=(DD,),
    dec_norms=(6, DD), dec_biases=(2, DD), dec_qkv=(DD, 3 * DD), dec_qkv_bias=(2, DD), dec_proj=(DD, DD), pixel_head=(DD, PATCH),
    head_bias=(PATCH,))
SPLIT = dict(
    enc_qkv=(D, 576), enc_qkv_bias=(2, 192), enc_proj=(192, D), enc_up=(D, 768), enc_up_bias=(768,), enc_down=(768, D),
    dec_up=(DD, 384), dec_up_bias=(384,), dec_down=(384, DD))


def row_table(layout):
    table, at = {}, 0
    for name, shape in layout.items():
        count = math.prod(shape) // LANES
        table[name] = (at, count)
        at += count
    return Namespace(**table)


CROW = row_table(COMMON)
SROW = row_table(SPLIT)
DEC_ROW = SROW.dec_up[0]
SPLIT_ROWS = SROW.dec_down[0] + SROW.dec_down[1]
COMMON_ROWS = CROW.head_bias[0] + CROW.head_bias[1]


class Plan:
    def __init__(self, parts, share, rows_step):
        self.parts, self.share = parts, share
        self.base = [i * share // BLOCK * TILE for i in range(parts)]
        self.rows = round_up(-(-(share + BLOCK - 1) // LANES), rows_step)

    def pieces(self, first, last):
        out = []
        for i in range(self.parts):
            start = self.base[i] + (TILE if i else 0)
            stop = self.base[i + 1] if i + 1 < self.parts else self.base[i] + self.rows
            low, high = max(start, first), min(stop, last)
            if i and first <= self.base[i] < last:
                out.append(("edge", i, self.base[i] - self.base[i - 1], self.base[i], TILE))
            if low < high:
                out.append(("body", i, low - self.base[i], low, high - low))
        return out

    def owners(self, first, last):
        return sorted({i for kind, i, *_ in self.pieces(first, last)} | {i - 1 for kind, i, *_ in self.pieces(first, last) if kind == "edge"})


def align_kernel(scalars, split_in, common_in, split_out, common_out):
    def move(source, target, lanes, rows_down, skip, step):
        def part(row, step):
            lane = lax.broadcasted_iota(jnp.int32, (step, LANES), 1)
            here = source[pl.ds(FRONT - rows_down + skip + row, step), :]
            before = source[pl.ds(FRONT - 1 - rows_down + skip + row, step), :]
            value = jnp.where(lane >= lanes, pltpu.roll(here, lanes, 1), pltpu.roll(before, lanes, 1))
            target[pl.ds(pl.multiple_of(row, TILE), step), :] = value.astype(BF16)

        def body(index, _):
            part(index * step, step)
            return 0

        whole = target.shape[0] // step
        lax.fori_loop(0, whole, body, 0)
        if target.shape[0] % step:
            part(whole * step, target.shape[0] % step)

    move(split_in, split_out, scalars[0], scalars[1], 0, 256)
    move(common_in, common_out, scalars[2], scalars[3], scalars[4], 256)


def aligned(master, plan):
    tail = (plan.rows + 8) * LANES - master.shape[-1]
    return jnp.pad(master, ((0, 0),) * (master.ndim - 1) + ((FRONT * LANES, tail),)).reshape(-1, LANES)


def align(common_master, split_master, cplan, splan):
    me, t = lax.axis_index(DP), lax.axis_index(TENSOR)
    soff = me * splan.share % BLOCK
    coff = me * cplan.share % BLOCK
    quarter = cplan.rows // 4
    scalars = jnp.stack([soff % LANES, soff // LANES, coff % LANES, coff // LANES, t * quarter]).astype(jnp.int32)
    return pl.pallas_call(
        align_kernel,
        out_shape=(jax.ShapeDtypeStruct((splan.rows, LANES), BF16), jax.ShapeDtypeStruct((quarter, LANES), BF16)),
        in_specs=[pl.BlockSpec(memory_space=pltpu.SMEM), pl.BlockSpec(memory_space=pltpu.VMEM), pl.BlockSpec(memory_space=pltpu.VMEM)],
        out_specs=[pl.BlockSpec(memory_space=pltpu.VMEM)] * 2,
        name="align",
    )(scalars, aligned(split_master, splan), aligned(common_master, cplan))


OUTS = Namespace(
    embedding=(PATCH, D), to_decoder=(D, DD), dec_qkv=(DD, 3 * DD), dec_proj=(DD, DD), pixel_head=(DD, PATCH),
    enc_qkv=(2, D, 576), enc_proj=(384, D), enc_up=(D, 1536), enc_down=(1536, D), dec_up=(DD, 1536), dec_down=(1536, DD))
OUT_NAMES = tuple(vars(OUTS))
CMATS = OUT_NAMES[:5]
SMALLS = ((CROW.embedding_bias[0], 54), (CROW.mask_token[0], 27), (CROW.dec_qkv_bias[0], 6), (CROW.head_bias[0], 12))


def copy_rows(pieces, frame, wide, first, chunk=64):
    for kind, part, row, at, count in pieces:
        if kind == "edge":
            wide[pl.ds(at - first, TILE), :] = frame(part)[pl.ds(0, TILE), :].astype(F32) + frame(part - 1)[pl.ds(row, TILE), :].astype(F32)
            continue
        source, whole = frame(part), count // chunk

        def body(index, _, source=source, row=row, at=at):
            wide[pl.ds(pl.multiple_of(at - first + index * chunk, TILE), chunk), :] = source[
                pl.ds(pl.multiple_of(row + index * chunk, TILE), chunk), :
            ].astype(F32)
            return 0

        if whole:
            lax.fori_loop(0, whole, body, 0)
        for rest in range(whole * chunk, count, TILE):
            wide[pl.ds(at - first + rest, TILE), :] = source[pl.ds(row + rest, TILE), :].astype(F32)


def matrix_out(wide, start, rows, width, target, row0, col0, step=64):
    per_row = width // LANES

    def body(index, _):
        at = index * step
        for j in range(per_row):
            value = wide[pl.ds(start + j + at * per_row, step, stride=per_row), :]
            target[pl.ds(pl.multiple_of(row0 + at, TILE), step), col0 + j * LANES : col0 + (j + 1) * LANES] = value.astype(BF16)
        return 0

    lax.fori_loop(0, rows // step, body, 0)


def qkv_out(wide, start, pair_buf, target):
    step = 32
    lane = lax.broadcasted_iota(jnp.int32, (step, LANES), 1)

    def body(index, _):
        at = start + index * step * 9
        for j in range(5):
            even = wide[pl.ds(at + j, step, stride=9), :]
            low = pltpu.roll(wide[pl.ds(at + 4 + j, step, stride=9), :], 64, 1)
            if j < 4:
                high = pltpu.roll(wide[pl.ds(at + 5 + j, step, stride=9), :], 64, 1)
                odd = jnp.where(lane < 64, low, high)
            else:
                odd = low
            pair_buf[j, pl.ds(0, step, stride=2), :] = even
            pair_buf[j, pl.ds(1, step, stride=2), :] = odd
            both = pair_buf[j].astype(BF16)
            rows = pl.ds(pl.multiple_of(index * 64, 64), 64)
            if j < 4:
                target[rows, j * LANES : (j + 1) * LANES] = both
            else:
                target[rows, 512:576] = both[:, :64]
        return 0

    lax.fori_loop(0, 12, body, 0)


def floor16(value):
    return value // TILE * TILE


def unpack_into(cplan, splan, common_frame, split_frame, dec_frame, stage, small_ref, bias_ref, dbias_ref, wide, pair_buf, done):
    def load(plan, frame, start, count):
        first, last = floor16(start), round_up(start + count, TILE)
        copy_rows(plan.pieces(first, last), frame, wide, first)
        return start - first

    for c in range(2):
        frame = functools.partial(split_frame, c)
        start, count = SROW.enc_qkv
        qkv_out(wide, load(splan, frame, start, count), pair_buf, stage.enc_qkv.at[c])
        if c:
            done(stage.enc_qkv)
        at = load(splan, frame, *SROW.enc_qkv_bias)
        bias_ref[c, 0:8, :] = wide[pl.ds(at, 8), :]
        at = load(splan, frame, *SROW.enc_proj)
        matrix_out(wide, at, 192, D, stage.enc_proj, c * 192, 0)
        if c:
            done(stage.enc_proj)
        at = load(splan, frame, *SROW.enc_up)
        matrix_out(wide, at, D, 768, stage.enc_up, 0, c * 768)
        if c:
            done(stage.enc_up)
        at = load(splan, frame, *SROW.enc_up_bias)
        bias_ref[c, 8:16, :] = wide[pl.ds(at, 8), :]
        at = load(splan, frame, *SROW.enc_down)
        matrix_out(wide, at, 768, D, stage.enc_down, c * 768, 0)
        if c:
            done(stage.enc_down)
    at = load(cplan, common_frame, *CROW.embedding)
    matrix_out(wide, at, PATCH, D, stage.embedding, 0, 0)
    done(stage.embedding)
    for name in CMATS[1:]:
        at = load(cplan, common_frame, *vars(CROW)[name])
        rows, width = vars(OUTS)[name]
        matrix_out(wide, at, rows, width, vars(stage)[name], 0, 0)
        done(vars(stage)[name])
    small_at = 0
    for start, count in SMALLS:
        at = load(cplan, common_frame, start, count)
        small_ref[pl.ds(small_at, round_up(count, 8)), :] = wide[pl.ds(at, round_up(count, 8)), :]
        small_at += round_up(count, 8)
    for slot in range(4):
        frame = functools.partial(split_frame, slot) if slot < 2 else functools.partial(dec_frame, slot - 2)
        at = load(splan, frame, DEC_ROW, SPLIT_ROWS - DEC_ROW)
        matrix_out(wide, at, DD, 384, stage.dec_up, 0, slot * 384)
        bias = at + SROW.dec_up_bias[0] - DEC_ROW
        dbias_ref[slot, :, :] = wide[pl.ds(bias, 8), :]
        matrix_out(wide, bias + 3, 384, DD, stage.dec_down, slot * 384, 0)
    done(stage.dec_up)
    done(stage.dec_down)


SMALL_ROWS = sum(round_up(count, 8) for _, count in SMALLS)
GATHERED = tuple(jax.ShapeDtypeStruct(vars(OUTS)[name], BF16) for name in OUT_NAMES) + (
    jax.ShapeDtypeStruct((SMALL_ROWS, LANES), F32), jax.ShapeDtypeStruct((2, 16, LANES), F32), jax.ShapeDtypeStruct((4, 8, LANES), F32))


def first_dec(splan):
    return splan.owners(floor16(DEC_ROW), round_up(SPLIT_ROWS, TILE))[0]


def unpack_scratch(cplan, splan):
    fd = first_dec(splan)
    return [
        pltpu.VMEM((2, splan.parts, splan.rows, LANES), BF16),
        pltpu.VMEM((2, splan.parts - fd, splan.rows, LANES), BF16),
        pltpu.VMEM((cplan.parts, 4, cplan.rows // 4, LANES), BF16),
        pltpu.VMEM((CROW.embedding[1] + 32, LANES), F32),
        pltpu.VMEM((5, 64, LANES), F32),
    ] + [pltpu.VMEM(vars(OUTS)[name], BF16) for name in OUT_NAMES] + [pltpu.SemaphoreType.DMA((len(OUT_NAMES),))]


def finish_unpack(cplan, splan, outs, smalls, sbuf, dbuf, cbuf, wide, pair_buf, stages, out_sem):
    fd = first_dec(splan)
    stage = Namespace(**dict(zip(OUT_NAMES, stages)))
    copies = []

    def done(whole):
        index = [ref is whole for ref in stages].index(True)
        copy = pltpu.make_async_copy(whole, outs[index], out_sem.at[index])
        copy.start()
        copies.append(copy)

    unpack_into(
        cplan, splan, lambda i: cbuf.at[i], lambda c, i: sbuf.at[c, i], lambda c, i: dbuf.at[c, i - fd],
        stage, smalls[0], smalls[1], smalls[2], wide, pair_buf, done)
    for copy in copies:
        copy.wait()


def gather_kernel(cplan, splan, s_own, c_own, *refs):
    nout = len(OUT_NAMES)
    outs, smalls = refs[:nout], refs[nout : nout + 3]
    sbuf, dbuf, cbuf, wide, pair_buf = refs[nout + 3 : nout + 8]
    stages, out_sem = refs[nout + 8 : 2 * nout + 8], refs[2 * nout + 8]
    send, recv, local = refs[2 * nout + 9 :]
    me, t = lax.axis_index(DP), lax.axis_index(TENSOR)
    z, x, y, c = me // 2, me % 2, t // 2, t % 2
    ty = (1 - y) * 2 + c
    fd = first_dec(splan)
    quarter = cplan.rows // 4

    def cblock(i, tt):
        return cbuf.at[i, pl.ds(pl.multiple_of(tt * quarter, TILE), quarter)]

    def sblock(i):
        return sbuf.at[c, i]

    zdev = [{DP: (z + k) % 4 * 2 + x, TENSOR: t} for k in range(4)]
    xdev, ydev, kdev = {DP: z * 2 + (1 - x), TENSOR: t}, {DP: me, TENSOR: ty}, {DP: me, TENSOR: y * 2 + (1 - c)}
    barrier = pltpu.get_barrier_semaphore()
    for device in zdev[1:] + [xdev, ydev, kdev]:
        pl.semaphore_signal(barrier, inc=1, device_id=device, device_id_type=MESH)
    own = [pltpu.make_async_copy(s_own, sblock(me), local.at[0]), pltpu.make_async_copy(c_own, cblock(me, t), local.at[1])]
    for copy in own:
        copy.start()
    pl.semaphore_wait(barrier, 6)
    for copy in own:
        copy.wait()

    def remote(source, target, slot, device):
        return pltpu.make_async_remote_copy(
            src_ref=source, dst_ref=target, send_sem=send.at[slot], recv_sem=recv.at[slot], device_id=device, device_id_type=MESH)

    def z_copy(common, down, hop, i):
        block = cblock(i, t) if common else sblock(i)
        return remote(block, block, common * 6 + down * 3 + hop - 1, zdev[3 if down else 1])

    def x_copy(common, i):
        block = cblock(i, t) if common else sblock(i)
        return remote(block, block, 12 + common * 4 + i // 2, xdev)

    def y_copy(i):
        return remote(cblock(i, t), cblock(i, t), 20 + i, ydev)

    def k_copy(i):
        return remote(sblock(i), sblock(i), 28 + i, kdev)

    def k_common(i):
        return remote(cblock(i, t), cblock(i, t), 36 + i, kdev)

    def k_far(i):
        return remote(cblock(i, ty), cblock(i, ty), 44 + i, kdev)

    def dec_rows(i):
        return pl.ds(max(0, DEC_FIRST - splan.base[i]), min(splan.rows, S_WIDE - splan.base[i]) - max(0, DEC_FIRST - splan.base[i]))

    def d_copy(i):
        return remote(sbuf.at[c, i, dec_rows(i)], dbuf.at[c, i - fd, dec_rows(i)], 52 + i - fd, ydev)

    def d_beside(i):
        return remote(dbuf.at[c, i - fd, dec_rows(i)], dbuf.at[c, i - fd, dec_rows(i)], 54 + i - fd, kdev)

    def send_z(common, down, hop):
        i = (z + (hop - 1 if down else 1 - hop)) * 2 + x
        able = jnp.logical_and(z > 0, z + hop - 1 <= 3) if down else jnp.logical_and(z < 3, z - hop + 1 >= 0)
        return i, able

    def pass_on(common, down, hop, action):
        i, able = send_z(common, down, hop)

        @pl.when(able)
        def _():
            action(z_copy(common, down, hop, i))

    def share_c(i):
        x_copy(1, i).start()
        y_copy(i).start()
        k_common(i).start()

    def share_s(i):
        x_copy(0, i).start()
        k_copy(i).start()
        dec_start(i)

    def dec_start(i):
        for known in range(fd, splan.parts):
            @pl.when(i == known)
            def _(known=known):
                d_copy(known).start()

    for common in (1, 0):
        for down in (0, 1):
            pass_on(common, down, 1, lambda copy: copy.start())
    share_c(me)
    share_s(me)
    for hop in (1, 2, 3):
        for common in (1, 0):
            for down in (0, 1):
                i = (z + (hop if down else -hop)) * 2 + x
                here = z + hop <= 3 if down else z >= hop

                @pl.when(here)
                def _(common=common, down=down, hop=hop, i=i):
                    z_copy(common, down, hop, i).wait_recv()
                    if hop < 3:
                        pass_on(common, down, hop + 1, lambda copy: copy.start())
                    if common:
                        share_c(i)
                    else:
                        share_s(i)

    for zz in range(4):
        i = zz * 2 + (1 - x)
        x_copy(1, i).wait_recv()
        y_copy(i).start()
        k_common(i).start()
    for i in range(8):
        y_copy(i).wait_recv()
        k_far(i).start()
    for zz in range(4):
        i = zz * 2 + (1 - x)
        x_copy(0, i).wait_recv()
        k_copy(i).start()
        dec_start(i)
    for i in range(fd, splan.parts):
        d_copy(i).wait_recv()
        d_beside(i).start()
    for i in range(8):
        k_common(i).wait_recv()
        k_far(i).wait_recv()
        k_copy(i).wait_recv()
    for i in range(fd, splan.parts):
        d_beside(i).wait_recv()
    for hop in (1, 2, 3):
        for common in (1, 0):
            for down in (0, 1):
                pass_on(common, down, hop, lambda copy: copy.wait_send())
    for zz in range(4):
        for common in (1, 0):
            x_copy(common, zz * 2 + x).wait_send()
    for i in range(8):
        for copy in (y_copy(i), k_copy(i), k_common(i), k_far(i)):
            copy.wait_send()
    for i in range(fd, splan.parts):
        d_copy(i).wait_send()
        d_beside(i).wait_send()
    finish_unpack(cplan, splan, outs, smalls, sbuf, dbuf, cbuf, wide, pair_buf, stages, out_sem)


def local_unpack_kernel(cplan, splan, s_all, d_all, c_all, *refs):
    nout = len(OUT_NAMES)
    outs, smalls = refs[:nout], refs[nout : nout + 3]
    sbuf, dbuf, cbuf, wide, pair_buf = refs[nout + 3 : nout + 8]
    stages, out_sem = refs[nout + 8 : 2 * nout + 8], refs[2 * nout + 8]
    local = refs[2 * nout + 9]
    copies = [pltpu.make_async_copy(source, target, local.at[k]) for k, (source, target) in enumerate(((s_all, sbuf), (d_all, dbuf), (c_all, cbuf)))]
    for copy in copies:
        copy.start()
    for copy in copies:
        copy.wait()
    finish_unpack(cplan, splan, outs, smalls, sbuf, dbuf, cbuf, wide, pair_buf, stages, out_sem)


def gather_weights(common_master, split_master, cplan, splan):
    s_own, c_own = align(common_master, split_master, cplan, splan)
    any_spec = pl.BlockSpec(memory_space=pl.ANY)
    vmem = pl.BlockSpec(memory_space=pltpu.VMEM)
    scratch = unpack_scratch(cplan, splan)
    scratch[2] = pltpu.VMEM((cplan.parts, cplan.rows, LANES), BF16)
    fd = first_dec(splan)
    out_specs = [any_spec] * len(OUT_NAMES) + [vmem] * 3
    limit = 64000 * 1024
    if cplan.parts == 8 and splan.parts == 8:
        copies = 60
        results = pl.pallas_call(
            functools.partial(gather_kernel, cplan, splan),
            out_shape=GATHERED, in_specs=[vmem, vmem], out_specs=out_specs,
            scratch_shapes=scratch + [pltpu.SemaphoreType.DMA((copies,)), pltpu.SemaphoreType.DMA((copies,)), pltpu.SemaphoreType.DMA((2,))],
            compiler_params=pltpu.CompilerParams(collective_id=0, has_side_effects=True, vmem_limit_bytes=limit),
            name="gather",
        )(s_own, c_own)
    else:
        y = lax.axis_index(TENSOR) // 2
        s_all = lax.all_gather(lax.all_gather(s_own, DP), TENSOR).reshape(2, 2, splan.parts, splan.rows, LANES)
        c_all = jnp.moveaxis(lax.all_gather(lax.all_gather(c_own, DP), TENSOR), 0, 1).reshape(cplan.parts, cplan.rows, LANES)
        s_mine = lax.dynamic_index_in_dim(s_all, y, 0, False)
        d_other = lax.dynamic_index_in_dim(s_all, 1 - y, 0, False)[:, fd:]
        results = pl.pallas_call(
            functools.partial(local_unpack_kernel, cplan, splan),
            out_shape=GATHERED, in_specs=[any_spec] * 3, out_specs=out_specs,
            scratch_shapes=scratch + [pltpu.SemaphoreType.DMA((3,))],
            compiler_params=pltpu.CompilerParams(vmem_limit_bytes=limit),
            name="unpack",
        )(s_mine, d_other, c_all)
    weights = Namespace(**dict(zip(OUT_NAMES, results)))
    small, bias, dbias = results[len(OUT_NAMES) :]
    at = 0
    rows = []
    for _, count in SMALLS:
        rows.append(small[at : at + count])
        at += round_up(count, 8)
    a, b, qkv_rows, head_rows = rows
    weights.embedding_bias = a[:6].reshape(1, D)
    weights.enc_norms = a[6:42].reshape(6, D)
    weights.enc_biases = a[42:54].reshape(2, D)
    weights.mask_token = b[:3].reshape(1, DD)
    weights.dec_norms = b[3:21].reshape(6, DD)
    weights.dec_biases = b[21:27].reshape(2, DD)
    weights.dec_qkv_bias = qkv_rows.reshape(2, DD)
    weights.head_bias = head_rows.reshape(1, PATCH)
    weights.enc_qkv_bias = bias[:, :3].reshape(2, 2, 192)
    weights.enc_up_bias = bias[:, 8:14].reshape(1, 1536)
    weights.dec_up_bias = dbias[:, :3].reshape(1, 1536)
    return weights


DEC_FIRST = floor16(DEC_ROW)
S_WIDE = round_up(SPLIT_ROWS, TILE)
C_WIDE = round_up(COMMON_ROWS, TILE)
D_WIDE = S_WIDE - DEC_FIRST
SLOTS = 3


def buffer_rows(plan, wide):
    return max(wide, plan.base[-1] + plan.rows)


def narrow(wide, target, count, chunk=128):
    def body(index, _):
        at = pl.ds(pl.multiple_of(index * chunk, TILE), chunk)
        target[at, :] = wide[at, :].astype(BF16)
        return 0

    whole = count // chunk
    lax.fori_loop(0, whole, body, 0)
    if count % chunk:
        target[whole * chunk : count, :] = wide[whole * chunk : count, :].astype(BF16)


def clear(wide, first, last, chunk=64):
    def body(index, _):
        wide[pl.ds(first + index * chunk, chunk), :] = jnp.zeros((chunk, LANES), F32)
        return 0

    whole = (last - first) // chunk
    lax.fori_loop(0, whole, body, 0)
    rest = (last - first) % chunk
    if rest:
        wide[pl.ds(first + whole * chunk, rest), :] = jnp.zeros((rest, LANES), F32)


def matrix_in(wide, start, per_row, stage, rows, width, j0, step=64):
    def body(index, _):
        at = index * step
        for j in range(width // LANES):
            wide[pl.ds(start + j0 + j + at * per_row, step, stride=per_row), :] = stage[
                pl.ds(pl.multiple_of(at, 8), step), j * LANES : (j + 1) * LANES
            ]
        return 0

    lax.fori_loop(0, rows // step, body, 0)


def qkv_in(wide, start, pair_buf, stage):
    step = 32
    lane = lax.broadcasted_iota(jnp.int32, (step, LANES), 1)

    def body(index, _):
        at = start + index * step * 9
        even, odd = [], []
        base = pl.multiple_of(index * 64, 8)
        for j in range(5):
            lanes = slice(j * LANES, (j + 1) * LANES) if j < 4 else slice(512, 640)
            pair_buf[j] = stage[pl.ds(base, 64), lanes]
            even.append(pair_buf[j, pl.ds(0, step, stride=2), :])
            odd.append(pltpu.roll(pair_buf[j, pl.ds(1, step, stride=2), :], 64, 1))
        for j in range(4):
            wide[pl.ds(at + j, step, stride=9), :] = even[j]
        wide[pl.ds(at + 4, step, stride=9), :] = jnp.where(lane < 64, even[4], odd[0])
        for j in range(4):
            wide[pl.ds(at + 5 + j, step, stride=9), :] = jnp.where(lane < 64, odd[j], odd[j + 1])
        return 0

    lax.fori_loop(0, 12, body, 0)


def add_rows(target, parts, count, chunk=None):
    chunk = chunk or max(c for c in (128, 64, 48, 32, 16) if count % c == 0)

    def body(index, _):
        at = index * chunk
        total = None
        for ref, start in parts:
            value = ref[pl.ds(pl.multiple_of(start + at, TILE), chunk), :].astype(F32)
            total = value if total is None else total + value
        target[pl.ds(pl.multiple_of(at, TILE), chunk), :] = total.astype(target.dtype)
        return 0

    lax.fori_loop(0, count // chunk, body, 0)


def unalign(source, target, share, offset):
    down, lanes = offset // LANES, offset % LANES
    step = 64
    lane = lax.broadcasted_iota(jnp.int32, (step, LANES), 1)
    row = lax.broadcasted_iota(jnp.int32, (step, LANES), 0)

    def body(index, total):
        at = index * step
        here = pltpu.roll(source[pl.ds(down + at, step), :], LANES - lanes, 1)
        after = pltpu.roll(source[pl.ds(down + at + 1, step), :], LANES - lanes, 1)
        value = jnp.where(lane < LANES - lanes, here, after)
        value = jnp.where((row + at) * LANES + lane < share, value, 0.0)
        target[pl.ds(pl.multiple_of(at, 8), step), :] = value
        square = (value * value).reshape(step // 8, 8, LANES)
        return total + jnp.sum(square, axis=0)

    return lax.fori_loop(0, target.shape[0] // step, body, jnp.zeros((8, LANES), F32))


def flat_rows(share):
    return round_up(-(-share // LANES), 64)


def grad_jobs(y, grads, small, bias, dbias, wide, pair_buf, gs, gd, gc):
    grad = Namespace(**dict(zip(OUT_NAMES, grads)))
    half = CROW.embedding[1] // 2

    def matrix(source, rows, width, per_row, start, j0=0):
        def place(stage):
            matrix_in(wide, start, per_row, stage, rows, width, j0)

        return (place, source, rows, width)

    def small_rows(source, start):
        def action():
            wide[pl.ds(start, source.shape[0]), :] = source[...]

        return (action,)

    def columns(slot, width):
        return pl.ds(pl.multiple_of(slot * width, LANES), width)

    def rows_of(slot, count):
        return pl.ds(pl.multiple_of(slot * count, 8), count)

    def dec_part(slot, first):
        return [
            matrix(grad.dec_up.at[:, columns(slot, 384)], DD, 384, 3, SROW.dec_up[0] - first),
            small_rows(dbias.at[slot, pl.ds(0, 3)], SROW.dec_up_bias[0] - first),
            matrix(grad.dec_down.at[rows_of(slot, 384)], 384, DD, 3, SROW.dec_down[0] - first),
            (functools.partial(clear, wide, SPLIT_ROWS - first, S_WIDE - first),)]

    def split_jobs(slot):
        return [
            (functools.partial(qkv_in, wide, SROW.enc_qkv[0], pair_buf), grad.enc_qkv.at[:, columns(slot, 640)], D, 640),
            small_rows(bias.at[slot, pl.ds(0, 3)], SROW.enc_qkv_bias[0]),
            matrix(grad.enc_proj.at[rows_of(slot, 192)], 192, D, 6, SROW.enc_proj[0]),
            matrix(grad.enc_up.at[:, columns(slot, 768)], D, 768, 6, SROW.enc_up[0]),
            small_rows(bias.at[slot, pl.ds(8, 6)], SROW.enc_up_bias[0]),
            matrix(grad.enc_down.at[rows_of(slot, 768)], 768, D, 6, SROW.enc_down[0]),
        ] + dec_part(slot, 0) + [(lambda: narrow(wide, gs.at[slot], S_WIDE),)]

    def dec_jobs(slot):
        return [(lambda: clear(wide, 0, DEC_ROW - DEC_FIRST),)] + dec_part(slot + 2, DEC_FIRST) + [(lambda: narrow(wide, gd.at[slot], D_WIDE),)]

    def clear_other():
        def body(index, _):
            wide[pl.ds((1 - y) * half + index * 64, 64), :] = jnp.zeros((64, LANES), F32)
            return 0

        lax.fori_loop(0, half // 64, body, 0)
        clear(wide, COMMON_ROWS, C_WIDE)

    common = [(clear_other,), matrix(grad.embedding, 768, D, 6, y * half)]
    at = 0
    for start, count in SMALLS:
        common.append(small_rows(small.at[pl.ds(at, count)], start))
        at += round_up(count, 8)
    for name in CMATS[1:]:
        rows, total = vars(OUTS)[name]
        for col in range(0, total, 768):
            width = min(768, total - col)
            common.append(matrix(vars(grad)[name].at[:, pl.ds(col, width)], rows, width, total // LANES, vars(CROW)[name][0], col // LANES))
    common.append((lambda: narrow(wide, gc, C_WIDE),))
    return split_jobs, dec_jobs, common


def run_jobs(jobs, stage, stage_sem):
    loads = [job for job in jobs if len(job) > 1]
    copies = [
        pltpu.make_async_copy(job[1], stage.at[n % SLOTS, pl.ds(0, job[2]), pl.ds(0, job[3])], stage_sem.at[n % SLOTS]) for n, job in enumerate(loads)]
    for copy in copies[: SLOTS - 1]:
        copy.start()
    index = 0
    for job in jobs:
        if len(job) == 1:
            job[0]()
            continue
        if index + SLOTS - 1 < len(copies):
            copies[index + SLOTS - 1].start()
        copies[index].wait()
        job[0](stage.at[index % SLOTS])
        index += 1


ZORDER = (0, 3, 1, 2)
SUBS = 4


def reduce_kernel(cplan, splan, *refs):
    nin = len(OUT_NAMES)
    grads, (small, bias, dbias, loss) = refs[:nin], refs[nin : nin + 4]
    g_split, g_common, sums = refs[nin + 4 : nin + 7]
    (wide, pair_buf, stage, gs, gd, gc, ks, xs, zs, kc, yc, xc, zc, kd, yd, cq, fin, finc, part, stage_sem, send, recv) = refs[nin + 7 :]
    me, t = lax.axis_index(DP), lax.axis_index(TENSOR)
    z, x, y, c = me // 2, me % 2, t // 2, t % 2
    rank = me * 4 + t
    srows, quarter = splan.rows, cplan.rows // 4
    sub = srows // SUBS
    updev, downdev = {DP: (z + 1) % 4 * 2 + x, TENSOR: t}, {DP: (z + 3) % 4 * 2 + x, TENSOR: t}
    xdev, ydev, kdev = {DP: z * 2 + (1 - x), TENSOR: t}, {DP: me, TENSOR: (1 - y) * 2 + c}, {DP: me, TENSOR: y * 2 + (1 - c)}
    others = [(rank + k) % 32 for k in range(1, 32)]
    devices = [{DP: other // 4, TENSOR: other % 4} for other in others]
    barrier = pltpu.get_barrier_semaphore()
    for device in devices:
        pl.semaphore_signal(barrier, inc=1, device_id=device, device_id_type=MESH)

    def remote(source, target, slot, device):
        return pltpu.make_async_remote_copy(
            src_ref=source, dst_ref=target, send_sem=send.at[slot], recv_sem=recv.at[slot], device_id=device, device_id_type=MESH)

    def s_at(i):
        return pl.multiple_of(i * splan.share // BLOCK * TILE, TILE)

    def c_at(i, tt):
        return pl.multiple_of(i * cplan.share // BLOCK * TILE + tt * quarter, TILE)

    def piece(q):
        return pl.ds(pl.multiple_of(q * sub, TILE), sub)

    def kd_copy():
        return remote(gd.at[1 - c], kd, 0, kdev)

    def ks_copy(i):
        return remote(gs.at[1 - c, pl.ds(s_at(i), srows)], ks.at[i], 1 + i, kdev)

    def kc_copy(i, yy):
        return remote(gc.at[pl.ds(c_at(i, 2 * yy + 1 - c), quarter)], kc.at[i, yy], 9 + i * 2 + yy, kdev)

    def yd_copy():
        return remote(kd, yd, 25, ydev)

    def yc_copy(i):
        return remote(kc.at[i, 1 - y], yc.at[i], 26 + i, ydev)

    def xs_copy(zz, q):
        return remote(ks.at[zz * 2 + (1 - x), piece(q)], xs.at[zz, piece(q)], 34 + zz * 4 + q, xdev)

    def xc_copy(zz):
        return remote(yc.at[zz * 2 + (1 - x)], xc.at[zz], 50 + zz, xdev)

    def zs_copy(down, zz, q):
        return remote(xs.at[zz, piece(q)], zs.at[down, zz, piece(q)], 54 + down * 16 + zz * 4 + q, downdev if down else updev)

    def zc_copy(down, zz):
        return remote(xc.at[zz], zc.at[down, zz], 86 + down * 4 + zz, downdev if down else updev)

    def along_z(zz, copy_of, add):
        for down in (0, 1):
            passes = z > zz if down else z < zz
            first = z == 3 if down else z == 0

            @pl.when(jnp.logical_and(passes, first))
            def _():
                add(None)

            @pl.when(jnp.logical_and(passes, jnp.logical_not(first)))
            def _(down=down):
                copy_of(down).wait_recv()
                add(down)

            @pl.when(passes)
            def _(down=down):
                copy_of(down).start()

    def across_x(zz):
        i = zz * 2 + (1 - x)
        ks_copy(i).wait_recv()

        def body(q, _):
            add_rows(ks.at[i, piece(q)], [(ks.at[i, piece(q)], 0), (gs.at[c], s_at(i) + q * sub)], sub)
            xs_copy(zz, q).start()
            return 0

        lax.fori_loop(0, SUBS, body, 0)

    def first_sends():
        pl.semaphore_wait(barrier, 31)
        kd_copy().start()

    def core_sends():
        for zz in ZORDER:
            ks_copy(zz * 2 + (1 - x)).start()
        for zz in ZORDER:
            ks_copy(zz * 2 + x).start()

    def dec_across():
        kd_copy().wait_recv()
        add_rows(kd, [(gd.at[c], 0), (kd, 0)], D_WIDE)
        yd_copy().start()

    def common_core_sends():
        for zz in ZORDER:
            for xx in (0, 1):
                for yy in (0, 1):
                    kc_copy(zz * 2 + xx, yy).start()

    split_jobs, dec_jobs, common_jobs = grad_jobs(y, grads, small, bias, dbias, wide, pair_buf, gs, gd, gc)
    run_jobs(
        dec_jobs(1 - c) + [(first_sends,)] + dec_jobs(c) + split_jobs(1 - c) + [(core_sends,), (dec_across,)] + split_jobs(c)
        + [(functools.partial(across_x, ZORDER[0]),)] + common_jobs + [(common_core_sends,)], stage, stage_sem)
    yd_copy().wait_recv()
    dec_rows = gs.at[c, pl.ds(DEC_FIRST, D_WIDE)]
    add_rows(dec_rows, [(dec_rows, 0), (yd, 0)], D_WIDE)
    for zz in ZORDER[1:]:
        across_x(zz)
    for zz in ZORDER:
        for xx in (0, 1):
            i = zz * 2 + xx
            for yy in (0, 1):
                kc_copy(i, yy).wait_recv()
            add_rows(kc.at[i, 1 - y], [(gc, c_at(i, 2 * (1 - y) + c)), (kc.at[i, 1 - y], 0)], quarter)
            yc_copy(i).start()
    for zz in ZORDER:
        i = zz * 2 + (1 - x)
        yc_copy(i).wait_recv()
        add_rows(yc.at[i], [(gc, c_at(i, t)), (kc.at[i, y], 0), (yc.at[i], 0)], quarter)
        xc_copy(zz).start()
        i = zz * 2 + x
        ks_copy(i).wait_recv()

        def body(q, _, zz=zz, i=i):
            xs_copy(zz, q).wait_recv()

            def add(flow):
                parts = [(xs.at[zz, piece(q)], 0), (gs.at[c], s_at(i) + q * sub), (ks.at[i, piece(q)], 0)]
                add_rows(xs.at[zz, piece(q)], parts + ([] if flow is None else [(zs.at[flow, zz, piece(q)], 0)]), sub)

            along_z(zz, lambda down: zs_copy(down, zz, q), add)
            return 0

        lax.fori_loop(0, SUBS, body, 0)
    for zz in ZORDER:
        i = zz * 2 + x
        yc_copy(i).wait_recv()
        xc_copy(zz).wait_recv()

        def add_common(flow, zz=zz, i=i):
            parts = [(xc.at[zz], 0), (gc, c_at(i, t)), (kc.at[i, y], 0), (yc.at[i], 0)]
            add_rows(xc.at[zz], parts + ([] if flow is None else [(zc.at[flow, zz], 0)]), quarter)

        along_z(zz, lambda down, zz=zz: zc_copy(down, zz), add_common)

    def ends(copy_of, action):
        for low, high in ((0, 1), (1, 1), (1, 0)):
            here = jnp.logical_and((z > 0) == bool(low), (z < 3) == bool(high))

            @pl.when(here)
            def _(low=low, high=high):
                flows = [0] * low + [1] * high
                for flow in flows:
                    copy_of(flow)
                action(flows)

    mine = pl.ds(pl.multiple_of(t * quarter, TILE), quarter)
    ends(
        lambda flow: zc_copy(flow, z).wait_recv(),
        lambda flows: add_rows(
            cq.at[mine], [(xc.at[z], 0), (gc, c_at(me, t)), (kc.at[me, y], 0), (yc.at[me], 0)] + [(zc.at[flow, z], 0) for flow in flows], quarter))
    far = pl.ds(pl.multiple_of(((1 - y) * 2 + c) * quarter, TILE), quarter)
    across_t, beside_t, beside_far = remote(cq.at[mine], cq.at[mine], 94, ydev), remote(cq.at[mine], cq.at[mine], 95, kdev), remote(cq.at[far], cq.at[far], 96, kdev)
    across_t.start()
    beside_t.start()

    def wait_split(flow):
        for q in range(SUBS):
            zs_copy(flow, z, q).wait_recv()

    ends(
        wait_split,
        lambda flows: add_rows(fin, [(xs.at[z], 0), (gs.at[c], s_at(me)), (ks.at[me], 0)] + [(zs.at[flow, z], 0) for flow in flows], srows))
    across_t.wait_recv()
    beside_far.start()
    squares = unalign(fin, g_split, splan.share, me * splan.share % BLOCK)
    beside_t.wait_recv()
    beside_far.wait_recv()
    add_rows(finc, [(cq, 0)], cplan.rows)
    squares += unalign(finc, g_common, cplan.share, me * cplan.share % BLOCK) * 0.25
    part[rank, 0:8, :] = squares
    part[rank, 8:16, :] = loss[...]
    shared = [remote(part.at[rank], part.at[rank], 97 + k, device) for k, device in enumerate(devices)]
    for copy in shared:
        copy.start()
    kd_copy().wait_send()
    yd_copy().wait_send()
    for i in range(8):
        ks_copy(i).wait_send()
        yc_copy(i).wait_send()
        for yy in range(2):
            kc_copy(i, yy).wait_send()
    for zz in range(4):
        xc_copy(zz).wait_send()
        for q in range(SUBS):
            xs_copy(zz, q).wait_send()
        for down in (0, 1):
            @pl.when(z > zz if down else z < zz)
            def _(down=down, zz=zz):
                zc_copy(down, zz).wait_send()
                for q in range(SUBS):
                    zs_copy(down, zz, q).wait_send()
    for copy in (across_t, beside_t, beside_far):
        copy.wait_send()
    for copy in shared:
        copy.wait_recv()

    def total(index, value):
        return value + part[index]

    sums[...] = lax.fori_loop(0, 32, total, jnp.zeros((16, LANES), F32))
    for copy in shared:
        copy.wait_send()


def pack_kernel(*refs):
    nin = len(OUT_NAMES)
    grads, (small, bias, dbias) = refs[:nin], refs[nin : nin + 3]
    gs_out, gd_out, gc_out = refs[nin + 3 : nin + 6]
    wide, pair_buf, stage, gs, gd, gc, stage_sem, out_sem = refs[nin + 6 :]
    split_jobs, dec_jobs, common_jobs = grad_jobs(lax.axis_index(TENSOR) // 2, grads, small, bias, dbias, wide, pair_buf, gs, gd, gc)
    run_jobs(dec_jobs(0) + dec_jobs(1) + split_jobs(0) + split_jobs(1) + common_jobs, stage, stage_sem)
    copies = [pltpu.make_async_copy(a, b, out_sem.at[k]) for k, (a, b) in enumerate(((gs, gs_out), (gd, gd_out), (gc, gc_out)))]
    for copy in copies:
        copy.start()
    for copy in copies:
        copy.wait()


def unalign_kernel(share_s, share_c, scalars, s_in, c_in, s_out, c_out, sums):
    sums[...] = unalign(s_in, s_out, share_s, scalars[0]) + unalign(c_in, c_out, share_c, scalars[1]) * 0.25


def reduce_grads(grads, small, bias, dbias, loss, cplan, splan):
    any_spec, vmem = pl.BlockSpec(memory_space=pl.ANY), pl.BlockSpec(memory_space=pltpu.VMEM)
    srows, quarter = splan.rows, cplan.rows // 4
    gs_rows, gc_rows = buffer_rows(splan, S_WIDE), buffer_rows(cplan, C_WIDE)
    flat = (jax.ShapeDtypeStruct((flat_rows(splan.share), LANES), F32), jax.ShapeDtypeStruct((flat_rows(cplan.share), LANES), F32))
    packing = [
        pltpu.VMEM((C_WIDE, LANES), F32), pltpu.VMEM((5, 64, LANES), F32), pltpu.VMEM((SLOTS, 768, 768), F32),
        pltpu.VMEM((2, gs_rows, LANES), BF16), pltpu.VMEM((2, D_WIDE, LANES), BF16), pltpu.VMEM((gc_rows, LANES), BF16)]
    operands = [vars(grads)[name] for name in OUT_NAMES]
    limit = 67_000_000
    if cplan.parts == 8 and splan.parts == 8:
        def rows(*shape, kind=BF16):
            return pltpu.VMEM(shape + (LANES,), kind)

        copies = 128
        return pl.pallas_call(
            functools.partial(reduce_kernel, cplan, splan),
            out_shape=flat + (jax.ShapeDtypeStruct((16, LANES), F32),),
            in_specs=[any_spec] * len(operands) + [vmem] * 4, out_specs=[vmem] * 3,
            scratch_shapes=packing + [
                rows(8, srows), rows(4, srows), rows(2, 4, srows), rows(8, 2, quarter), rows(8, quarter), rows(4, quarter), rows(2, 4, quarter),
                rows(D_WIDE), rows(D_WIDE), rows(cplan.rows),
                rows(srows + 64, kind=F32), rows(cplan.rows + 64, kind=F32), rows(32, 16, kind=F32),
                pltpu.SemaphoreType.DMA((SLOTS,)), pltpu.SemaphoreType.DMA((copies,)), pltpu.SemaphoreType.DMA((copies,))],
            compiler_params=pltpu.CompilerParams(collective_id=1, has_side_effects=True, vmem_limit_bytes=limit),
            name="reduce",
        )(*operands, small, bias, dbias, loss)
    shapes = [jax.ShapeDtypeStruct((2, gs_rows, LANES), BF16), jax.ShapeDtypeStruct((2, D_WIDE, LANES), BF16), jax.ShapeDtypeStruct((gc_rows, LANES), BF16)]
    gs, gd, gc = pl.pallas_call(
        pack_kernel, out_shape=shapes, in_specs=[any_spec] * len(operands) + [vmem] * 3, out_specs=[any_spec] * 3,
        scratch_shapes=packing + [pltpu.SemaphoreType.DMA((SLOTS,)), pltpu.SemaphoreType.DMA((3,))],
        compiler_params=pltpu.CompilerParams(vmem_limit_bytes=limit), name="pack",
    )(*operands, small, bias, dbias)
    me, t = lax.axis_index(DP), lax.axis_index(TENSOR)
    c = t % 2

    def swap(value, bit):
        return lax.ppermute(value, TENSOR, [(i, i ^ bit) for i in range(4)])

    def mine(value):
        keep = lax.dynamic_index_in_dim(value, c, 0, False).astype(F32)
        return keep + swap(lax.dynamic_index_in_dim(value, 1 - c, 0, False), 1).astype(F32)

    far = swap(mine(gd).astype(BF16), 2)
    split_sum = mine(gs).at[DEC_FIRST : DEC_FIRST + D_WIDE].add(far.astype(F32))
    common_sum = lax.psum(gc, TENSOR).astype(F32)

    def scattered(value, plan):
        frames = jnp.stack([value[base : base + plan.rows] for base in plan.base])
        return lax.psum_scatter(frames.astype(BF16), DP, scatter_dimension=0, tiled=True)[0].astype(F32)

    s_frame, c_frame = scattered(split_sum, splan), scattered(common_sum, cplan)
    pad = ((0, 64), (0, 0))
    g_split, g_common, squares = pl.pallas_call(
        functools.partial(unalign_kernel, splan.share, cplan.share), out_shape=flat + (jax.ShapeDtypeStruct((8, LANES), F32),),
        in_specs=[pl.BlockSpec(memory_space=pltpu.SMEM), vmem, vmem], out_specs=[vmem] * 3, name="unalign",
    )(jnp.stack([me * splan.share % BLOCK, me * cplan.share % BLOCK]).astype(jnp.int32), jnp.pad(s_frame, pad), jnp.pad(c_frame, pad))
    return g_split, g_common, lax.psum(jnp.concatenate([squares, loss]), (DP, TENSOR))


QROWS = 208
QBLOCKS = 4
OWN = TUBES // 2
SCALE = HEAD ** (-0.5)


def nt(a, b):
    return lax.dot_general(a, b, (((1,), (1,)), ((), ())), preferred_element_type=F32)


def nn(a, b):
    return lax.dot_general(a, b, (((1,), (0,)), ((), ())), preferred_element_type=F32)


def head_masks(rows):
    lane = lax.broadcasted_iota(jnp.int32, (rows, LANES), 1)
    return lane < HEAD, lane >= HEAD


def attend_kernel(q_ref, k_ref, vt_ref, o_ref, lse_ref):
    q, k = q_ref[...], k_ref[...]
    pieces = []
    for head, mask in enumerate(head_masks(QROWS)):
        scores = nt(k, jnp.where(mask, q, jnp.zeros_like(q)))
        top = jnp.max(scores, axis=0, keepdims=True)
        shifted = jnp.exp((scores - top) * SCALE)
        total = jnp.sum(shifted, axis=0, keepdims=True)
        value = nn(vt_ref[head * HEAD : (head + 1) * HEAD, :], shifted.astype(BF16))
        pieces.append(value / total)
        lse_ref[0, 0, head : head + 1, :] = top * SCALE + jnp.log(total)
    o_ref[...] = jnp.concatenate(pieces, axis=0).T


def attend(q, k, vt):
    return pl.pallas_call(
        attend_kernel, grid=(3, QBLOCKS),
        out_shape=(jax.ShapeDtypeStruct((QROWS * QBLOCKS, DD), F32), jax.ShapeDtypeStruct((3, QBLOCKS, 8, QROWS), F32)),
        in_specs=[
            pl.BlockSpec((QROWS, LANES), lambda h, i: (i, h)), pl.BlockSpec((TUBES, LANES), lambda h, i: (0, h)),
            pl.BlockSpec((LANES, TUBES), lambda h, i: (h, 0))],
        out_specs=[pl.BlockSpec((QROWS, LANES), lambda h, i: (i, h)), pl.BlockSpec((1, 1, 8, QROWS), lambda h, i: (h, i, 0, 0))],
        name="attend",
    )(q, k, vt)


def attend_back_kernel(q_ref, k_ref, v_ref, kt_ref, do_ref, o_ref, lse_ref, dq_ref, dk_ref, dv_ref):
    @pl.when(pl.program_id(1) == 0)
    def _():
        dk_ref[...] = jnp.zeros_like(dk_ref)
        dv_ref[...] = jnp.zeros_like(dv_ref)

    q, do, k, v = q_ref[...], do_ref[...], k_ref[...], v_ref[...]
    along = (do.astype(F32) * o_ref[...]).T
    pieces, dk, dv = [], None, None
    for head, mask in enumerate(head_masks(QROWS)):
        qm, dom = jnp.where(mask, q, jnp.zeros_like(q)), jnp.where(mask, do, jnp.zeros_like(do))
        delta = jnp.sum(along[head * HEAD : (head + 1) * HEAD], axis=0, keepdims=True)
        probs = jnp.exp(nt(k, qm) * SCALE - lse_ref[0, 0, head : head + 1, :])
        value = nn(probs.astype(BF16), dom)
        dv = value if dv is None else dv + value
        ds = (probs * (nt(v, dom) - delta)).astype(BF16)
        key = nn(ds, qm)
        dk = key if dk is None else dk + key
        pieces.append(nn(kt_ref[head * HEAD : (head + 1) * HEAD, :], ds))
    dq_ref[...] = (jnp.concatenate(pieces, axis=0) * SCALE).T.astype(BF16)
    dk_ref[...] += dk * SCALE
    dv_ref[...] += dv


def attend_back(q, k, v, kt, do, o, lse):
    block = pl.BlockSpec((QROWS, LANES), lambda h, i: (i, h))
    whole = pl.BlockSpec((TUBES, LANES), lambda h, i: (0, h))
    return pl.pallas_call(
        attend_back_kernel, grid=(3, QBLOCKS),
        out_shape=(jax.ShapeDtypeStruct((QROWS * QBLOCKS, DD), BF16), jax.ShapeDtypeStruct((TUBES, DD), F32), jax.ShapeDtypeStruct((TUBES, DD), F32)),
        in_specs=[block, whole, whole, pl.BlockSpec((LANES, TUBES), lambda h, i: (h, 0)), block, block, pl.BlockSpec((1, 1, 8, QROWS), lambda h, i: (h, i, 0, 0))],
        out_specs=[block, whole, whole],
        name="attend_back",
    )(q, k, v, kt, do, o, lse)


NORM_EPS = 1e-06
PIXEL_EPS = 1e-06
CLIP_RATIO = 1.5
BETA_FIRST = 0.9
BETA_SECOND = 0.95
LEARN_RATE = 0.05
DECAY_RATE = 0.05
ADAM_EPS = 1e-08


def layer_norm(inputs, gain, shift):
    centered = inputs - jnp.mean(inputs, axis=-1, keepdims=True)
    spread = jnp.mean(centered * centered, axis=-1, keepdims=True)
    return centered * lax.rsqrt(spread + NORM_EPS) * gain + shift


def norm_back(inputs, gain, grad):
    centered = inputs - jnp.mean(inputs, axis=-1, keepdims=True)
    scale = lax.rsqrt(jnp.mean(centered * centered, axis=-1, keepdims=True) + NORM_EPS)
    unit = centered * scale
    inner = grad * gain
    back = scale * (inner - jnp.mean(inner, axis=-1, keepdims=True) - unit * jnp.mean(inner * unit, axis=-1, keepdims=True))
    return back, jnp.sum(grad * unit, axis=0), jnp.sum(grad, axis=0)


def tn(a, b):
    return lax.dot_general(a, b, (((0,), (0,)), ((), ())), preferred_element_type=F32)


def gelu(inputs):
    return jax.nn.gelu(inputs, approximate=False)


def gelu_slope(inputs):
    return 0.5 * (1.0 + lax.erf(inputs * math.sqrt(0.5))) + inputs * jnp.exp(-0.5 * inputs * inputs) * (1.0 / math.sqrt(2.0 * math.pi))


def sine_rows(position, width):
    column = jnp.arange(width)
    exponent = (2 * (column // 2)).astype(F32) / width
    angles = position.astype(F32)[:, None] / jnp.power(10000.0, exponent)[None, :]
    return jnp.where((column % 2 == 0)[None, :], jnp.sin(angles), jnp.cos(angles))


def sine_table(width, step=32):
    column = np.arange(width)
    rate = 10000.0 ** (-(2 * (column // 2)) / width)
    high, low = np.arange(0, TUBES, step)[:, None] * rate, np.arange(step)[:, None] * rate
    even = column % 2 == 0
    a = np.where(even, np.sin(high), np.cos(high)).astype(np.float32)
    b = np.where(even, np.cos(high), -np.sin(high)).astype(np.float32)
    c, s = np.cos(low).astype(np.float32), np.sin(low).astype(np.float32)
    table = a[:, None] * jnp.asarray(c)[None] + b[:, None] * jnp.asarray(s)[None]
    return table.reshape(TUBES, width)


def across(value):
    return lax.ppermute(value, TENSOR, [(i, i ^ 2) for i in range(4)])


def beside(value):
    return lax.ppermute(value, TENSOR, [(i, i ^ 1) for i in range(4)])


def y_total(partial):
    low = partial.astype(BF16)
    return low.astype(F32) + across(low).astype(F32)


def heads_of(mixed):
    parts = mixed.reshape(VIS, 2, 3, 3, HEAD)
    return [parts[:, :, k].transpose(1, 2, 0, 3).reshape(6, VIS, HEAD) for k in range(3)]


def heads_back(parts):
    stacked = jnp.stack([part.reshape(2, 3, VIS, HEAD) for part in parts], axis=1)
    return stacked.transpose(3, 0, 1, 2, 4).reshape(VIS, 1152)


def step_grads(pixels, order, w, scale_back):
    t = lax.axis_index(TENSOR)
    y, c = t // 2, t % 2
    first_y = (y == 0).astype(F32)
    seen = lax.dynamic_index_in_dim(order, c, 0, False)[:VIS]
    seen_y = lax.dynamic_index_in_dim(order, y, 0, False)[:VIS]
    rows = pixels.reshape(2 * TUBES, PATCH)
    seen_pixels = jnp.take(rows, c * TUBES + seen, axis=0)
    embedded = nn(seen_pixels, w.embedding) + w.embedding_bias + sine_rows(seen, D)
    norms, biases = w.enc_norms, w.enc_biases
    normed_a = layer_norm(embedded, norms[0], norms[1]).astype(BF16)
    qkv_w = jnp.concatenate([w.enc_qkv[0], w.enc_qkv[1]], axis=1)
    zero = jnp.zeros((192,), F32)
    qkv_b = jnp.concatenate([piece for k in range(2) for piece in (w.enc_qkv_bias[k, 0], zero, w.enc_qkv_bias[k, 1])])
    q, k, v = heads_of((nn(normed_a, qkv_w) + qkv_b).astype(BF16))
    scores = jnp.einsum("hqe,hke->hqk", q, k, preferred_element_type=F32) * SCALE
    probs = jax.nn.softmax(scores, axis=-1)
    probs_low = probs.astype(BF16)
    out = jnp.einsum("hqk,hke->hqe", probs_low, v, preferred_element_type=F32).astype(BF16)
    merged = out.transpose(1, 0, 2).reshape(VIS, 384)
    after = embedded + (y_total(nn(merged, w.enc_proj)) + biases[0])
    normed_m = layer_norm(after, norms[2], norms[3]).astype(BF16)
    raised = nn(normed_m, w.enc_up) + w.enc_up_bias
    active = gelu(raised).astype(BF16)
    encoded = after + (y_total(nn(active, w.enc_down)) + biases[1])
    final_low = layer_norm(encoded, norms[4], norms[5]).astype(BF16)
    moved = lax.ppermute(final_low, TENSOR, [(0, 1), (3, 2)])
    mine = jnp.where(y == c, final_low, moved)
    lowered = nn(mine, w.to_decoder)
    select = seen_y[None, :] == jnp.arange(TUBES, dtype=jnp.int32)[:, None]
    visible = jnp.any(select, axis=1, keepdims=True)
    placed = lax.dot_general(select.astype(F32), lowered, (((1,), (0,)), ((), ())), precision=lax.Precision.HIGHEST, preferred_element_type=F32)
    dec_in = placed + jnp.where(visible, 0.0, w.mask_token) + sine_table(DD)
    start = c * OWN

    def own(value):
        return lax.dynamic_slice_in_dim(value, start, OWN, 0)

    dnorms, dbiases = w.dec_norms, w.dec_biases
    normed_all = layer_norm(dec_in, dnorms[0], dnorms[1]).astype(BF16)
    normed_q = own(normed_all)
    dec_own = own(dec_in)
    query = (nn(normed_q, w.dec_qkv[:, :DD]) + w.dec_qkv_bias[0]).astype(BF16)
    key = nn(normed_all, w.dec_qkv[:, DD : 2 * DD]).astype(BF16)
    value = (nn(normed_all, w.dec_qkv[:, 2 * DD :]) + w.dec_qkv_bias[1]).astype(BF16)
    pad = ((0, QROWS * QBLOCKS - OWN), (0, 0))
    query = jnp.pad(query, pad)
    attended, lse = attend(query, key, value.T)
    attended_low = attended[:OWN].astype(BF16)
    mid = dec_own + (nn(attended_low, w.dec_proj) + dbiases[0])
    normed_d = layer_norm(mid, dnorms[2], dnorms[3]).astype(BF16)
    draised = nn(normed_d, w.dec_up) + w.dec_up_bias
    dactive = gelu(draised).astype(BF16)
    decoded = mid + (nn(dactive, w.dec_down) + dbiases[1])
    head_low = layer_norm(decoded, dnorms[4], dnorms[5]).astype(BF16)
    predicted = nn(head_low, w.pixel_head) + w.head_bias
    target = lax.dynamic_slice_in_dim(rows, y * TUBES + start, OWN, 0).astype(F32)
    target = target - jnp.mean(target, axis=-1, keepdims=True)
    target = target * lax.rsqrt(jnp.mean(target * target, axis=-1, keepdims=True) + PIXEL_EPS)
    hidden = 1.0 - own(visible.astype(F32))
    missing = (predicted - target) * hidden
    loss = jnp.sum((missing * missing).reshape(-1, 8, PATCH // LANES, LANES), axis=(0, 2))
    pred_grad = (2.0 * scale_back * missing).astype(BF16)
    grads, small = Namespace(), Namespace()
    grads.pixel_head = tn(head_low, pred_grad)
    small.head_bias = jnp.sum(pred_grad, axis=0, dtype=F32)
    decoded_grad, dg4, dg5 = norm_back(decoded, dnorms[4], nt(pred_grad, w.pixel_head))
    branch = decoded_grad.astype(BF16)
    grads.dec_down = tn(dactive, branch)
    db1 = jnp.sum(branch, axis=0, dtype=F32)
    draised_grad = (nt(branch, w.dec_down) * gelu_slope(draised)).astype(BF16)
    grads.dec_up = tn(normed_d, draised_grad)
    dec_up_bias = jnp.sum(draised_grad, axis=0, dtype=F32)
    back, dg2, dg3 = norm_back(mid, dnorms[2], nt(draised_grad, w.dec_up))
    mid_grad = decoded_grad + back
    branch = mid_grad.astype(BF16)
    grads.dec_proj = tn(attended_low, branch)
    db0 = jnp.sum(branch, axis=0, dtype=F32)
    attended_grad = jnp.pad(nt(branch, w.dec_proj).astype(BF16), pad)
    query_grad, key_grad, value_grad = attend_back(query, key, value, key.T, attended_grad, attended, lse)

    def shared(total):
        keep = lax.dynamic_slice_in_dim(total, start, OWN, 0)
        give = lax.dynamic_slice_in_dim(total, OWN - start, OWN, 0).astype(BF16)
        return (keep + beside(give).astype(F32)).astype(BF16)

    mixed = jnp.concatenate([query_grad[:OWN], shared(key_grad), shared(value_grad)], axis=1)
    grads.dec_qkv = tn(normed_q, mixed)
    dqb = jnp.sum(mixed, axis=0, dtype=F32)
    small.dec_qkv_bias = jnp.concatenate([dqb[:DD], dqb[2 * DD :]])
    back, dg0, dg1 = norm_back(dec_own, dnorms[0], nt(mixed, w.dec_qkv))
    in_grad = mid_grad + back
    small.mask_token = jnp.sum(in_grad * hidden, axis=0)
    part = tn(own(select).astype(BF16), in_grad.astype(BF16)).astype(BF16)
    near = lax.ppermute(part, TENSOR, [(1, 0), (2, 3)])
    joined = part + near
    far = lax.ppermute(joined, TENSOR, [(0, 2), (3, 1)])
    lowered_grad = jnp.where(y == c, joined, far)
    grads.to_decoder = tn(final_low, lowered_grad) * first_y
    encoded_grad, eg4, eg5 = norm_back(encoded, norms[4], nt(lowered_grad, w.to_decoder))
    branch = encoded_grad.astype(BF16)
    grads.enc_down = tn(active, branch)
    eb1 = jnp.sum(branch, axis=0, dtype=F32)
    raised_grad = (nt(branch, w.enc_down) * gelu_slope(raised)).astype(BF16)
    grads.enc_up = tn(normed_m, raised_grad)
    enc_up_bias = jnp.sum(raised_grad, axis=0, dtype=F32)
    back, eg2, eg3 = norm_back(after, norms[2], y_total(nt(raised_grad, w.enc_up)))
    after_grad = encoded_grad + back
    branch = after_grad.astype(BF16)
    grads.enc_proj = tn(merged, branch)
    eb0 = jnp.sum(branch, axis=0, dtype=F32)
    merged_grad = nt(branch, w.enc_proj).astype(BF16).reshape(VIS, 6, HEAD).transpose(1, 0, 2)
    v_grad = jnp.einsum("hqk,hqe->hke", probs_low, merged_grad, preferred_element_type=F32).astype(BF16)
    probs_grad = jnp.einsum("hqe,hke->hqk", merged_grad, v, preferred_element_type=F32)
    scores_low = (probs * (probs_grad - jnp.sum(probs_grad * probs, axis=-1, keepdims=True))).astype(BF16)
    q_grad = (jnp.einsum("hqk,hke->hqe", scores_low, k, preferred_element_type=F32) * SCALE).astype(BF16)
    k_grad = (jnp.einsum("hqk,hqe->hke", scores_low, q, preferred_element_type=F32) * SCALE).astype(BF16)
    emixed = heads_back([q_grad, k_grad, v_grad])
    wide_mixed = jnp.pad(emixed.reshape(VIS, 2, 576), ((0, 0), (0, 0), (0, 64))).reshape(VIS, 1280)
    grads.enc_qkv = tn(normed_a, wide_mixed)
    eqb = jnp.sum(emixed, axis=0, dtype=F32).reshape(2, 3, 192)
    back, eg0, eg1 = norm_back(embedded, norms[0], y_total(nt(emixed, qkv_w)))
    embedded_low = (after_grad + back).astype(BF16)
    grads.embedding = tn(lax.dynamic_slice_in_dim(seen_pixels, y * 768, 768, 1), embedded_low)
    embedding_bias = jnp.sum(embedded_low, axis=0, dtype=F32)
    small_a = jnp.concatenate([embedding_bias, eg0, eg1, eg2, eg3, eg4, eg5, eb0, eb1]) * first_y
    small_b = jnp.concatenate([small.mask_token, dg0, dg1, dg2, dg3, dg4, dg5, db0, db1])
    tiles = []
    for piece in (small_a, small_b, small.dec_qkv_bias, small.head_bias):
        count = piece.shape[0] // LANES
        tiles.append(jnp.pad(piece.reshape(count, LANES), ((0, -count % 8), (0, 0))))
    bias = jnp.concatenate(
        [jnp.pad(eqb[:, ::2].reshape(2, 3, LANES), ((0, 0), (0, 5), (0, 0))), jnp.pad(enc_up_bias.reshape(2, 6, LANES), ((0, 0), (0, 2), (0, 0)))], axis=1)
    dbias = jnp.pad(dec_up_bias.reshape(4, 3, LANES), ((0, 0), (0, 5), (0, 0)))
    return loss, grads, jnp.concatenate(tiles), bias, dbias


def adamw(master, first, second, gradient):
    first_new = BETA_FIRST * first + (1.0 - BETA_FIRST) * gradient
    second_new = BETA_SECOND * second + (1.0 - BETA_SECOND) * gradient * gradient
    first_hat = first_new / (1.0 - BETA_FIRST**STEP)
    second_hat = second_new / (1.0 - BETA_SECOND**STEP)
    master_new = master - LEARN_RATE * (first_hat / (jnp.sqrt(second_hat) + ADAM_EPS) + DECAY_RATE * master)
    return (master_new, first_new, second_new, master_new.astype(BF16))


def shards(tubes, tube_order, common_master, common_first, common_second, split_master, split_first, split_second):
    groups = lax.axis_size(DP)
    cplan = Plan(groups, common_master.shape[0], 64)
    splan = Plan(groups, split_master.shape[1], TILE)
    masked_total = tubes.shape[0] * groups * (TUBES - VIS)
    pixel_count = masked_total * PATCH
    w = gather_weights(common_master, split_master, cplan, splan)
    loss, grads, small, bias, dbias = step_grads(tubes, tube_order, w, 1.0 / pixel_count)
    g_split, g_common, sums = reduce_grads(grads, small, bias, dbias, loss, cplan, splan)
    loss_mean = jnp.sum(sums[8:]) / pixel_count
    grad_norm = jnp.sqrt(jnp.sum(sums[:8]))
    factor = jnp.minimum(1.0, CLIP_RATIO / math.sqrt(masked_total) / (grad_norm + 1e-06))
    common = adamw(common_master, common_first, common_second, g_common.reshape(-1)[: common_master.shape[0]] * factor)
    split = adamw(split_master, split_first, split_second, g_split.reshape(1, -1)[:, : split_master.shape[1]] * factor)
    return (loss_mean.reshape(1), grad_norm.reshape(1)) + common + split


def solution(mesh):
    in_specs = (P(DP, None, None), P(DP, None), P(DP), P(DP), P(DP), P(TENSOR, DP), P(TENSOR, DP), P(TENSOR, DP))
    out_specs = (P(), P()) + (P(DP),) * 4 + (P(TENSOR, DP),) * 4
    return jax.shard_map(shards, mesh=mesh, in_specs=in_specs, out_specs=out_specs, check_vma=False)
```

```python
import functools
import math
from types import SimpleNamespace as Namespace

import jax
import jax.numpy as jnp
import numpy as np
from jax import lax
from jax.experimental import pallas as pl
from jax.experimental.pallas import tpu as pltpu
from jax.sharding import PartitionSpec as P

DP = "dp"
TENSOR = "tensor"
D = 768
HEAD = 64
FF = 3072
DD = 384
DFF = 1536
PATCH = 1536
TUBES = 1568
VIS = 157
STEP = 10
LANES = 128
TILE = 16
BLOCK = TILE * LANES
FRONT = 24
MESH = pl.DeviceIdType.MESH
F32 = jnp.float32
BF16 = jnp.bfloat16


def round_up(value, step):
    return -(-value // step) * step


COMMON = dict(
    embedding=(PATCH, D), embedding_bias=(D,), enc_norms=(6, D), enc_biases=(2, D), to_decoder=(D, DD), mask_token=(DD,),
    dec_norms=(6, DD), dec_biases=(2, DD), dec_qkv=(DD, 3 * DD), dec_qkv_bias=(2, DD), dec_proj=(DD, DD), pixel_head=(DD, PATCH),
    head_bias=(PATCH,))
SPLIT = dict(
    enc_qkv=(D, 576), enc_qkv_bias=(2, 192), enc_proj=(192, D), enc_up=(D, 768), enc_up_bias=(768,), enc_down=(768, D),
    dec_up=(DD, 384), dec_up_bias=(384,), dec_down=(384, DD))


def row_table(layout):
    table, at = {}, 0
    for name, shape in layout.items():
        count = math.prod(shape) // LANES
        table[name] = (at, count)
        at += count
    return Namespace(**table)


CROW = row_table(COMMON)
SROW = row_table(SPLIT)
DEC_ROW = SROW.dec_up[0]
SPLIT_ROWS = SROW.dec_down[0] + SROW.dec_down[1]
COMMON_ROWS = CROW.head_bias[0] + CROW.head_bias[1]


class Plan:
    def __init__(self, parts, share, rows_step):
        self.parts, self.share = parts, share
        self.base = [i * share // BLOCK * TILE for i in range(parts)]
        self.rows = round_up(-(-(share + BLOCK - 1) // LANES), rows_step)

    def pieces(self, first, last):
        out = []
        for i in range(self.parts):
            start = self.base[i] + (TILE if i else 0)
            stop = self.base[i + 1] if i + 1 < self.parts else self.base[i] + self.rows
            low, high = max(start, first), min(stop, last)
            if i and first <= self.base[i] < last:
                out.append(("edge", i, self.base[i] - self.base[i - 1], self.base[i], TILE))
            if low < high:
                out.append(("body", i, low - self.base[i], low, high - low))
        return out

    def owners(self, first, last):
        return sorted({i for kind, i, *_ in self.pieces(first, last)} | {i - 1 for kind, i, *_ in self.pieces(first, last) if kind == "edge"})


def align_kernel(scalars, split_in, common_in, split_out, common_out):
    def move(source, target, lanes, rows_down, skip, step):
        def part(row, step):
            lane = lax.broadcasted_iota(jnp.int32, (step, LANES), 1)
            here = source[pl.ds(FRONT - rows_down + skip + row, step), :]
            before = source[pl.ds(FRONT - 1 - rows_down + skip + row, step), :]
            value = jnp.where(lane >= lanes, pltpu.roll(here, lanes, 1), pltpu.roll(before, lanes, 1))
            target[pl.ds(pl.multiple_of(row, TILE), step), :] = value.astype(BF16)

        def body(index, _):
            part(index * step, step)
            return 0

        whole = target.shape[0] // step
        lax.fori_loop(0, whole, body, 0)
        if target.shape[0] % step:
            part(whole * step, target.shape[0] % step)

    move(split_in, split_out, scalars[0], scalars[1], 0, 256)
    move(common_in, common_out, scalars[2], scalars[3], scalars[4], 256)


def aligned(master, plan):
    tail = (plan.rows + 8) * LANES - master.shape[-1]
    return jnp.pad(master, ((0, 0),) * (master.ndim - 1) + ((FRONT * LANES, tail),)).reshape(-1, LANES)


def align(common_master, split_master, cplan, splan):
    me, t = lax.axis_index(DP), lax.axis_index(TENSOR)
    soff = me * splan.share % BLOCK
    coff = me * cplan.share % BLOCK
    quarter = cplan.rows // 4
    scalars = jnp.stack([soff % LANES, soff // LANES, coff % LANES, coff // LANES, t * quarter]).astype(jnp.int32)
    return pl.pallas_call(
        align_kernel,
        out_shape=(jax.ShapeDtypeStruct((splan.rows, LANES), BF16), jax.ShapeDtypeStruct((quarter, LANES), BF16)),
        in_specs=[pl.BlockSpec(memory_space=pltpu.SMEM), pl.BlockSpec(memory_space=pltpu.VMEM), pl.BlockSpec(memory_space=pltpu.VMEM)],
        out_specs=[pl.BlockSpec(memory_space=pltpu.VMEM)] * 2,
        name="align",
    )(scalars, aligned(split_master, splan), aligned(common_master, cplan))


OUTS = Namespace(
    embedding=(PATCH, D), to_decoder=(D, DD), dec_qkv=(DD, 3 * DD), dec_proj=(DD, DD), pixel_head=(DD, PATCH),
    enc_qkv=(2, D, 576), enc_proj=(384, D), enc_up=(D, 1536), enc_down=(1536, D), dec_up=(DD, 1536), dec_down=(1536, DD))
OUT_NAMES = tuple(vars(OUTS))
CMATS = OUT_NAMES[:5]
SMALLS = ((CROW.embedding_bias[0], 54), (CROW.mask_token[0], 27), (CROW.dec_qkv_bias[0], 6), (CROW.head_bias[0], 12))


def copy_rows(pieces, frame, wide, first, chunk=64):
    for kind, part, row, at, count in pieces:
        if kind == "edge":
            wide[pl.ds(at - first, TILE), :] = frame(part)[pl.ds(0, TILE), :].astype(F32) + frame(part - 1)[pl.ds(row, TILE), :].astype(F32)
            continue
        source, whole = frame(part), count // chunk

        def body(index, _, source=source, row=row, at=at):
            wide[pl.ds(pl.multiple_of(at - first + index * chunk, TILE), chunk), :] = source[
                pl.ds(pl.multiple_of(row + index * chunk, TILE), chunk), :
            ].astype(F32)
            return 0

        if whole:
            lax.fori_loop(0, whole, body, 0)
        for rest in range(whole * chunk, count, TILE):
            wide[pl.ds(at - first + rest, TILE), :] = source[pl.ds(row + rest, TILE), :].astype(F32)


def matrix_out(wide, start, rows, width, target, row0, col0, step=64):
    per_row = width // LANES

    def body(index, _):
        at = index * step
        for j in range(per_row):
            value = wide[pl.ds(start + j + at * per_row, step, stride=per_row), :]
            target[pl.ds(pl.multiple_of(row0 + at, TILE), step), col0 + j * LANES : col0 + (j + 1) * LANES] = value.astype(BF16)
        return 0

    lax.fori_loop(0, rows // step, body, 0)


def qkv_out(wide, start, pair_buf, target):
    step = 32
    lane = lax.broadcasted_iota(jnp.int32, (step, LANES), 1)

    def body(index, _):
        at = start + index * step * 9
        for j in range(5):
            even = wide[pl.ds(at + j, step, stride=9), :]
            low = pltpu.roll(wide[pl.ds(at + 4 + j, step, stride=9), :], 64, 1)
            if j < 4:
                high = pltpu.roll(wide[pl.ds(at + 5 + j, step, stride=9), :], 64, 1)
                odd = jnp.where(lane < 64, low, high)
            else:
                odd = low
            pair_buf[j, pl.ds(0, step, stride=2), :] = even
            pair_buf[j, pl.ds(1, step, stride=2), :] = odd
            both = pair_buf[j].astype(BF16)
            rows = pl.ds(pl.multiple_of(index * 64, 64), 64)
            if j < 4:
                target[rows, j * LANES : (j + 1) * LANES] = both
            else:
                target[rows, 512:576] = both[:, :64]
        return 0

    lax.fori_loop(0, 12, body, 0)


def floor16(value):
    return value // TILE * TILE


SCALE = HEAD ** (-0.5)


def nt(a, b):
    return lax.dot_general(a, b, (((1,), (1,)), ((), ())), preferred_element_type=F32)


def nn(a, b):
    return lax.dot_general(a, b, (((1,), (0,)), ((), ())), preferred_element_type=F32)


VP = 160
SAVED = Namespace(
    embedded=((VP, D), F32), normed_a=((VP, D), BF16), mixed=((2, VP, 576), BF16), probs=((6, VP, VP), F32), merged=((VP, 384), BF16),
    after=((VP, D), F32), normed_m=((VP, D), BF16), raised=((VP, 1536), F32), active=((VP, 1536), BF16), encoded=((VP, D), F32),
    final_low=((VP, D), BF16), lowered=((VP, DD), F32))
NSAVED = len(vars(SAVED))
SMALL_AT = []
for _, _count in SMALLS:
    SMALL_AT.append(sum(round_up(count, 8) for _, count in SMALLS[: len(SMALL_AT)]))


def norm_rows(inputs, gain, shift):
    centered = inputs - jnp.mean(inputs, axis=-1, keepdims=True)
    spread = jnp.mean(centered * centered, axis=-1, keepdims=True)
    return centered * lax.rsqrt(spread + 1e-06) * gain + shift


def unpacker(cplan, splan, common_frame, split_frame, dec_frame, stage, small_ref, bias_ref, dbias_ref, wide, pair_buf, done):
    def load(plan, frame, start, count):
        first, last = floor16(start), round_up(start + count, TILE)
        copy_rows(plan.pieces(first, last), frame, wide, first)
        return start - first

    def split(c):
        frame = functools.partial(split_frame, c)
        start, count = SROW.enc_qkv
        qkv_out(wide, load(splan, frame, start, count), pair_buf, stage.enc_qkv.at[c])
        at = load(splan, frame, *SROW.enc_qkv_bias)
        bias_ref[c, 0:8, :] = wide[pl.ds(at, 8), :]
        at = load(splan, frame, *SROW.enc_proj)
        matrix_out(wide, at, 192, D, stage.enc_proj, c * 192, 0)
        at = load(splan, frame, *SROW.enc_up)
        matrix_out(wide, at, D, 768, stage.enc_up, 0, c * 768)
        at = load(splan, frame, *SROW.enc_up_bias)
        bias_ref[c, 8:16, :] = wide[pl.ds(at, 8), :]
        at = load(splan, frame, *SROW.enc_down)
        matrix_out(wide, at, 768, D, stage.enc_down, c * 768, 0)
        if c:
            for whole in (stage.enc_qkv, stage.enc_proj, stage.enc_up, stage.enc_down):
                done(whole)

    def common(name):
        at = load(cplan, common_frame, *vars(CROW)[name])
        rows, width = vars(OUTS)[name]
        matrix_out(wide, at, rows, width, vars(stage)[name], 0, 0)
        if name != CMATS[0]:
            done(vars(stage)[name])

    def smalls():
        for small_at, (start, count) in zip(SMALL_AT, SMALLS):
            at = load(cplan, common_frame, start, count)
            small_ref[pl.ds(small_at, round_up(count, 8)), :] = wide[pl.ds(at, round_up(count, 8)), :]

    def dec():
        for slot in range(4):
            frame = functools.partial(split_frame, slot) if slot < 2 else functools.partial(dec_frame, slot - 2)
            at = load(splan, frame, DEC_ROW, SPLIT_ROWS - DEC_ROW)
            matrix_out(wide, at, DD, 384, stage.dec_up, 0, slot * 384)
            bias = at + SROW.dec_up_bias[0] - DEC_ROW
            dbias_ref[slot, :, :] = wide[pl.ds(bias, 8), :]
            matrix_out(wide, bias + 3, 384, DD, stage.dec_down, slot * 384, 0)
        done(stage.dec_up)
        done(stage.dec_down)

    return split, common, smalls, dec


def row_of(ref, at, count):
    return jnp.concatenate([ref[at + k : at + k + 1, :] for k in range(count)], axis=1)


def embed(pix, pos, stage, small_ref, saved):
    saved.embedded[...] = nn(pix[...], stage.embedding[...]) + row_of(small_ref, 0, 6) + pos[...]


def encode(stage, small_ref, bias_ref, saved, swap, while_first, while_second):
    def norm(k):
        return row_of(small_ref, 6 + 6 * k, 6)

    embedded = saved.embedded[...]
    normed = norm_rows(embedded, norm(0), norm(1)).astype(BF16)
    saved.normed_a[...] = normed
    keys = lax.broadcasted_iota(jnp.int32, (VP, VP), 1) < VIS
    outs = []
    for slot in range(2):
        flat = row_of(bias_ref.at[slot], 0, 3)
        bias = jnp.concatenate([flat[:, :192], jnp.zeros((1, 192), F32), flat[:, 192:]], axis=1)
        saved.mixed[slot] = (nn(normed, stage.enc_qkv[slot]) + bias).astype(BF16)
        for head in range(3):
            q, k, v = [saved.mixed[slot, :, 192 * n + HEAD * head : 192 * n + HEAD * (head + 1)] for n in range(3)]
            scores = jnp.where(keys, nt(q, k) * SCALE, -1e30)
            shifted = jnp.exp(scores - jnp.max(scores, axis=1, keepdims=True))
            probs = shifted / jnp.sum(shifted, axis=1, keepdims=True)
            saved.probs[slot * 3 + head] = probs
            outs.append(nn(probs.astype(BF16), v).astype(BF16))
    merged = jnp.concatenate(outs, axis=1)
    saved.merged[...] = merged
    mine, copy, other = swap(0)
    mine[...] = nn(merged, stage.enc_proj[...]).astype(BF16)
    copy.start()
    while_first()
    copy.wait_recv()
    after = embedded + (mine[...].astype(F32) + other[...].astype(F32) + row_of(small_ref, 42, 6))
    saved.after[...] = after
    normed = norm_rows(after, norm(2), norm(3)).astype(BF16)
    saved.normed_m[...] = normed
    up_bias = jnp.concatenate([row_of(bias_ref.at[slot], 8, 6) for slot in range(2)], axis=1)
    for col in range(0, 1536, 384):
        raised = nn(normed, stage.enc_up[:, col : col + 384]) + up_bias[:, col : col + 384]
        saved.raised[:, col : col + 384] = raised
        saved.active[:, col : col + 384] = (0.5 * raised * (1.0 + lax.erf(raised * math.sqrt(0.5)))).astype(BF16)
    mine, second, other = swap(1)
    mine[...] = nn(saved.active[...], stage.enc_down[...]).astype(BF16)
    second.start()
    while_second()
    second.wait_recv()
    encoded = saved.after[...] + (mine[...].astype(F32) + other[...].astype(F32) + row_of(small_ref, 48, 6))
    saved.encoded[...] = encoded
    saved.final_low[...] = norm_rows(encoded, norm(4), norm(5)).astype(BF16)
    copy.wait_send()
    second.wait_send()


def unpack_and_encode(cplan, splan, refs, ready):
    pix, pos, outs, smalls, saved, (sbuf, dbuf, cbuf, wide, pair_buf), stages, out_sem, (swaps, moved, send, recv) = refs
    t = lax.axis_index(TENSOR)
    y, c = t // 2, t % 2
    me = lax.axis_index(DP)
    fd = first_dec(splan)
    stage = Namespace(**dict(zip(OUT_NAMES, stages)))
    copies = []

    def done(whole):
        index = [ref is whole for ref in stages].index(True)
        copy = pltpu.make_async_copy(whole, outs[index], out_sem.at[index])
        copy.start()
        copies.append(copy)

    split, common, common_smalls, dec = unpacker(
        cplan, splan, lambda i: cbuf.at[i], lambda c, i: sbuf.at[c, i], lambda c, i: dbuf.at[c, i - fd],
        stage, smalls[0], smalls[1], smalls[2], wide, pair_buf, done)

    def swap(n):
        copy = pltpu.make_async_remote_copy(
            src_ref=swaps.at[n, 0], dst_ref=swaps.at[n, 1], send_sem=send.at[n], recv_sem=recv.at[n],
            device_id={DP: me, TENSOR: (1 - y) * 2 + c}, device_id_type=MESH)
        return swaps.at[n, 0], copy, swaps.at[n, 1]

    ready(0)
    common(CMATS[0])
    common_smalls()
    embed(pix, pos, stage, smalls[0], saved)
    ready(1)
    split(0)
    split(1)

    def first():
        common(CMATS[1])
        common(CMATS[2])

    def second():
        common(CMATS[3])
        common(CMATS[4])

    encode(stage, smalls[0], smalls[1], saved, swap, first, second)
    move = pltpu.make_async_remote_copy(
        src_ref=saved.final_low, dst_ref=moved, send_sem=send.at[2], recv_sem=recv.at[2],
        device_id={DP: me, TENSOR: y * 2 + (1 - c)}, device_id_type=MESH)

    @pl.when(y == c)
    def _():
        move.start()

    ready(2)
    dec()

    @pl.when(y == c)
    def _():
        saved.lowered[...] = nn(saved.final_low[...], stage.to_decoder[...])
        move.wait_send()

    @pl.when(y != c)
    def _():
        move.wait_recv()
        saved.lowered[...] = nn(moved[...], stage.to_decoder[...])

    for copy in copies:
        copy.wait()


SMALL_ROWS = sum(round_up(count, 8) for _, count in SMALLS)
GATHERED = tuple(jax.ShapeDtypeStruct(vars(OUTS)[name], BF16) for name in OUT_NAMES) + (
    jax.ShapeDtypeStruct((SMALL_ROWS, LANES), F32), jax.ShapeDtypeStruct((2, 16, LANES), F32), jax.ShapeDtypeStruct((4, 8, LANES), F32),
) + tuple(jax.ShapeDtypeStruct(*pair) for pair in vars(SAVED).values())


def first_dec(splan):
    return splan.owners(floor16(DEC_ROW), round_up(SPLIT_ROWS, TILE))[0]


def unpack_scratch(cplan, splan):
    fd = first_dec(splan)
    return [
        pltpu.VMEM((2, splan.parts, splan.rows, LANES), BF16),
        pltpu.VMEM((2, splan.parts - fd, splan.rows, LANES), BF16),
        pltpu.VMEM((cplan.parts, cplan.rows, LANES), BF16),
        pltpu.VMEM((CROW.embedding[1] + 32, LANES), F32),
        pltpu.VMEM((5, 64, LANES), F32),
    ] + [pltpu.VMEM(vars(OUTS)[name], BF16) for name in OUT_NAMES] + [
        pltpu.SemaphoreType.DMA((len(OUT_NAMES),)), pltpu.VMEM((2, 2, VP, D), BF16), pltpu.VMEM((VP, D), BF16),
        pltpu.SemaphoreType.DMA((3,)), pltpu.SemaphoreType.DMA((3,))]


def shared_refs(refs):
    nout = len(OUT_NAMES)
    pix, pos = refs[:2]
    outs, smalls = refs[2 : nout + 2], refs[nout + 2 : nout + 5]
    saved = Namespace(**dict(zip(vars(SAVED), refs[nout + 5 : nout + 5 + NSAVED])))
    refs = refs[nout + 5 + NSAVED :]
    return (pix, pos, outs, smalls, saved, refs[:5], refs[5 : 5 + nout], refs[5 + nout], refs[6 + nout : 10 + nout]), refs[10 + nout :]


def gather_kernel(cplan, splan, s_own, c_own, *refs):
    shared, (send, recv, local) = shared_refs(refs)
    sbuf, dbuf, cbuf = shared[5][:3]
    me, t = lax.axis_index(DP), lax.axis_index(TENSOR)
    z, x, y, c = me // 2, me % 2, t // 2, t % 2
    ty = (1 - y) * 2 + c
    fd = first_dec(splan)
    quarter = cplan.rows // 4

    def cblock(i, tt):
        return cbuf.at[i, pl.ds(pl.multiple_of(tt * quarter, TILE), quarter)]

    def sblock(i):
        return sbuf.at[c, i]

    zdev = [{DP: (z + k) % 4 * 2 + x, TENSOR: t} for k in range(4)]
    xdev, ydev, kdev = {DP: z * 2 + (1 - x), TENSOR: t}, {DP: me, TENSOR: ty}, {DP: me, TENSOR: y * 2 + (1 - c)}
    barrier = pltpu.get_barrier_semaphore()
    for device in zdev[1:] + [xdev, ydev, kdev]:
        pl.semaphore_signal(barrier, inc=1, device_id=device, device_id_type=MESH)
    own = [pltpu.make_async_copy(s_own, sblock(me), local.at[0]), pltpu.make_async_copy(c_own, cblock(me, t), local.at[1])]
    for copy in own:
        copy.start()
    pl.semaphore_wait(barrier, 6)
    for copy in own:
        copy.wait()

    def remote(source, target, slot, device):
        return pltpu.make_async_remote_copy(
            src_ref=source, dst_ref=target, send_sem=send.at[slot], recv_sem=recv.at[slot], device_id=device, device_id_type=MESH)

    def z_copy(common, down, hop, i):
        block = cblock(i, t) if common else sblock(i)
        return remote(block, block, common * 6 + down * 3 + hop - 1, zdev[3 if down else 1])

    def x_copy(common, i):
        block = cblock(i, t) if common else sblock(i)
        return remote(block, block, 12 + common * 4 + i // 2, xdev)

    def y_copy(i):
        return remote(cblock(i, t), cblock(i, t), 20 + i, ydev)

    def k_copy(i):
        return remote(sblock(i), sblock(i), 28 + i, kdev)

    def k_common(i):
        return remote(cblock(i, t), cblock(i, t), 36 + i, kdev)

    def k_far(i):
        return remote(cblock(i, ty), cblock(i, ty), 44 + i, kdev)

    def dec_rows(i):
        return pl.ds(max(0, DEC_FIRST - splan.base[i]), min(splan.rows, S_WIDE - splan.base[i]) - max(0, DEC_FIRST - splan.base[i]))

    def d_copy(i):
        return remote(sbuf.at[c, i, dec_rows(i)], dbuf.at[c, i - fd, dec_rows(i)], 52 + i - fd, ydev)

    def d_beside(i):
        return remote(dbuf.at[c, i - fd, dec_rows(i)], dbuf.at[c, i - fd, dec_rows(i)], 54 + i - fd, kdev)

    def send_z(common, down, hop):
        i = (z + (hop - 1 if down else 1 - hop)) * 2 + x
        able = jnp.logical_and(z > 0, z + hop - 1 <= 3) if down else jnp.logical_and(z < 3, z - hop + 1 >= 0)
        return i, able

    def pass_on(common, down, hop, action):
        i, able = send_z(common, down, hop)

        @pl.when(able)
        def _():
            action(z_copy(common, down, hop, i))

    def share_c(i):
        x_copy(1, i).start()
        y_copy(i).start()
        k_common(i).start()

    def share_s(i):
        x_copy(0, i).start()
        k_copy(i).start()
        dec_start(i)

    def dec_start(i):
        for known in range(fd, splan.parts):
            @pl.when(i == known)
            def _(known=known):
                d_copy(known).start()

    for common in (1, 0):
        for down in (0, 1):
            pass_on(common, down, 1, lambda copy: copy.start())
    share_c(me)
    share_s(me)
    for hop in (1, 2, 3):
        for common in (1, 0):
            for down in (0, 1):
                i = (z + (hop if down else -hop)) * 2 + x
                here = z + hop <= 3 if down else z >= hop

                @pl.when(here)
                def _(common=common, down=down, hop=hop, i=i):
                    z_copy(common, down, hop, i).wait_recv()
                    if hop < 3:
                        pass_on(common, down, hop + 1, lambda copy: copy.start())
                    if common:
                        share_c(i)
                    else:
                        share_s(i)

    def split_here(zz):
        i = zz * 2 + (1 - x)
        x_copy(0, i).wait_recv()
        k_copy(i).start()
        dec_start(i)

    def ready(stage):
        if stage == 0:
            for zz in range(4):
                i = zz * 2 + (1 - x)
                x_copy(1, i).wait_recv()
                y_copy(i).start()
                k_common(i).start()
            for i in range(8):
                y_copy(i).wait_recv()
                k_far(i).start()
            for i in range(8):
                k_common(i).wait_recv()
                k_far(i).wait_recv()
        if stage == 1:
            for zz in range(4):
                split_here(zz)
            for i in range(8):
                k_copy(i).wait_recv()
        if stage == 2:
            for i in range(fd, splan.parts):
                d_copy(i).wait_recv()
                d_beside(i).start()
            for i in range(fd, splan.parts):
                d_beside(i).wait_recv()

    unpack_and_encode(cplan, splan, shared, ready)
    for hop in (1, 2, 3):
        for common in (1, 0):
            for down in (0, 1):
                pass_on(common, down, hop, lambda copy: copy.wait_send())
    for zz in range(4):
        for common in (1, 0):
            x_copy(common, zz * 2 + x).wait_send()
    for i in range(8):
        for copy in (y_copy(i), k_copy(i), k_common(i), k_far(i)):
            copy.wait_send()
    for i in range(fd, splan.parts):
        d_copy(i).wait_send()
        d_beside(i).wait_send()


def local_unpack_kernel(cplan, splan, s_all, d_all, c_all, *refs):
    shared, (local,) = shared_refs(refs)
    t = lax.axis_index(TENSOR)
    barrier = pltpu.get_barrier_semaphore()
    for other in (t // 2 * 2 + 1 - t % 2, (1 - t // 2) * 2 + t % 2):
        pl.semaphore_signal(barrier, inc=1, device_id={DP: lax.axis_index(DP), TENSOR: other}, device_id_type=MESH)
    copies = [pltpu.make_async_copy(source, target, local.at[k]) for k, (source, target) in enumerate(zip((s_all, d_all, c_all), shared[5][:3]))]
    for copy in copies:
        copy.start()
    for copy in copies:
        copy.wait()
    pl.semaphore_wait(barrier, 2)
    unpack_and_encode(cplan, splan, shared, lambda stage: None)


def gather_weights(common_master, split_master, pix, pos, cplan, splan):
    s_own, c_own = align(common_master, split_master, cplan, splan)
    any_spec = pl.BlockSpec(memory_space=pl.ANY)
    vmem = pl.BlockSpec(memory_space=pltpu.VMEM)
    scratch = unpack_scratch(cplan, splan)
    fd = first_dec(splan)
    out_specs = [any_spec] * len(OUT_NAMES) + [vmem] * (3 + NSAVED)
    params = pltpu.CompilerParams(collective_id=0, has_side_effects=True, vmem_limit_bytes=64000 * 1024)
    if cplan.parts == 8 and splan.parts == 8:
        results = pl.pallas_call(
            functools.partial(gather_kernel, cplan, splan),
            out_shape=GATHERED, in_specs=[vmem] * 4, out_specs=out_specs,
            scratch_shapes=scratch + [pltpu.SemaphoreType.DMA((56,)), pltpu.SemaphoreType.DMA((56,)), pltpu.SemaphoreType.DMA((2,))],
            compiler_params=params, name="gather",
        )(s_own, c_own, pix, pos)
    else:
        y = lax.axis_index(TENSOR) // 2
        s_all = lax.all_gather(lax.all_gather(s_own, DP), TENSOR).reshape(2, 2, splan.parts, splan.rows, LANES)
        c_all = jnp.moveaxis(lax.all_gather(lax.all_gather(c_own, DP), TENSOR), 0, 1).reshape(cplan.parts, cplan.rows, LANES)
        s_mine = lax.dynamic_index_in_dim(s_all, y, 0, False)
        d_other = lax.dynamic_index_in_dim(s_all, 1 - y, 0, False)[:, fd:]
        results = pl.pallas_call(
            functools.partial(local_unpack_kernel, cplan, splan),
            out_shape=GATHERED, in_specs=[any_spec] * 3 + [vmem] * 2, out_specs=out_specs,
            scratch_shapes=scratch + [pltpu.SemaphoreType.DMA((3,))], compiler_params=params, name="unpack",
        )(s_mine, d_other, c_all, pix, pos)
    weights = Namespace(**dict(zip(OUT_NAMES, results)))
    small, bias, dbias = results[len(OUT_NAMES) : len(OUT_NAMES) + 3]
    at = 0
    rows = []
    for _, count in SMALLS:
        rows.append(small[at : at + count])
        at += round_up(count, 8)
    a, b, qkv_rows, head_rows = rows
    weights.embedding_bias = a[:6].reshape(1, D)
    weights.enc_norms = a[6:42].reshape(6, D)
    weights.enc_biases = a[42:54].reshape(2, D)
    weights.mask_token = b[:3].reshape(1, DD)
    weights.dec_norms = b[3:21].reshape(6, DD)
    weights.dec_biases = b[21:27].reshape(2, DD)
    weights.dec_qkv_bias = qkv_rows.reshape(2, DD)
    weights.head_bias = head_rows.reshape(1, PATCH)
    weights.enc_qkv_bias = bias[:, :3].reshape(2, 2, 192)
    weights.enc_up_bias = bias[:, 8:14].reshape(1, 1536)
    weights.dec_up_bias = dbias[:, :3].reshape(1, 1536)
    return weights, Namespace(**dict(zip(vars(SAVED), results[len(OUT_NAMES) + 3 :])))


DEC_FIRST = floor16(DEC_ROW)
S_WIDE = round_up(SPLIT_ROWS, TILE)
C_WIDE = round_up(COMMON_ROWS, TILE)
D_WIDE = S_WIDE - DEC_FIRST
SLOTS = 3


def buffer_rows(plan, wide):
    return max(wide, plan.base[-1] + plan.rows)


def narrow(wide, target, count, chunk=128):
    def body(index, _):
        at = pl.ds(pl.multiple_of(index * chunk, TILE), chunk)
        target[at, :] = wide[at, :].astype(BF16)
        return 0

    whole = count // chunk
    lax.fori_loop(0, whole, body, 0)
    if count % chunk:
        target[whole * chunk : count, :] = wide[whole * chunk : count, :].astype(BF16)


def clear(wide, first, last, chunk=64):
    def body(index, _):
        wide[pl.ds(first + index * chunk, chunk), :] = jnp.zeros((chunk, LANES), F32)
        return 0

    whole = (last - first) // chunk
    lax.fori_loop(0, whole, body, 0)
    rest = (last - first) % chunk
    if rest:
        wide[pl.ds(first + whole * chunk, rest), :] = jnp.zeros((rest, LANES), F32)


def matrix_in(wide, start, per_row, stage, rows, width, j0, step=64):
    def body(index, _):
        at = index * step
        for j in range(width // LANES):
            wide[pl.ds(start + j0 + j + at * per_row, step, stride=per_row), :] = stage[
                pl.ds(pl.multiple_of(at, 8), step), j * LANES : (j + 1) * LANES
            ]
        return 0

    lax.fori_loop(0, rows // step, body, 0)


def qkv_in(wide, start, pair_buf, stage):
    step = 32
    lane = lax.broadcasted_iota(jnp.int32, (step, LANES), 1)

    def body(index, _):
        at = start + index * step * 9
        even, odd = [], []
        base = pl.multiple_of(index * 64, 8)
        for j in range(5):
            lanes = slice(j * LANES, (j + 1) * LANES) if j < 4 else slice(512, 640)
            pair_buf[j] = stage[pl.ds(base, 64), lanes]
            even.append(pair_buf[j, pl.ds(0, step, stride=2), :])
            odd.append(pltpu.roll(pair_buf[j, pl.ds(1, step, stride=2), :], 64, 1))
        for j in range(4):
            wide[pl.ds(at + j, step, stride=9), :] = even[j]
        wide[pl.ds(at + 4, step, stride=9), :] = jnp.where(lane < 64, even[4], odd[0])
        for j in range(4):
            wide[pl.ds(at + 5 + j, step, stride=9), :] = jnp.where(lane < 64, odd[j], odd[j + 1])
        return 0

    lax.fori_loop(0, 12, body, 0)


def add_rows(target, parts, count, chunk=None):
    chunk = chunk or max(c for c in (128, 64, 48, 32, 16) if count % c == 0)

    def body(index, _):
        at = index * chunk
        total = None
        for ref, start in parts:
            value = ref[pl.ds(pl.multiple_of(start + at, TILE), chunk), :].astype(F32)
            total = value if total is None else total + value
        target[pl.ds(pl.multiple_of(at, TILE), chunk), :] = total.astype(target.dtype)
        return 0

    lax.fori_loop(0, count // chunk, body, 0)


def unalign(source, target, share, offset):
    down, lanes = offset // LANES, offset % LANES
    step = 64
    lane = lax.broadcasted_iota(jnp.int32, (step, LANES), 1)
    row = lax.broadcasted_iota(jnp.int32, (step, LANES), 0)

    def body(index, total):
        at = index * step
        here = pltpu.roll(source[pl.ds(down + at, step), :], LANES - lanes, 1)
        after = pltpu.roll(source[pl.ds(down + at + 1, step), :], LANES - lanes, 1)
        value = jnp.where(lane < LANES - lanes, here, after)
        value = jnp.where((row + at) * LANES + lane < share, value, 0.0)
        target[pl.ds(pl.multiple_of(at, 8), step), :] = value
        square = (value * value).reshape(step // 8, 8, LANES)
        return total + jnp.sum(square, axis=0)

    return lax.fori_loop(0, target.shape[0] // step, body, jnp.zeros((8, LANES), F32))


def flat_rows(share):
    return round_up(-(-share // LANES), 64)


def grad_jobs(y, grads, small, bias, dbias, wide, pair_buf, gs, gd, gc):
    grad = Namespace(**dict(zip(OUT_NAMES, grads)))
    half = CROW.embedding[1] // 2

    def matrix(source, rows, width, per_row, start, j0=0):
        def place(stage):
            matrix_in(wide, start, per_row, stage, rows, width, j0)

        return (place, source, rows, width)

    def small_rows(source, start):
        def action():
            wide[pl.ds(start, source.shape[0]), :] = source[...]

        return (action,)

    def columns(slot, width):
        return pl.ds(pl.multiple_of(slot * width, LANES), width)

    def rows_of(slot, count):
        return pl.ds(pl.multiple_of(slot * count, 8), count)

    def dec_part(slot, first):
        return [
            matrix(grad.dec_up.at[:, columns(slot, 384)], DD, 384, 3, SROW.dec_up[0] - first),
            small_rows(dbias.at[slot, pl.ds(0, 3)], SROW.dec_up_bias[0] - first),
            matrix(grad.dec_down.at[rows_of(slot, 384)], 384, DD, 3, SROW.dec_down[0] - first),
            (functools.partial(clear, wide, SPLIT_ROWS - first, S_WIDE - first),)]

    def split_jobs(slot):
        return [
            (functools.partial(qkv_in, wide, SROW.enc_qkv[0], pair_buf), grad.enc_qkv.at[:, columns(slot, 640)], D, 640),
            small_rows(bias.at[slot, pl.ds(0, 3)], SROW.enc_qkv_bias[0]),
            matrix(grad.enc_proj.at[rows_of(slot, 192)], 192, D, 6, SROW.enc_proj[0]),
            matrix(grad.enc_up.at[:, columns(slot, 768)], D, 768, 6, SROW.enc_up[0]),
            small_rows(bias.at[slot, pl.ds(8, 6)], SROW.enc_up_bias[0]),
            matrix(grad.enc_down.at[rows_of(slot, 768)], 768, D, 6, SROW.enc_down[0]),
        ] + dec_part(slot, 0) + [(lambda: narrow(wide, gs.at[slot], S_WIDE),)]

    def dec_jobs(slot):
        return [(lambda: clear(wide, 0, DEC_ROW - DEC_FIRST),)] + dec_part(slot + 2, DEC_FIRST) + [(lambda: narrow(wide, gd.at[slot], D_WIDE),)]

    def clear_other():
        def body(index, _):
            wide[pl.ds((1 - y) * half + index * 64, 64), :] = jnp.zeros((64, LANES), F32)
            return 0

        lax.fori_loop(0, half // 64, body, 0)
        clear(wide, COMMON_ROWS, C_WIDE)

    common = [(clear_other,), matrix(grad.embedding, 768, D, 6, y * half)]
    at = 0
    for start, count in SMALLS:
        common.append(small_rows(small.at[pl.ds(at, count)], start))
        at += round_up(count, 8)
    for name in CMATS[1:]:
        rows, total = vars(OUTS)[name]
        for col in range(0, total, 768):
            width = min(768, total - col)
            common.append(matrix(vars(grad)[name].at[:, pl.ds(col, width)], rows, width, total // LANES, vars(CROW)[name][0], col // LANES))
    common.append((lambda: narrow(wide, gc, C_WIDE),))
    return split_jobs, dec_jobs, common


def run_jobs(jobs, stage, stage_sem):
    loads = [job for job in jobs if len(job) > 1]
    copies = [
        pltpu.make_async_copy(job[1], stage.at[n % SLOTS, pl.ds(0, job[2]), pl.ds(0, job[3])], stage_sem.at[n % SLOTS]) for n, job in enumerate(loads)]
    for copy in copies[: SLOTS - 1]:
        copy.start()
    index = 0
    for job in jobs:
        if len(job) == 1:
            job[0]()
            continue
        if index + SLOTS - 1 < len(copies):
            copies[index + SLOTS - 1].start()
        copies[index].wait()
        job[0](stage.at[index % SLOTS])
        index += 1


ZORDER = (0, 3, 1, 2)
SUBS = 4


def reduce_kernel(cplan, splan, *refs):
    nin = len(OUT_NAMES)
    grads, (small, bias, dbias, loss) = refs[:nin], refs[nin : nin + 4]
    g_split, g_common, sums = refs[nin + 4 : nin + 7]
    (wide, pair_buf, stage, gs, gd, gc, ks, xs, zs, kc, yc, xc, zc, kd, yd, cq, fin, finc, part, stage_sem, send, recv) = refs[nin + 7 :]
    me, t = lax.axis_index(DP), lax.axis_index(TENSOR)
    z, x, y, c = me // 2, me % 2, t // 2, t % 2
    rank = me * 4 + t
    srows, quarter = splan.rows, cplan.rows // 4
    sub = srows // SUBS
    updev, downdev = {DP: (z + 1) % 4 * 2 + x, TENSOR: t}, {DP: (z + 3) % 4 * 2 + x, TENSOR: t}
    xdev, ydev, kdev = {DP: z * 2 + (1 - x), TENSOR: t}, {DP: me, TENSOR: (1 - y) * 2 + c}, {DP: me, TENSOR: y * 2 + (1 - c)}
    others = [(rank + k) % 32 for k in range(1, 32)]
    devices = [{DP: other // 4, TENSOR: other % 4} for other in others]
    barrier = pltpu.get_barrier_semaphore()
    for device in devices:
        pl.semaphore_signal(barrier, inc=1, device_id=device, device_id_type=MESH)

    def remote(source, target, slot, device):
        return pltpu.make_async_remote_copy(
            src_ref=source, dst_ref=target, send_sem=send.at[slot], recv_sem=recv.at[slot], device_id=device, device_id_type=MESH)

    def s_at(i):
        return pl.multiple_of(i * splan.share // BLOCK * TILE, TILE)

    def c_at(i, tt):
        return pl.multiple_of(i * cplan.share // BLOCK * TILE + tt * quarter, TILE)

    def piece(q):
        return pl.ds(pl.multiple_of(q * sub, TILE), sub)

    def kd_copy():
        return remote(gd.at[1 - c], kd, 0, kdev)

    def ks_copy(i):
        return remote(gs.at[1 - c, pl.ds(s_at(i), srows)], ks.at[i], 1 + i, kdev)

    def kc_copy(i, yy):
        return remote(gc.at[pl.ds(c_at(i, 2 * yy + 1 - c), quarter)], kc.at[i, yy], 9 + i * 2 + yy, kdev)

    def yd_copy():
        return remote(kd, yd, 25, ydev)

    def yc_copy(i):
        return remote(kc.at[i, 1 - y], yc.at[i], 26 + i, ydev)

    def xs_copy(zz, q):
        return remote(ks.at[zz * 2 + (1 - x), piece(q)], xs.at[zz, piece(q)], 34 + zz * 4 + q, xdev)

    def xc_copy(zz):
        return remote(yc.at[zz * 2 + (1 - x)], xc.at[zz], 50 + zz, xdev)

    def zs_copy(down, zz, q):
        return remote(xs.at[zz, piece(q)], zs.at[down, zz, piece(q)], 54 + down * 16 + zz * 4 + q, downdev if down else updev)

    def zc_copy(down, zz):
        return remote(xc.at[zz], zc.at[down, zz], 86 + down * 4 + zz, downdev if down else updev)

    def along_z(zz, copy_of, add):
        for down in (0, 1):
            passes = z > zz if down else z < zz
            first = z == 3 if down else z == 0

            @pl.when(jnp.logical_and(passes, first))
            def _():
                add(None)

            @pl.when(jnp.logical_and(passes, jnp.logical_not(first)))
            def _(down=down):
                copy_of(down).wait_recv()
                add(down)

            @pl.when(passes)
            def _(down=down):
                copy_of(down).start()

    def across_x(zz):
        i = zz * 2 + (1 - x)
        ks_copy(i).wait_recv()

        def body(q, _):
            add_rows(ks.at[i, piece(q)], [(ks.at[i, piece(q)], 0), (gs.at[c], s_at(i) + q * sub)], sub)
            xs_copy(zz, q).start()
            return 0

        lax.fori_loop(0, SUBS, body, 0)

    def first_sends():
        pl.semaphore_wait(barrier, 31)
        kd_copy().start()

    def core_sends():
        for zz in ZORDER:
            ks_copy(zz * 2 + (1 - x)).start()
        for zz in ZORDER:
            ks_copy(zz * 2 + x).start()

    def dec_across():
        kd_copy().wait_recv()
        add_rows(kd, [(gd.at[c], 0), (kd, 0)], D_WIDE)
        yd_copy().start()

    def common_core_sends():
        for zz in ZORDER:
            for xx in (0, 1):
                for yy in (0, 1):
                    kc_copy(zz * 2 + xx, yy).start()

    split_jobs, dec_jobs, common_jobs = grad_jobs(y, grads, small, bias, dbias, wide, pair_buf, gs, gd, gc)
    run_jobs(
        dec_jobs(1 - c) + [(first_sends,)] + dec_jobs(c) + split_jobs(1 - c) + [(core_sends,), (dec_across,)] + split_jobs(c)
        + [(functools.partial(across_x, ZORDER[0]),)] + common_jobs + [(common_core_sends,)], stage, stage_sem)
    yd_copy().wait_recv()
    dec_rows = gs.at[c, pl.ds(DEC_FIRST, D_WIDE)]
    add_rows(dec_rows, [(dec_rows, 0), (yd, 0)], D_WIDE)
    for zz in ZORDER[1:]:
        across_x(zz)
    for zz in ZORDER:
        for xx in (0, 1):
            i = zz * 2 + xx
            for yy in (0, 1):
                kc_copy(i, yy).wait_recv()
            add_rows(kc.at[i, 1 - y], [(gc, c_at(i, 2 * (1 - y) + c)), (kc.at[i, 1 - y], 0)], quarter)
            yc_copy(i).start()
    for zz in ZORDER:
        i = zz * 2 + (1 - x)
        yc_copy(i).wait_recv()
        add_rows(yc.at[i], [(gc, c_at(i, t)), (kc.at[i, y], 0), (yc.at[i], 0)], quarter)
        xc_copy(zz).start()
        i = zz * 2 + x
        ks_copy(i).wait_recv()

        def body(q, _, zz=zz, i=i):
            xs_copy(zz, q).wait_recv()

            def add(flow):
                parts = [(xs.at[zz, piece(q)], 0), (gs.at[c], s_at(i) + q * sub), (ks.at[i, piece(q)], 0)]
                add_rows(xs.at[zz, piece(q)], parts + ([] if flow is None else [(zs.at[flow, zz, piece(q)], 0)]), sub)

            along_z(zz, lambda down: zs_copy(down, zz, q), add)
            return 0

        lax.fori_loop(0, SUBS, body, 0)
    for zz in ZORDER:
        i = zz * 2 + x
        yc_copy(i).wait_recv()
        xc_copy(zz).wait_recv()

        def add_common(flow, zz=zz, i=i):
            parts = [(xc.at[zz], 0), (gc, c_at(i, t)), (kc.at[i, y], 0), (yc.at[i], 0)]
            add_rows(xc.at[zz], parts + ([] if flow is None else [(zc.at[flow, zz], 0)]), quarter)

        along_z(zz, lambda down, zz=zz: zc_copy(down, zz), add_common)

    def ends(copy_of, action):
        for low, high in ((0, 1), (1, 1), (1, 0)):
            here = jnp.logical_and((z > 0) == bool(low), (z < 3) == bool(high))

            @pl.when(here)
            def _(low=low, high=high):
                flows = [0] * low + [1] * high
                for flow in flows:
                    copy_of(flow)
                action(flows)

    mine = pl.ds(pl.multiple_of(t * quarter, TILE), quarter)
    ends(
        lambda flow: zc_copy(flow, z).wait_recv(),
        lambda flows: add_rows(
            cq.at[mine], [(xc.at[z], 0), (gc, c_at(me, t)), (kc.at[me, y], 0), (yc.at[me], 0)] + [(zc.at[flow, z], 0) for flow in flows], quarter))
    far = pl.ds(pl.multiple_of(((1 - y) * 2 + c) * quarter, TILE), quarter)
    across_t, beside_t, beside_far = remote(cq.at[mine], cq.at[mine], 94, ydev), remote(cq.at[mine], cq.at[mine], 95, kdev), remote(cq.at[far], cq.at[far], 96, kdev)
    across_t.start()
    beside_t.start()

    def wait_split(flow):
        for q in range(SUBS):
            zs_copy(flow, z, q).wait_recv()

    ends(
        wait_split,
        lambda flows: add_rows(fin, [(xs.at[z], 0), (gs.at[c], s_at(me)), (ks.at[me], 0)] + [(zs.at[flow, z], 0) for flow in flows], srows))
    across_t.wait_recv()
    beside_far.start()
    squares = unalign(fin, g_split, splan.share, me * splan.share % BLOCK)
    beside_t.wait_recv()
    beside_far.wait_recv()
    add_rows(finc, [(cq, 0)], cplan.rows)
    squares += unalign(finc, g_common, cplan.share, me * cplan.share % BLOCK) * 0.25
    part[rank, 0:8, :] = squares
    part[rank, 8:16, :] = loss[...]
    shared = [remote(part.at[rank], part.at[rank], 97 + k, device) for k, device in enumerate(devices)]
    for copy in shared:
        copy.start()
    kd_copy().wait_send()
    yd_copy().wait_send()
    for i in range(8):
        ks_copy(i).wait_send()
        yc_copy(i).wait_send()
        for yy in range(2):
            kc_copy(i, yy).wait_send()
    for zz in range(4):
        xc_copy(zz).wait_send()
        for q in range(SUBS):
            xs_copy(zz, q).wait_send()
        for down in (0, 1):
            @pl.when(z > zz if down else z < zz)
            def _(down=down, zz=zz):
                zc_copy(down, zz).wait_send()
                for q in range(SUBS):
                    zs_copy(down, zz, q).wait_send()
    for copy in (across_t, beside_t, beside_far):
        copy.wait_send()
    for copy in shared:
        copy.wait_recv()

    def total(index, value):
        return value + part[index]

    sums[...] = lax.fori_loop(0, 32, total, jnp.zeros((16, LANES), F32))
    for copy in shared:
        copy.wait_send()


def pack_kernel(*refs):
    nin = len(OUT_NAMES)
    grads, (small, bias, dbias) = refs[:nin], refs[nin : nin + 3]
    gs_out, gd_out, gc_out = refs[nin + 3 : nin + 6]
    wide, pair_buf, stage, gs, gd, gc, stage_sem, out_sem = refs[nin + 6 :]
    split_jobs, dec_jobs, common_jobs = grad_jobs(lax.axis_index(TENSOR) // 2, grads, small, bias, dbias, wide, pair_buf, gs, gd, gc)
    run_jobs(dec_jobs(0) + dec_jobs(1) + split_jobs(0) + split_jobs(1) + common_jobs, stage, stage_sem)
    copies = [pltpu.make_async_copy(a, b, out_sem.at[k]) for k, (a, b) in enumerate(((gs, gs_out), (gd, gd_out), (gc, gc_out)))]
    for copy in copies:
        copy.start()
    for copy in copies:
        copy.wait()


def unalign_kernel(share_s, share_c, scalars, s_in, c_in, s_out, c_out, sums):
    sums[...] = unalign(s_in, s_out, share_s, scalars[0]) + unalign(c_in, c_out, share_c, scalars[1]) * 0.25


def reduce_grads(grads, small, bias, dbias, loss, cplan, splan):
    any_spec, vmem = pl.BlockSpec(memory_space=pl.ANY), pl.BlockSpec(memory_space=pltpu.VMEM)
    srows, quarter = splan.rows, cplan.rows // 4
    gs_rows, gc_rows = buffer_rows(splan, S_WIDE), buffer_rows(cplan, C_WIDE)
    flat = (jax.ShapeDtypeStruct((flat_rows(splan.share), LANES), F32), jax.ShapeDtypeStruct((flat_rows(cplan.share), LANES), F32))
    packing = [
        pltpu.VMEM((C_WIDE, LANES), F32), pltpu.VMEM((5, 64, LANES), F32), pltpu.VMEM((SLOTS, 768, 768), F32),
        pltpu.VMEM((2, gs_rows, LANES), BF16), pltpu.VMEM((2, D_WIDE, LANES), BF16), pltpu.VMEM((gc_rows, LANES), BF16)]
    operands = [vars(grads)[name] for name in OUT_NAMES]
    limit = 67_000_000
    if cplan.parts == 8 and splan.parts == 8:
        def rows(*shape, kind=BF16):
            return pltpu.VMEM(shape + (LANES,), kind)

        copies = 128
        return pl.pallas_call(
            functools.partial(reduce_kernel, cplan, splan),
            out_shape=flat + (jax.ShapeDtypeStruct((16, LANES), F32),),
            in_specs=[any_spec] * len(operands) + [vmem] * 4, out_specs=[vmem] * 3,
            scratch_shapes=packing + [
                rows(8, srows), rows(4, srows), rows(2, 4, srows), rows(8, 2, quarter), rows(8, quarter), rows(4, quarter), rows(2, 4, quarter),
                rows(D_WIDE), rows(D_WIDE), rows(cplan.rows),
                rows(srows + 64, kind=F32), rows(cplan.rows + 64, kind=F32), rows(32, 16, kind=F32),
                pltpu.SemaphoreType.DMA((SLOTS,)), pltpu.SemaphoreType.DMA((copies,)), pltpu.SemaphoreType.DMA((copies,))],
            compiler_params=pltpu.CompilerParams(collective_id=1, has_side_effects=True, vmem_limit_bytes=limit),
            name="reduce",
        )(*operands, small, bias, dbias, loss)
    shapes = [jax.ShapeDtypeStruct((2, gs_rows, LANES), BF16), jax.ShapeDtypeStruct((2, D_WIDE, LANES), BF16), jax.ShapeDtypeStruct((gc_rows, LANES), BF16)]
    gs, gd, gc = pl.pallas_call(
        pack_kernel, out_shape=shapes, in_specs=[any_spec] * len(operands) + [vmem] * 3, out_specs=[any_spec] * 3,
        scratch_shapes=packing + [pltpu.SemaphoreType.DMA((SLOTS,)), pltpu.SemaphoreType.DMA((3,))],
        compiler_params=pltpu.CompilerParams(vmem_limit_bytes=limit), name="pack",
    )(*operands, small, bias, dbias)
    me, t = lax.axis_index(DP), lax.axis_index(TENSOR)
    c = t % 2

    def swap(value, bit):
        return lax.ppermute(value, TENSOR, [(i, i ^ bit) for i in range(4)])

    def mine(value):
        keep = lax.dynamic_index_in_dim(value, c, 0, False).astype(F32)
        return keep + swap(lax.dynamic_index_in_dim(value, 1 - c, 0, False), 1).astype(F32)

    far = swap(mine(gd).astype(BF16), 2)
    split_sum = mine(gs).at[DEC_FIRST : DEC_FIRST + D_WIDE].add(far.astype(F32))
    common_sum = lax.psum(gc, TENSOR).astype(F32)

    def scattered(value, plan):
        frames = jnp.stack([value[base : base + plan.rows] for base in plan.base])
        return lax.psum_scatter(frames.astype(BF16), DP, scatter_dimension=0, tiled=True)[0].astype(F32)

    s_frame, c_frame = scattered(split_sum, splan), scattered(common_sum, cplan)
    pad = ((0, 64), (0, 0))
    g_split, g_common, squares = pl.pallas_call(
        functools.partial(unalign_kernel, splan.share, cplan.share), out_shape=flat + (jax.ShapeDtypeStruct((8, LANES), F32),),
        in_specs=[pl.BlockSpec(memory_space=pltpu.SMEM), vmem, vmem], out_specs=[vmem] * 3, name="unalign",
    )(jnp.stack([me * splan.share % BLOCK, me * cplan.share % BLOCK]).astype(jnp.int32), jnp.pad(s_frame, pad), jnp.pad(c_frame, pad))
    return g_split, g_common, lax.psum(jnp.concatenate([squares, loss]), (DP, TENSOR))


OWN = TUBES // 2
KEYS = 392


def head_masks(rows):
    lane = lax.broadcasted_iota(jnp.int32, (rows, LANES), 1)
    return lane < HEAD, lane >= HEAD


def attend_kernel(q_ref, k_ref, v_ref, o_ref, lse_ref, vt_ref, shifted_ref):
    q = q_ref[...]
    vt_ref[...] = v_ref[...].T
    pieces = []
    for head, mask in enumerate(head_masks(OWN)):
        qm = jnp.where(mask, q * SCALE, jnp.zeros_like(q))
        top = None
        for first in range(0, TUBES, KEYS):
            most = jnp.max(nt(k_ref[first : first + KEYS, :], qm), axis=0, keepdims=True)
            top = most if top is None else jnp.maximum(top, most)
        total = None
        qm = jnp.where(mask, q, jnp.zeros_like(q))
        for first in range(0, TUBES, KEYS):
            shifted = jnp.exp(nt(k_ref[first : first + KEYS, :], qm) * SCALE - top)
            part = jnp.sum(shifted, axis=0, keepdims=True)
            total = part if total is None else total + part
            shifted_ref[first : first + KEYS, :] = shifted.astype(BF16)
        pieces.append(nn(vt_ref[head * HEAD : (head + 1) * HEAD, :], shifted_ref[...]) / total)
        lse_ref[0, head : head + 1, :] = top + jnp.log(total)
    o_ref[...] = jnp.concatenate(pieces, axis=0).T


def attend(q, k, v):
    block, whole = pl.BlockSpec((OWN, LANES), lambda h: (0, h)), pl.BlockSpec((TUBES, LANES), lambda h: (0, h))
    return pl.pallas_call(
        attend_kernel, grid=(3,),
        out_shape=(jax.ShapeDtypeStruct((OWN, DD), F32), jax.ShapeDtypeStruct((3, 8, OWN), F32)),
        in_specs=[block, whole, whole], out_specs=[block, pl.BlockSpec((1, 8, OWN), lambda h: (h, 0, 0))],
        scratch_shapes=[pltpu.VMEM((LANES, TUBES), BF16), pltpu.VMEM((TUBES, OWN), BF16)], name="attend",
    )(q, k, v)


def attend_back_kernel(q_ref, k_ref, v_ref, do_ref, o_ref, lse_ref, dq_ref, dk_ref, dv_ref, kt_ref, ds_ref):
    q, do = q_ref[...], do_ref[...]
    kt_ref[...] = k_ref[...].T
    along = (do.astype(F32) * o_ref[...]).T
    pieces = []
    for head, mask in enumerate(head_masks(OWN)):
        qm, dom = jnp.where(mask, q * SCALE, jnp.zeros_like(q)), jnp.where(mask, do, jnp.zeros_like(do))
        delta = jnp.sum(along[head * HEAD : (head + 1) * HEAD], axis=0, keepdims=True)
        lse = lse_ref[0, head : head + 1, :]
        for first in range(0, TUBES, KEYS):
            rows = slice(first, first + KEYS)
            probs = jnp.exp(nt(k_ref[rows, :], qm) - lse)
            dv = nn(probs.astype(BF16), dom)
            ds = (probs * (nt(v_ref[rows, :], dom) - delta)).astype(BF16)
            ds_ref[rows, :] = ds
            dk = nn(ds, qm)
            if head:
                dk_ref[rows, :] += dk
                dv_ref[rows, :] += dv
            else:
                dk_ref[rows, :] = dk
                dv_ref[rows, :] = dv
        pieces.append(nn(kt_ref[head * HEAD : (head + 1) * HEAD, :], ds_ref[...]))
    dq_ref[...] = (jnp.concatenate(pieces, axis=0) * SCALE).T.astype(BF16)


def attend_back(q, k, v, do, o, lse):
    block, whole = pl.BlockSpec((OWN, LANES), lambda h: (0, h)), pl.BlockSpec((TUBES, LANES), lambda h: (0, h))
    return pl.pallas_call(
        attend_back_kernel, grid=(3,),
        out_shape=(jax.ShapeDtypeStruct((OWN, DD), BF16), jax.ShapeDtypeStruct((TUBES, DD), F32), jax.ShapeDtypeStruct((TUBES, DD), F32)),
        in_specs=[block, whole, whole, block, block, pl.BlockSpec((1, 8, OWN), lambda h: (h, 0, 0))], out_specs=[block, whole, whole],
        scratch_shapes=[pltpu.VMEM((LANES, TUBES), BF16), pltpu.VMEM((TUBES, OWN), BF16)], name="attend_back",
    )(q, k, v, do, o, lse)


NORM_EPS = 1e-06
PIXEL_EPS = 1e-06
CLIP_RATIO = 1.5
BETA_FIRST = 0.9
BETA_SECOND = 0.95
LEARN_RATE = 0.05
DECAY_RATE = 0.05
ADAM_EPS = 1e-08


def layer_norm(inputs, gain, shift):
    centered = inputs - jnp.mean(inputs, axis=-1, keepdims=True)
    spread = jnp.mean(centered * centered, axis=-1, keepdims=True)
    return centered * lax.rsqrt(spread + NORM_EPS) * gain + shift


def norm_back(inputs, gain, grad):
    centered = inputs - jnp.mean(inputs, axis=-1, keepdims=True)
    scale = lax.rsqrt(jnp.mean(centered * centered, axis=-1, keepdims=True) + NORM_EPS)
    unit = centered * scale
    inner = grad * gain
    back = scale * (inner - jnp.mean(inner, axis=-1, keepdims=True) - unit * jnp.mean(inner * unit, axis=-1, keepdims=True))
    return back, jnp.sum(grad * unit, axis=0), jnp.sum(grad, axis=0)


def tn(a, b):
    return lax.dot_general(a, b, (((0,), (0,)), ((), ())), preferred_element_type=F32)


def gelu(inputs):
    return jax.nn.gelu(inputs, approximate=False)


def gelu_slope(inputs):
    return 0.5 * (1.0 + lax.erf(inputs * math.sqrt(0.5))) + inputs * jnp.exp(-0.5 * inputs * inputs) * (1.0 / math.sqrt(2.0 * math.pi))


def sine_rows(position, width):
    column = jnp.arange(width)
    exponent = (2 * (column // 2)).astype(F32) / width
    angles = position.astype(F32)[:, None] / jnp.power(10000.0, exponent)[None, :]
    return jnp.where((column % 2 == 0)[None, :], jnp.sin(angles), jnp.cos(angles))


def sine_table(width, step=32):
    column = np.arange(width)
    rate = 10000.0 ** (-(2 * (column // 2)) / width)
    high, low = np.arange(0, TUBES, step)[:, None] * rate, np.arange(step)[:, None] * rate
    even = column % 2 == 0
    a = np.where(even, np.sin(high), np.cos(high)).astype(np.float32)
    b = np.where(even, np.cos(high), -np.sin(high)).astype(np.float32)
    c, s = np.cos(low).astype(np.float32), np.sin(low).astype(np.float32)
    table = a[:, None] * jnp.asarray(c)[None] + b[:, None] * jnp.asarray(s)[None]
    return table.reshape(TUBES, width)


def across(value):
    return lax.ppermute(value, TENSOR, [(i, i ^ 2) for i in range(4)])


def beside(value):
    return lax.ppermute(value, TENSOR, [(i, i ^ 1) for i in range(4)])


def y_total(partial):
    low = partial.astype(BF16)
    return low.astype(F32) + across(low).astype(F32)


def heads_back(parts):
    stacked = jnp.stack([part.reshape(2, 3, VP, HEAD) for part in parts], axis=1)
    return stacked.transpose(3, 0, 1, 2, 4).reshape(VP, 1152)


def seen_inputs(pixels, order):
    c = lax.axis_index(TENSOR) % 2
    seen = jnp.pad(lax.dynamic_index_in_dim(order, c, 0, False)[:VIS], (0, VP - VIS))
    return jnp.take(pixels.reshape(2 * TUBES, PATCH), c * TUBES + seen, axis=0), sine_rows(seen, D)


def step_grads(pixels, order, seen_pixels, w, saved, scale_back):
    t = lax.axis_index(TENSOR)
    y, c = t // 2, t % 2
    first_y = (y == 0).astype(F32)
    seen_y = jnp.pad(lax.dynamic_index_in_dim(order, y, 0, False)[:VIS], (0, VP - VIS), constant_values=-1)
    rows = pixels.reshape(2 * TUBES, PATCH)
    norms = w.enc_norms
    embedded, normed_a, merged, after, normed_m = saved.embedded, saved.normed_a, saved.merged, saved.after, saved.normed_m
    raised, active, encoded, final_low = saved.raised, saved.active, saved.encoded, saved.final_low
    parts = saved.mixed.reshape(2, VP, 3, 3, HEAD)
    q, k, v = [parts[:, :, n].transpose(0, 2, 1, 3).reshape(6, VP, HEAD) for n in range(3)]
    probs = saved.probs
    probs_low = probs.astype(BF16)
    qkv_w = jnp.concatenate([w.enc_qkv[0], w.enc_qkv[1]], axis=1)
    lowered = saved.lowered
    select = seen_y[None, :] == jnp.arange(TUBES, dtype=jnp.int32)[:, None]
    visible = jnp.any(select, axis=1, keepdims=True)
    placed = lax.dot_general(select.astype(F32), lowered, (((1,), (0,)), ((), ())), precision=lax.Precision.HIGHEST, preferred_element_type=F32)
    dec_in = placed + jnp.where(visible, 0.0, w.mask_token) + sine_table(DD)
    start = c * OWN

    def own(value):
        return lax.dynamic_slice_in_dim(value, start, OWN, 0)

    dnorms, dbiases = w.dec_norms, w.dec_biases
    normed_all = layer_norm(dec_in, dnorms[0], dnorms[1]).astype(BF16)
    normed_q = own(normed_all)
    dec_own = own(dec_in)
    query = (nn(normed_q, w.dec_qkv[:, :DD]) + w.dec_qkv_bias[0]).astype(BF16)
    key = nn(normed_all, w.dec_qkv[:, DD : 2 * DD]).astype(BF16)
    value = (nn(normed_all, w.dec_qkv[:, 2 * DD :]) + w.dec_qkv_bias[1]).astype(BF16)
    attended, lse = attend(query, key, value)
    attended_low = attended.astype(BF16)
    mid = dec_own + (nn(attended_low, w.dec_proj) + dbiases[0])
    normed_d = layer_norm(mid, dnorms[2], dnorms[3]).astype(BF16)
    draised = nn(normed_d, w.dec_up) + w.dec_up_bias
    dactive = gelu(draised).astype(BF16)
    decoded = mid + (nn(dactive, w.dec_down) + dbiases[1])
    head_low = layer_norm(decoded, dnorms[4], dnorms[5]).astype(BF16)
    predicted = nn(head_low, w.pixel_head) + w.head_bias
    target = lax.dynamic_slice_in_dim(rows, y * TUBES + start, OWN, 0).astype(F32)
    target = target - jnp.mean(target, axis=-1, keepdims=True)
    target = target * lax.rsqrt(jnp.mean(target * target, axis=-1, keepdims=True) + PIXEL_EPS)
    hidden = 1.0 - own(visible.astype(F32))
    missing = (predicted - target) * hidden
    loss = jnp.sum((missing * missing).reshape(-1, 8, PATCH // LANES, LANES), axis=(0, 2))
    pred_grad = (2.0 * scale_back * missing).astype(BF16)
    grads, small = Namespace(), Namespace()
    grads.pixel_head = tn(head_low, pred_grad)
    small.head_bias = jnp.sum(pred_grad, axis=0, dtype=F32)
    decoded_grad, dg4, dg5 = norm_back(decoded, dnorms[4], nt(pred_grad, w.pixel_head))
    branch = decoded_grad.astype(BF16)
    grads.dec_down = tn(dactive, branch)
    db1 = jnp.sum(branch, axis=0, dtype=F32)
    draised_grad = (nt(branch, w.dec_down) * gelu_slope(draised)).astype(BF16)
    grads.dec_up = tn(normed_d, draised_grad)
    dec_up_bias = jnp.sum(draised_grad, axis=0, dtype=F32)
    back, dg2, dg3 = norm_back(mid, dnorms[2], nt(draised_grad, w.dec_up))
    mid_grad = decoded_grad + back
    branch = mid_grad.astype(BF16)
    grads.dec_proj = tn(attended_low, branch)
    db0 = jnp.sum(branch, axis=0, dtype=F32)
    attended_grad = nt(branch, w.dec_proj).astype(BF16)
    query_grad, key_grad, value_grad = attend_back(query, key, value, attended_grad, attended, lse)

    def shared(total):
        keep = lax.dynamic_slice_in_dim(total, start, OWN, 0)
        give = lax.dynamic_slice_in_dim(total, OWN - start, OWN, 0).astype(BF16)
        return (keep + beside(give).astype(F32)).astype(BF16)

    mixed = jnp.concatenate([query_grad, shared(key_grad), shared(value_grad)], axis=1)
    grads.dec_qkv = tn(normed_q, mixed)
    dqb = jnp.sum(mixed, axis=0, dtype=F32)
    small.dec_qkv_bias = jnp.concatenate([dqb[:DD], dqb[2 * DD :]])
    back, dg0, dg1 = norm_back(dec_own, dnorms[0], nt(mixed, w.dec_qkv))
    in_grad = mid_grad + back
    small.mask_token = jnp.sum(in_grad * hidden, axis=0)
    part = tn(own(select).astype(BF16), in_grad.astype(BF16)).astype(BF16)
    near = lax.ppermute(part, TENSOR, [(1, 0), (2, 3)])
    joined = part + near
    far = lax.ppermute(joined, TENSOR, [(0, 2), (3, 1)])
    lowered_grad = jnp.where(y == c, joined, far)
    grads.to_decoder = tn(final_low, lowered_grad) * first_y
    encoded_grad, eg4, eg5 = norm_back(encoded, norms[4], nt(lowered_grad, w.to_decoder))
    branch = encoded_grad.astype(BF16)
    grads.enc_down = tn(active, branch)
    eb1 = jnp.sum(branch, axis=0, dtype=F32)
    raised_grad = (nt(branch, w.enc_down) * gelu_slope(raised)).astype(BF16)
    grads.enc_up = tn(normed_m, raised_grad)
    enc_up_bias = jnp.sum(raised_grad, axis=0, dtype=F32)
    back, eg2, eg3 = norm_back(after, norms[2], y_total(nt(raised_grad, w.enc_up)))
    after_grad = encoded_grad + back
    branch = after_grad.astype(BF16)
    grads.enc_proj = tn(merged, branch)
    eb0 = jnp.sum(branch, axis=0, dtype=F32)
    merged_grad = nt(branch, w.enc_proj).astype(BF16).reshape(VP, 6, HEAD).transpose(1, 0, 2)
    v_grad = jnp.einsum("hqk,hqe->hke", probs_low, merged_grad, preferred_element_type=F32).astype(BF16)
    probs_grad = jnp.einsum("hqe,hke->hqk", merged_grad, v, preferred_element_type=F32)
    scores_low = (probs * (probs_grad - jnp.sum(probs_grad * probs, axis=-1, keepdims=True))).astype(BF16)
    q_grad = (jnp.einsum("hqk,hke->hqe", scores_low, k, preferred_element_type=F32) * SCALE).astype(BF16)
    k_grad = (jnp.einsum("hqk,hqe->hke", scores_low, q, preferred_element_type=F32) * SCALE).astype(BF16)
    emixed = heads_back([q_grad, k_grad, v_grad])
    wide_mixed = jnp.pad(emixed.reshape(VP, 2, 576), ((0, 0), (0, 0), (0, 64))).reshape(VP, 1280)
    grads.enc_qkv = tn(normed_a, wide_mixed)
    eqb = jnp.sum(emixed, axis=0, dtype=F32).reshape(2, 3, 192)
    back, eg0, eg1 = norm_back(embedded, norms[0], y_total(nt(emixed, qkv_w)))
    embedded_low = (after_grad + back).astype(BF16)
    grads.embedding = tn(lax.dynamic_slice_in_dim(seen_pixels, y * 768, 768, 1), embedded_low)
    embedding_bias = jnp.sum(embedded_low, axis=0, dtype=F32)
    small_a = jnp.concatenate([embedding_bias, eg0, eg1, eg2, eg3, eg4, eg5, eb0, eb1]) * first_y
    small_b = jnp.concatenate([small.mask_token, dg0, dg1, dg2, dg3, dg4, dg5, db0, db1])
    tiles = []
    for piece in (small_a, small_b, small.dec_qkv_bias, small.head_bias):
        count = piece.shape[0] // LANES
        tiles.append(jnp.pad(piece.reshape(count, LANES), ((0, -count % 8), (0, 0))))
    bias = jnp.concatenate(
        [jnp.pad(eqb[:, ::2].reshape(2, 3, LANES), ((0, 0), (0, 5), (0, 0))), jnp.pad(enc_up_bias.reshape(2, 6, LANES), ((0, 0), (0, 2), (0, 0)))], axis=1)
    dbias = jnp.pad(dec_up_bias.reshape(4, 3, LANES), ((0, 0), (0, 5), (0, 0)))
    return loss, grads, jnp.concatenate(tiles), bias, dbias


def adamw(master, first, second, gradient):
    first_new = BETA_FIRST * first + (1.0 - BETA_FIRST) * gradient
    second_new = BETA_SECOND * second + (1.0 - BETA_SECOND) * gradient * gradient
    first_hat = first_new / (1.0 - BETA_FIRST**STEP)
    second_hat = second_new / (1.0 - BETA_SECOND**STEP)
    master_new = master - LEARN_RATE * (first_hat / (jnp.sqrt(second_hat) + ADAM_EPS) + DECAY_RATE * master)
    return (master_new, first_new, second_new, master_new.astype(BF16))


def shards(tubes, tube_order, common_master, common_first, common_second, split_master, split_first, split_second):
    groups = lax.axis_size(DP)
    cplan = Plan(groups, common_master.shape[0], 64)
    splan = Plan(groups, split_master.shape[1], TILE)
    masked_total = tubes.shape[0] * groups * (TUBES - VIS)
    pixel_count = masked_total * PATCH
    seen_pixels, places = seen_inputs(tubes, tube_order)
    w, saved = gather_weights(common_master, split_master, seen_pixels, places, cplan, splan)
    loss, grads, small, bias, dbias = step_grads(tubes, tube_order, seen_pixels, w, saved, 1.0 / pixel_count)
    g_split, g_common, sums = reduce_grads(grads, small, bias, dbias, loss, cplan, splan)
    loss_mean = jnp.sum(sums[8:]) / pixel_count
    grad_norm = jnp.sqrt(jnp.sum(sums[:8]))
    factor = jnp.minimum(1.0, CLIP_RATIO / math.sqrt(masked_total) / (grad_norm + 1e-06))
    common = adamw(common_master, common_first, common_second, g_common.reshape(-1)[: common_master.shape[0]] * factor)
    split = adamw(split_master, split_first, split_second, g_split.reshape(1, -1)[:, : split_master.shape[1]] * factor)
    return (loss_mean.reshape(1), grad_norm.reshape(1)) + common + split


def solution(mesh):
    in_specs = (P(DP, None, None), P(DP, None), P(DP), P(DP), P(DP), P(TENSOR, DP), P(TENSOR, DP), P(TENSOR, DP))
    out_specs = (P(), P()) + (P(DP),) * 4 + (P(TENSOR, DP),) * 4
    return jax.shard_map(shards, mesh=mesh, in_specs=in_specs, out_specs=out_specs, check_vma=False)
```

```python
import functools
import math
from types import SimpleNamespace as Namespace

import jax
import jax.numpy as jnp
import numpy as np
from jax import lax
from jax.experimental import pallas as pl
from jax.experimental.pallas import tpu as pltpu
from jax.sharding import PartitionSpec as P

DP = "dp"
TENSOR = "tensor"
D = 768
HEAD = 64
FF = 3072
DD = 384
DFF = 1536
PATCH = 1536
TUBES = 1568
VIS = 157
STEP = 10
LANES = 128
TILE = 16
BLOCK = TILE * LANES
FRONT = 24
MESH = pl.DeviceIdType.MESH
F32 = jnp.float32
BF16 = jnp.bfloat16


def round_up(value, step):
    return -(-value // step) * step


COMMON = dict(
    embedding=(PATCH, D), embedding_bias=(D,), enc_norms=(6, D), enc_biases=(2, D), to_decoder=(D, DD), mask_token=(DD,),
    dec_norms=(6, DD), dec_biases=(2, DD), dec_qkv=(DD, 3 * DD), dec_qkv_bias=(2, DD), dec_proj=(DD, DD), pixel_head=(DD, PATCH),
    head_bias=(PATCH,))
SPLIT = dict(
    enc_qkv=(D, 576), enc_qkv_bias=(2, 192), enc_proj=(192, D), enc_up=(D, 768), enc_up_bias=(768,), enc_down=(768, D),
    dec_up=(DD, 384), dec_up_bias=(384,), dec_down=(384, DD))


def row_table(layout):
    table, at = {}, 0
    for name, shape in layout.items():
        count = math.prod(shape) // LANES
        table[name] = (at, count)
        at += count
    return Namespace(**table)


CROW = row_table(COMMON)
SROW = row_table(SPLIT)
DEC_ROW = SROW.dec_up[0]
SPLIT_ROWS = SROW.dec_down[0] + SROW.dec_down[1]
COMMON_ROWS = CROW.head_bias[0] + CROW.head_bias[1]


class Plan:
    def __init__(self, parts, share, rows_step):
        self.parts, self.share = parts, share
        self.base = [i * share // BLOCK * TILE for i in range(parts)]
        self.rows = round_up(-(-(share + BLOCK - 1) // LANES), rows_step)

    def pieces(self, first, last):
        out = []
        for i in range(self.parts):
            start = self.base[i] + (TILE if i else 0)
            stop = self.base[i + 1] if i + 1 < self.parts else self.base[i] + self.rows
            low, high = max(start, first), min(stop, last)
            if i and first <= self.base[i] < last:
                out.append(("edge", i, self.base[i] - self.base[i - 1], self.base[i], TILE))
            if low < high:
                out.append(("body", i, low - self.base[i], low, high - low))
        return out

    def owners(self, first, last):
        return sorted({i for kind, i, *_ in self.pieces(first, last)} | {i - 1 for kind, i, *_ in self.pieces(first, last) if kind == "edge"})


def align_kernel(scalars, split_in, common_in, split_out, common_out):
    def move(source, target, lanes, rows_down, skip, step):
        def part(row, step):
            lane = lax.broadcasted_iota(jnp.int32, (step, LANES), 1)
            here = source[pl.ds(FRONT - rows_down + skip + row, step), :]
            before = source[pl.ds(FRONT - 1 - rows_down + skip + row, step), :]
            value = jnp.where(lane >= lanes, pltpu.roll(here, lanes, 1), pltpu.roll(before, lanes, 1))
            target[pl.ds(pl.multiple_of(row, TILE), step), :] = value.astype(BF16)

        def body(index, _):
            part(index * step, step)
            return 0

        whole = target.shape[0] // step
        lax.fori_loop(0, whole, body, 0)
        if target.shape[0] % step:
            part(whole * step, target.shape[0] % step)

    move(split_in, split_out, scalars[0], scalars[1], 0, 256)
    move(common_in, common_out, scalars[2], scalars[3], scalars[4], 256)


def aligned(master, plan):
    tail = (plan.rows + 8) * LANES - master.shape[-1]
    return jnp.pad(master, ((0, 0),) * (master.ndim - 1) + ((FRONT * LANES, tail),)).reshape(-1, LANES)


def align(common_master, split_master, cplan, splan):
    me, t = lax.axis_index(DP), lax.axis_index(TENSOR)
    soff = me * splan.share % BLOCK
    coff = me * cplan.share % BLOCK
    quarter = cplan.rows // 4
    scalars = jnp.stack([soff % LANES, soff // LANES, coff % LANES, coff // LANES, t * quarter]).astype(jnp.int32)
    return pl.pallas_call(
        align_kernel,
        out_shape=(jax.ShapeDtypeStruct((splan.rows, LANES), BF16), jax.ShapeDtypeStruct((quarter, LANES), BF16)),
        in_specs=[pl.BlockSpec(memory_space=pltpu.SMEM), pl.BlockSpec(memory_space=pltpu.VMEM), pl.BlockSpec(memory_space=pltpu.VMEM)],
        out_specs=[pl.BlockSpec(memory_space=pltpu.VMEM)] * 2,
        name="align",
    )(scalars, aligned(split_master, splan), aligned(common_master, cplan))


OUTS = Namespace(
    embedding=(PATCH, D), to_decoder=(D, DD), dec_qkv=(DD, 3 * DD), dec_proj=(DD, DD), pixel_head=(DD, PATCH),
    enc_qkv=(2, D, 576), enc_proj=(384, D), enc_up=(D, 1536), enc_down=(1536, D), dec_up=(DD, 1536), dec_down=(1536, DD))
OUT_NAMES = tuple(vars(OUTS))
CMATS = OUT_NAMES[:5]
SMALLS = ((CROW.embedding_bias[0], 54), (CROW.mask_token[0], 27), (CROW.dec_qkv_bias[0], 6), (CROW.head_bias[0], 12))


def copy_rows(pieces, frame, wide, first, chunk=64):
    for kind, part, row, at, count in pieces:
        if kind == "edge":
            wide[pl.ds(at - first, TILE), :] = frame(part)[pl.ds(0, TILE), :].astype(F32) + frame(part - 1)[pl.ds(row, TILE), :].astype(F32)
            continue
        source, whole = frame(part), count // chunk

        def body(index, _, source=source, row=row, at=at):
            wide[pl.ds(pl.multiple_of(at - first + index * chunk, TILE), chunk), :] = source[
                pl.ds(pl.multiple_of(row + index * chunk, TILE), chunk), :
            ].astype(F32)
            return 0

        if whole:
            lax.fori_loop(0, whole, body, 0)
        for rest in range(whole * chunk, count, TILE):
            wide[pl.ds(at - first + rest, TILE), :] = source[pl.ds(row + rest, TILE), :].astype(F32)


def matrix_out(wide, start, rows, width, target, row0, col0, step=64):
    per_row = width // LANES

    def body(index, _):
        at = index * step
        for j in range(per_row):
            value = wide[pl.ds(start + j + at * per_row, step, stride=per_row), :]
            target[pl.ds(pl.multiple_of(row0 + at, TILE), step), col0 + j * LANES : col0 + (j + 1) * LANES] = value.astype(BF16)
        return 0

    lax.fori_loop(0, rows // step, body, 0)


def qkv_out(wide, start, pair_buf, target):
    step = 32
    lane = lax.broadcasted_iota(jnp.int32, (step, LANES), 1)

    def body(index, _):
        at = start + index * step * 9
        for j in range(5):
            even = wide[pl.ds(at + j, step, stride=9), :]
            low = pltpu.roll(wide[pl.ds(at + 4 + j, step, stride=9), :], 64, 1)
            if j < 4:
                high = pltpu.roll(wide[pl.ds(at + 5 + j, step, stride=9), :], 64, 1)
                odd = jnp.where(lane < 64, low, high)
            else:
                odd = low
            pair_buf[j, pl.ds(0, step, stride=2), :] = even
            pair_buf[j, pl.ds(1, step, stride=2), :] = odd
            both = pair_buf[j].astype(BF16)
            rows = pl.ds(pl.multiple_of(index * 64, 64), 64)
            if j < 4:
                target[rows, j * LANES : (j + 1) * LANES] = both
            else:
                target[rows, 512:576] = both[:, :64]
        return 0

    lax.fori_loop(0, 12, body, 0)


def floor16(value):
    return value // TILE * TILE


SCALE = HEAD ** (-0.5)


def nt(a, b):
    return lax.dot_general(a, b, (((1,), (1,)), ((), ())), preferred_element_type=F32)


def nn(a, b):
    return lax.dot_general(a, b, (((1,), (0,)), ((), ())), preferred_element_type=F32)


def tn(a, b):
    return lax.dot_general(a, b, (((0,), (0,)), ((), ())), preferred_element_type=F32)


VP = 160
SAVED = Namespace(
    embedded=((VP, D), F32), normed_a=((VP, D), BF16), mixed=((2, VP, 576), BF16), probs=((6, VP, VP), F32), merged=((VP, 384), BF16),
    after=((VP, D), F32), normed_m=((VP, D), BF16), raised=((VP, 1536), F32), active=((VP, 1536), BF16), encoded=((VP, D), F32),
    final_low=((VP, D), BF16), lowered=((VP, DD), F32))
NSAVED = len(vars(SAVED))
SMALL_AT = []
for _, _count in SMALLS:
    SMALL_AT.append(sum(round_up(count, 8) for _, count in SMALLS[: len(SMALL_AT)]))


def norm_rows(inputs, gain, shift):
    centered = inputs - jnp.mean(inputs, axis=-1, keepdims=True)
    spread = jnp.mean(centered * centered, axis=-1, keepdims=True)
    return centered * lax.rsqrt(spread + 1e-06) * gain + shift


def unpacker(cplan, splan, common_frame, split_frame, dec_frame, stage, small_ref, bias_ref, dbias_ref, wide, pair_buf, done):
    def load(plan, frame, start, count):
        first, last = floor16(start), round_up(start + count, TILE)
        copy_rows(plan.pieces(first, last), frame, wide, first)
        return start - first

    def split(c):
        frame = functools.partial(split_frame, c)
        start, count = SROW.enc_qkv
        qkv_out(wide, load(splan, frame, start, count), pair_buf, stage.enc_qkv.at[c])
        at = load(splan, frame, *SROW.enc_qkv_bias)
        bias_ref[c, 0:8, :] = wide[pl.ds(at, 8), :]
        at = load(splan, frame, *SROW.enc_proj)
        matrix_out(wide, at, 192, D, stage.enc_proj, c * 192, 0)
        at = load(splan, frame, *SROW.enc_up)
        matrix_out(wide, at, D, 768, stage.enc_up, 0, c * 768)
        at = load(splan, frame, *SROW.enc_up_bias)
        bias_ref[c, 8:16, :] = wide[pl.ds(at, 8), :]
        at = load(splan, frame, *SROW.enc_down)
        matrix_out(wide, at, 768, D, stage.enc_down, c * 768, 0)
        if c:
            for whole in (stage.enc_qkv, stage.enc_proj, stage.enc_up, stage.enc_down):
                done(whole)

    def common(name):
        at = load(cplan, common_frame, *vars(CROW)[name])
        rows, width = vars(OUTS)[name]
        matrix_out(wide, at, rows, width, vars(stage)[name], 0, 0)
        if name != CMATS[0]:
            done(vars(stage)[name])

    def smalls():
        for small_at, (start, count) in zip(SMALL_AT, SMALLS):
            at = load(cplan, common_frame, start, count)
            small_ref[pl.ds(small_at, round_up(count, 8)), :] = wide[pl.ds(at, round_up(count, 8)), :]

    def dec():
        for slot in range(4):
            frame = functools.partial(split_frame, slot) if slot < 2 else functools.partial(dec_frame, slot - 2)
            at = load(splan, frame, DEC_ROW, SPLIT_ROWS - DEC_ROW)
            matrix_out(wide, at, DD, 384, stage.dec_up, 0, slot * 384)
            bias = at + SROW.dec_up_bias[0] - DEC_ROW
            dbias_ref[slot, :, :] = wide[pl.ds(bias, 8), :]
            matrix_out(wide, bias + 3, 384, DD, stage.dec_down, slot * 384, 0)
        done(stage.dec_up)
        done(stage.dec_down)

    return split, common, smalls, dec


def row_of(ref, at, count):
    return jnp.concatenate([ref[at + k : at + k + 1, :] for k in range(count)], axis=1)


def embed(pix, pos, stage, small_ref, saved):
    saved.embedded[...] = nn(pix[...], stage.embedding[...]) + row_of(small_ref, 0, 6) + pos[...]


def encode(stage, small_ref, bias_ref, saved, swap, while_first, while_second):
    def norm(k):
        return row_of(small_ref, 6 + 6 * k, 6)

    embedded = saved.embedded[...]
    normed = norm_rows(embedded, norm(0), norm(1)).astype(BF16)
    saved.normed_a[...] = normed
    keys = lax.broadcasted_iota(jnp.int32, (VP, VP), 1) < VIS
    outs = []
    for slot in range(2):
        flat = row_of(bias_ref.at[slot], 0, 3)
        bias = jnp.concatenate([flat[:, :192], jnp.zeros((1, 192), F32), flat[:, 192:]], axis=1)
        saved.mixed[slot] = (nn(normed, stage.enc_qkv[slot]) + bias).astype(BF16)
        for head in range(3):
            q, k, v = [saved.mixed[slot, :, 192 * n + HEAD * head : 192 * n + HEAD * (head + 1)] for n in range(3)]
            scores = jnp.where(keys, nt(q, k) * SCALE, -1e30)
            shifted = jnp.exp(scores - jnp.max(scores, axis=1, keepdims=True))
            probs = shifted / jnp.sum(shifted, axis=1, keepdims=True)
            saved.probs[slot * 3 + head] = probs
            outs.append(nn(probs.astype(BF16), v).astype(BF16))
    merged = jnp.concatenate(outs, axis=1)
    saved.merged[...] = merged
    mine, copy, other = swap(0)
    mine[...] = nn(merged, stage.enc_proj[...]).astype(BF16)
    copy.start()
    while_first()
    copy.wait_recv()
    after = embedded + (mine[...].astype(F32) + other[...].astype(F32) + row_of(small_ref, 42, 6))
    saved.after[...] = after
    normed = norm_rows(after, norm(2), norm(3)).astype(BF16)
    saved.normed_m[...] = normed
    up_bias = jnp.concatenate([row_of(bias_ref.at[slot], 8, 6) for slot in range(2)], axis=1)
    for col in range(0, 1536, 384):
        raised = nn(normed, stage.enc_up[:, col : col + 384]) + up_bias[:, col : col + 384]
        saved.raised[:, col : col + 384] = raised
        saved.active[:, col : col + 384] = (0.5 * raised * (1.0 + lax.erf(raised * math.sqrt(0.5)))).astype(BF16)
    mine, second, other = swap(1)
    mine[...] = nn(saved.active[...], stage.enc_down[...]).astype(BF16)
    second.start()
    while_second()
    second.wait_recv()
    encoded = saved.after[...] + (mine[...].astype(F32) + other[...].astype(F32) + row_of(small_ref, 48, 6))
    saved.encoded[...] = encoded
    saved.final_low[...] = norm_rows(encoded, norm(4), norm(5)).astype(BF16)
    copy.wait_send()
    second.wait_send()


def unpack_and_encode(cplan, splan, refs, ready):
    pix, pos, outs, smalls, saved, (sbuf, dbuf, cbuf, wide, pair_buf), stages, out_sem, (swaps, moved, send, recv) = refs
    t = lax.axis_index(TENSOR)
    y, c = t // 2, t % 2
    me = lax.axis_index(DP)
    fd = first_dec(splan)
    stage = Namespace(**dict(zip(OUT_NAMES, stages)))
    copies = []

    def done(whole):
        index = [ref is whole for ref in stages].index(True)
        copy = pltpu.make_async_copy(whole, outs[index], out_sem.at[index])
        copy.start()
        copies.append(copy)

    split, common, common_smalls, dec = unpacker(
        cplan, splan, lambda i: cbuf.at[i], lambda c, i: sbuf.at[c, i], lambda c, i: dbuf.at[c, i - fd],
        stage, smalls[0], smalls[1], smalls[2], wide, pair_buf, done)

    def swap(n):
        copy = pltpu.make_async_remote_copy(
            src_ref=swaps.at[n, 0], dst_ref=swaps.at[n, 1], send_sem=send.at[n], recv_sem=recv.at[n],
            device_id={DP: me, TENSOR: (1 - y) * 2 + c}, device_id_type=MESH)
        return swaps.at[n, 0], copy, swaps.at[n, 1]

    ready(0)
    common(CMATS[0])
    common_smalls()
    embed(pix, pos, stage, smalls[0], saved)
    ready(1)
    split(0)
    split(1)

    def first():
        common(CMATS[1])
        common(CMATS[2])

    def second():
        common(CMATS[3])
        common(CMATS[4])

    encode(stage, smalls[0], smalls[1], saved, swap, first, second)
    move = pltpu.make_async_remote_copy(
        src_ref=saved.final_low, dst_ref=moved, send_sem=send.at[2], recv_sem=recv.at[2],
        device_id={DP: me, TENSOR: y * 2 + (1 - c)}, device_id_type=MESH)

    @pl.when(y == c)
    def _():
        move.start()

    ready(2)
    dec()

    @pl.when(y == c)
    def _():
        saved.lowered[...] = nn(saved.final_low[...], stage.to_decoder[...])
        move.wait_send()

    @pl.when(y != c)
    def _():
        move.wait_recv()
        saved.lowered[...] = nn(moved[...], stage.to_decoder[...])

    for copy in copies:
        copy.wait()


SMALL_ROWS = sum(round_up(count, 8) for _, count in SMALLS)
GATHERED = tuple(jax.ShapeDtypeStruct(vars(OUTS)[name], BF16) for name in OUT_NAMES) + (
    jax.ShapeDtypeStruct((SMALL_ROWS, LANES), F32), jax.ShapeDtypeStruct((2, 16, LANES), F32), jax.ShapeDtypeStruct((4, 8, LANES), F32),
) + tuple(jax.ShapeDtypeStruct(*pair) for pair in vars(SAVED).values())


def first_dec(splan):
    return splan.owners(floor16(DEC_ROW), round_up(SPLIT_ROWS, TILE))[0]


def unpack_scratch(cplan, splan):
    fd = first_dec(splan)
    return [
        pltpu.VMEM((2, splan.parts, splan.rows, LANES), BF16),
        pltpu.VMEM((2, splan.parts - fd, splan.rows, LANES), BF16),
        pltpu.VMEM((cplan.parts, cplan.rows, LANES), BF16),
        pltpu.VMEM((CROW.embedding[1] + 32, LANES), F32),
        pltpu.VMEM((5, 64, LANES), F32),
    ] + [pltpu.VMEM(vars(OUTS)[name], BF16) for name in OUT_NAMES] + [
        pltpu.SemaphoreType.DMA((len(OUT_NAMES),)), pltpu.VMEM((2, 2, VP, D), BF16), pltpu.VMEM((VP, D), BF16),
        pltpu.SemaphoreType.DMA((3,)), pltpu.SemaphoreType.DMA((3,))]


def shared_refs(refs):
    nout = len(OUT_NAMES)
    pix, pos = refs[:2]
    outs, smalls = refs[2 : nout + 2], refs[nout + 2 : nout + 5]
    saved = Namespace(**dict(zip(vars(SAVED), refs[nout + 5 : nout + 5 + NSAVED])))
    refs = refs[nout + 5 + NSAVED :]
    return (pix, pos, outs, smalls, saved, refs[:5], refs[5 : 5 + nout], refs[5 + nout], refs[6 + nout : 10 + nout]), refs[10 + nout :]


def gather_kernel(cplan, splan, s_own, c_own, *refs):
    shared, (send, recv, local) = shared_refs(refs)
    sbuf, dbuf, cbuf = shared[5][:3]
    me, t = lax.axis_index(DP), lax.axis_index(TENSOR)
    z, x, y, c = me // 2, me % 2, t // 2, t % 2
    ty = (1 - y) * 2 + c
    fd = first_dec(splan)
    quarter = cplan.rows // 4

    def cblock(i, tt):
        return cbuf.at[i, pl.ds(pl.multiple_of(tt * quarter, TILE), quarter)]

    def sblock(i):
        return sbuf.at[c, i]

    zdev = [{DP: (z + k) % 4 * 2 + x, TENSOR: t} for k in range(4)]
    xdev, ydev, kdev = {DP: z * 2 + (1 - x), TENSOR: t}, {DP: me, TENSOR: ty}, {DP: me, TENSOR: y * 2 + (1 - c)}
    barrier = pltpu.get_barrier_semaphore()
    for device in zdev[1:] + [xdev, ydev, kdev]:
        pl.semaphore_signal(barrier, inc=1, device_id=device, device_id_type=MESH)
    own = [pltpu.make_async_copy(s_own, sblock(me), local.at[0]), pltpu.make_async_copy(c_own, cblock(me, t), local.at[1])]
    for copy in own:
        copy.start()
    pl.semaphore_wait(barrier, 6)
    for copy in own:
        copy.wait()

    def remote(source, target, slot, device):
        return pltpu.make_async_remote_copy(
            src_ref=source, dst_ref=target, send_sem=send.at[slot], recv_sem=recv.at[slot], device_id=device, device_id_type=MESH)

    def z_copy(common, down, hop, i):
        block = cblock(i, t) if common else sblock(i)
        return remote(block, block, common * 6 + down * 3 + hop - 1, zdev[3 if down else 1])

    def x_copy(common, i):
        block = cblock(i, t) if common else sblock(i)
        return remote(block, block, 12 + common * 4 + i // 2, xdev)

    def y_copy(i):
        return remote(cblock(i, t), cblock(i, t), 20 + i, ydev)

    def k_copy(i):
        return remote(sblock(i), sblock(i), 28 + i, kdev)

    def k_common(i):
        return remote(cblock(i, t), cblock(i, t), 36 + i, kdev)

    def k_far(i):
        return remote(cblock(i, ty), cblock(i, ty), 44 + i, kdev)

    def dec_rows(i):
        return pl.ds(max(0, DEC_FIRST - splan.base[i]), min(splan.rows, S_WIDE - splan.base[i]) - max(0, DEC_FIRST - splan.base[i]))

    def d_copy(i):
        return remote(sbuf.at[c, i, dec_rows(i)], dbuf.at[c, i - fd, dec_rows(i)], 52 + i - fd, ydev)

    def d_beside(i):
        return remote(dbuf.at[c, i - fd, dec_rows(i)], dbuf.at[c, i - fd, dec_rows(i)], 54 + i - fd, kdev)

    def send_z(common, down, hop):
        i = (z + (hop - 1 if down else 1 - hop)) * 2 + x
        able = jnp.logical_and(z > 0, z + hop - 1 <= 3) if down else jnp.logical_and(z < 3, z - hop + 1 >= 0)
        return i, able

    def pass_on(common, down, hop, action):
        i, able = send_z(common, down, hop)

        @pl.when(able)
        def _():
            action(z_copy(common, down, hop, i))

    def share_c(i):
        x_copy(1, i).start()
        y_copy(i).start()
        k_common(i).start()

    def share_s(i):
        x_copy(0, i).start()
        k_copy(i).start()
        dec_start(i)

    def dec_start(i):
        for known in range(fd, splan.parts):
            @pl.when(i == known)
            def _(known=known):
                d_copy(known).start()

    for common in (1, 0):
        for down in (0, 1):
            pass_on(common, down, 1, lambda copy: copy.start())
    share_c(me)
    share_s(me)
    for hop in (1, 2, 3):
        for common in (1, 0):
            for down in (0, 1):
                i = (z + (hop if down else -hop)) * 2 + x
                here = z + hop <= 3 if down else z >= hop

                @pl.when(here)
                def _(common=common, down=down, hop=hop, i=i):
                    z_copy(common, down, hop, i).wait_recv()
                    if hop < 3:
                        pass_on(common, down, hop + 1, lambda copy: copy.start())
                    if common:
                        share_c(i)
                    else:
                        share_s(i)

    def split_here(zz):
        i = zz * 2 + (1 - x)
        x_copy(0, i).wait_recv()
        k_copy(i).start()
        dec_start(i)

    def ready(stage):
        if stage == 0:
            for zz in range(4):
                i = zz * 2 + (1 - x)
                x_copy(1, i).wait_recv()
                y_copy(i).start()
                k_common(i).start()
            for i in range(8):
                y_copy(i).wait_recv()
                k_far(i).start()
            for i in range(8):
                k_common(i).wait_recv()
                k_far(i).wait_recv()
        if stage == 1:
            for zz in range(4):
                split_here(zz)
            for i in range(8):
                k_copy(i).wait_recv()
        if stage == 2:
            for i in range(fd, splan.parts):
                d_copy(i).wait_recv()
                d_beside(i).start()
            for i in range(fd, splan.parts):
                d_beside(i).wait_recv()

    unpack_and_encode(cplan, splan, shared, ready)
    for hop in (1, 2, 3):
        for common in (1, 0):
            for down in (0, 1):
                pass_on(common, down, hop, lambda copy: copy.wait_send())
    for zz in range(4):
        for common in (1, 0):
            x_copy(common, zz * 2 + x).wait_send()
    for i in range(8):
        for copy in (y_copy(i), k_copy(i), k_common(i), k_far(i)):
            copy.wait_send()
    for i in range(fd, splan.parts):
        d_copy(i).wait_send()
        d_beside(i).wait_send()


def local_unpack_kernel(cplan, splan, s_all, d_all, c_all, *refs):
    shared, (local,) = shared_refs(refs)
    t = lax.axis_index(TENSOR)
    barrier = pltpu.get_barrier_semaphore()
    for other in (t // 2 * 2 + 1 - t % 2, (1 - t // 2) * 2 + t % 2):
        pl.semaphore_signal(barrier, inc=1, device_id={DP: lax.axis_index(DP), TENSOR: other}, device_id_type=MESH)
    copies = [pltpu.make_async_copy(source, target, local.at[k]) for k, (source, target) in enumerate(zip((s_all, d_all, c_all), shared[5][:3]))]
    for copy in copies:
        copy.start()
    for copy in copies:
        copy.wait()
    pl.semaphore_wait(barrier, 2)
    unpack_and_encode(cplan, splan, shared, lambda stage: None)


def gather_weights(common_master, split_master, pix, pos, cplan, splan):
    s_own, c_own = align(common_master, split_master, cplan, splan)
    any_spec = pl.BlockSpec(memory_space=pl.ANY)
    vmem = pl.BlockSpec(memory_space=pltpu.VMEM)
    scratch = unpack_scratch(cplan, splan)
    fd = first_dec(splan)
    out_specs = [any_spec] * len(OUT_NAMES) + [vmem] * (3 + NSAVED)
    params = pltpu.CompilerParams(collective_id=0, has_side_effects=True, vmem_limit_bytes=64000 * 1024)
    if cplan.parts == 8 and splan.parts == 8:
        results = pl.pallas_call(
            functools.partial(gather_kernel, cplan, splan),
            out_shape=GATHERED, in_specs=[vmem] * 4, out_specs=out_specs,
            scratch_shapes=scratch + [pltpu.SemaphoreType.DMA((56,)), pltpu.SemaphoreType.DMA((56,)), pltpu.SemaphoreType.DMA((2,))],
            compiler_params=params, name="gather",
        )(s_own, c_own, pix, pos)
    else:
        y = lax.axis_index(TENSOR) // 2
        s_all = lax.all_gather(lax.all_gather(s_own, DP), TENSOR).reshape(2, 2, splan.parts, splan.rows, LANES)
        c_all = jnp.moveaxis(lax.all_gather(lax.all_gather(c_own, DP), TENSOR), 0, 1).reshape(cplan.parts, cplan.rows, LANES)
        s_mine = lax.dynamic_index_in_dim(s_all, y, 0, False)
        d_other = lax.dynamic_index_in_dim(s_all, 1 - y, 0, False)[:, fd:]
        results = pl.pallas_call(
            functools.partial(local_unpack_kernel, cplan, splan),
            out_shape=GATHERED, in_specs=[any_spec] * 3 + [vmem] * 2, out_specs=out_specs,
            scratch_shapes=scratch + [pltpu.SemaphoreType.DMA((3,))], compiler_params=params, name="unpack",
        )(s_mine, d_other, c_all, pix, pos)
    weights = Namespace(**dict(zip(OUT_NAMES, results)))
    small, bias, dbias = results[len(OUT_NAMES) : len(OUT_NAMES) + 3]
    at = 0
    rows = []
    for _, count in SMALLS:
        rows.append(small[at : at + count])
        at += round_up(count, 8)
    a, b, qkv_rows, head_rows = rows
    weights.embedding_bias = a[:6].reshape(1, D)
    weights.enc_norms = a[6:42].reshape(6, D)
    weights.enc_biases = a[42:54].reshape(2, D)
    weights.mask_token = b[:3].reshape(1, DD)
    weights.dec_norms = b[3:21].reshape(6, DD)
    weights.dec_biases = b[21:27].reshape(2, DD)
    weights.dec_qkv_bias = qkv_rows.reshape(2, DD)
    weights.head_bias = head_rows.reshape(1, PATCH)
    weights.enc_qkv_bias = bias[:, :3].reshape(2, 2, 192)
    weights.enc_up_bias = bias[:, 8:14].reshape(1, 1536)
    weights.dec_up_bias = dbias[:, :3].reshape(1, 1536)
    return weights, Namespace(**dict(zip(vars(SAVED), results[len(OUT_NAMES) + 3 :])))


DEC_FIRST = floor16(DEC_ROW)
S_WIDE = round_up(SPLIT_ROWS, TILE)
C_WIDE = round_up(COMMON_ROWS, TILE)
D_WIDE = S_WIDE - DEC_FIRST
SLOTS = 2


def buffer_rows(plan, wide):
    return max(wide, plan.base[-1] + plan.rows)


def clear(wide, first, last, chunk=64):
    def body(index, _):
        wide[pl.ds(first + index * chunk, chunk), :] = jnp.zeros((chunk, LANES), F32)
        return 0

    whole = (last - first) // chunk
    lax.fori_loop(0, whole, body, 0)
    rest = (last - first) % chunk
    if rest:
        wide[pl.ds(first + whole * chunk, rest), :] = jnp.zeros((rest, LANES), F32)


def matrix_in(wide, start, per_row, stage, rows, width, j0, step=64):
    def body(index, _):
        at = index * step
        for j in range(width // LANES):
            wide[pl.ds(start + j0 + j + at * per_row, step, stride=per_row), :] = stage[
                pl.ds(pl.multiple_of(at, 8), step), j * LANES : (j + 1) * LANES
            ]
        return 0

    lax.fori_loop(0, rows // step, body, 0)


def qkv_in(wide, start, pair_buf, stage):
    step = 32
    lane = lax.broadcasted_iota(jnp.int32, (step, LANES), 1)

    def body(index, _):
        at = start + index * step * 9
        even, odd = [], []
        base = pl.multiple_of(index * 64, 8)
        for j in range(5):
            lanes = slice(j * LANES, (j + 1) * LANES) if j < 4 else slice(512, 640)
            pair_buf[j] = stage[pl.ds(base, 64), lanes]
            even.append(pair_buf[j, pl.ds(0, step, stride=2), :])
            odd.append(pltpu.roll(pair_buf[j, pl.ds(1, step, stride=2), :], 64, 1))
        for j in range(4):
            wide[pl.ds(at + j, step, stride=9), :] = even[j]
        wide[pl.ds(at + 4, step, stride=9), :] = jnp.where(lane < 64, even[4], odd[0])
        for j in range(4):
            wide[pl.ds(at + 5 + j, step, stride=9), :] = jnp.where(lane < 64, odd[j], odd[j + 1])
        return 0

    lax.fori_loop(0, 12, body, 0)


def add_rows(target, parts, count, chunk=None):
    chunk = chunk or max(c for c in (128, 64, 48, 32, 16) if count % c == 0)

    def body(index, _):
        at = index * chunk
        total = None
        for ref, start in parts:
            value = ref[pl.ds(pl.multiple_of(start + at, TILE), chunk), :].astype(F32)
            total = value if total is None else total + value
        target[pl.ds(pl.multiple_of(at, TILE), chunk), :] = total.astype(target.dtype)
        return 0

    lax.fori_loop(0, count // chunk, body, 0)


def unalign(source, target, share, offset):
    down, lanes = offset // LANES, offset % LANES
    step = 64
    lane = lax.broadcasted_iota(jnp.int32, (step, LANES), 1)
    row = lax.broadcasted_iota(jnp.int32, (step, LANES), 0)

    def body(index, total):
        at = index * step
        here = pltpu.roll(source[pl.ds(down + at, step), :], LANES - lanes, 1)
        after = pltpu.roll(source[pl.ds(down + at + 1, step), :], LANES - lanes, 1)
        value = jnp.where(lane < LANES - lanes, here, after)
        value = jnp.where((row + at) * LANES + lane < share, value, 0.0)
        target[pl.ds(pl.multiple_of(at, 8), step), :] = value
        square = (value * value).reshape(step // 8, 8, LANES)
        return total + jnp.sum(square, axis=0)

    return lax.fori_loop(0, target.shape[0] // step, body, jnp.zeros((8, LANES), F32))


def flat_rows(share):
    return round_up(-(-share // LANES), 64)


SPLIT_EARLY = round_up(SROW.enc_up[0], TILE)
SPLIT_LATE = floor16(SROW.enc_up[0])
COMMON_EARLY = round_up(CROW.to_decoder[0], TILE)
COMMON_LATE = floor16(CROW.to_decoder[0])
WIDE_ROWS = max(S_WIDE - SPLIT_LATE, C_WIDE - COMMON_LATE)
BACK_WEIGHTS = OUT_NAMES[5:9] + OUT_NAMES[1:2]
LATE_NAMES = OUT_NAMES[2:5] + OUT_NAMES[9:]
KEPT = tuple(vars(SAVED))[:-1]


def norm_rows_back(inputs, gain, grad):
    centered = inputs - jnp.mean(inputs, axis=-1, keepdims=True)
    scale = lax.rsqrt(jnp.mean(centered * centered, axis=-1, keepdims=True) + 1e-06)
    unit = centered * scale
    inner = grad * gain
    back = scale * (inner - jnp.mean(inner, axis=-1, keepdims=True) - unit * jnp.mean(inner * unit, axis=-1, keepdims=True))
    return back, jnp.sum(grad * unit, axis=0, keepdims=True), jnp.sum(grad, axis=0, keepdims=True)


def value_in(wide, start, per_row, value, j0=0):
    rows = value.shape[0]
    for j in range(value.shape[1] // LANES):
        wide[pl.ds(start + j0 + j, rows, stride=per_row), :] = value[:, j * LANES : (j + 1) * LANES]


def row_in(wide, start, value):
    for j in range(value.shape[1] // LANES):
        wide[start + j : start + j + 1, :] = value[:, j * LANES : (j + 1) * LANES]


def narrow_part(wide, at, target, row, count, chunk=128):
    def body(index, _):
        target[pl.ds(pl.multiple_of(row + index * chunk, TILE), chunk), :] = wide[pl.ds(pl.multiple_of(at + index * chunk, TILE), chunk), :].astype(BF16)
        return 0

    whole = count // chunk
    lax.fori_loop(0, whole, body, 0)
    rest = count % chunk
    if rest:
        target[row + whole * chunk : row + count, :] = wide[at + whole * chunk : at + count, :].astype(BF16)


def back_and_pack(refs, hooks):
    (grads, part, seen, norms, small, dbias, weights, saved, wide, pair_buf, stage, stage_sem, gs, gd, gc, held,
     wq, wp, wu, wd, wt, weight_sem, raised_grad, mixed_grad, deep, swaps, joined, near, send, recv) = refs
    t = lax.axis_index(TENSOR)
    me = lax.axis_index(DP)
    y, c = t // 2, t % 2
    first_y = jnp.where(y == 0, 1.0, 0.0)
    ydev, kdev = {DP: me, TENSOR: (1 - y) * 2 + c}, {DP: me, TENSOR: y * 2 + (1 - c)}
    grad = Namespace(**dict(zip(LATE_NAMES, grads)))
    loads = [pltpu.make_async_copy(source, target, weight_sem.at[n]) for n, (source, target) in enumerate(zip(weights, (wq, wp, wu, wd, wt)))]
    for copy in loads:
        copy.start()

    def matrix(source, rows, width, per_row, start, j0=0):
        return (lambda here: matrix_in(wide, start, per_row, here, rows, width, j0), source, rows, width)

    def small_rows(source, start):
        def action():
            wide[pl.ds(start, source.shape[0]), :] = source[...]

        return (action,)

    def columns(slot, width):
        return pl.ds(pl.multiple_of(slot * width, LANES), width)

    def rows_of(slot, count):
        return pl.ds(pl.multiple_of(slot * count, 8), count)

    def dec_part(slot, first):
        return [
            matrix(grad.dec_up.at[:, columns(slot, 384)], DD, 384, 3, SROW.dec_up[0] - first),
            small_rows(dbias.at[slot, pl.ds(0, 3)], SROW.dec_up_bias[0] - first),
            matrix(grad.dec_down.at[rows_of(slot, 384)], 384, DD, 3, SROW.dec_down[0] - first),
            (functools.partial(clear, wide, SPLIT_ROWS - first, S_WIDE - first),)]

    def dec_jobs(slot):
        return [(lambda: clear(wide, 0, DEC_ROW - DEC_FIRST),)] + dec_part(slot + 2, DEC_FIRST) + [(lambda: narrow_part(wide, 0, gd.at[slot], 0, D_WIDE),)]

    def remote(source, target, slot, device):
        return pltpu.make_async_remote_copy(
            src_ref=source, dst_ref=target, send_sem=send.at[slot], recv_sem=recv.at[slot], device_id=device, device_id_type=MESH)

    def norm(k):
        return jnp.concatenate([norms[6 * k + n : 6 * k + n + 1, :] for n in range(6)], axis=1)

    run_jobs(dec_jobs(1 - c), stage, stage_sem)
    hooks.first()
    to_near, to_far = remote(part, near, 0, kdev), remote(joined, joined, 1, ydev)

    @pl.when(y != c)
    def _():
        to_near.start()

    run_jobs(dec_jobs(c), stage, stage_sem)

    @pl.when(y == c)
    def _():
        to_near.wait_recv()
        joined[...] = part[...] + near[...]
        to_far.start()

    for copy in loads:
        copy.wait()

    @pl.when(y != c)
    def _():
        to_far.wait_recv()

    lowered_grad = joined[...]
    encoded_grad, eg4, eg5 = norm_rows_back(saved.encoded[...], norm(4), nt(lowered_grad, wt[...]))
    deep[0] = encoded_grad
    branch = encoded_grad.astype(BF16)
    eb1 = jnp.sum(branch.astype(F32), axis=0, keepdims=True)
    for col in range(0, 1536, 384):
        raised = saved.raised[:, col : col + 384]
        slope = 0.5 * (1.0 + lax.erf(raised * math.sqrt(0.5))) + raised * jnp.exp(-0.5 * raised * raised) * (1.0 / math.sqrt(2.0 * math.pi))
        raised_grad[:, col : col + 384] = (nt(branch, wd[col : col + 384, :]) * slope).astype(BF16)
    swaps[0, 0] = nt(raised_grad[...], wu[...]).astype(BF16)
    swap = remote(swaps.at[0, 0], swaps.at[0, 1], 2, ydev)
    swap.start()
    base = SPLIT_LATE
    for away in (True, False):
        slot = 1 - c if away else c
        cols = columns(slot, 768)
        value_in(wide, SROW.enc_down[0] - base, 6, tn(saved.active[:, cols], branch))
        here = raised_grad[:, cols]
        value_in(wide, SROW.enc_up[0] - base, 6, tn(saved.normed_m[...], here))
        row_in(wide, SROW.enc_up_bias[0] - base, jnp.sum(here.astype(F32), axis=0, keepdims=True))
        run_jobs(dec_part(slot, base), stage, stage_sem)
        held[slot] = wide[0:TILE, :]
        narrow_part(wide, SPLIT_EARLY - base, gs.at[slot], SPLIT_EARLY, S_WIDE - SPLIT_EARLY)
        (hooks.early_away if away else hooks.early_own)()
    swap.wait_recv()
    back, eg2, eg3 = norm_rows_back(saved.after[...], norm(2), swaps[0, 0].astype(F32) + swaps[0, 1].astype(F32))
    after_grad = deep[0] + back
    deep[0] = after_grad
    branch = after_grad.astype(BF16)
    eb0 = jnp.sum(branch.astype(F32), axis=0, keepdims=True)
    merged_grad = nt(branch, wp[...]).astype(BF16)
    total = None
    for slot in range(2):
        pieces = [[], [], []]
        for head in range(3):
            q, k, v = [saved.mixed[slot, :, 192 * n + HEAD * head : 192 * n + HEAD * (head + 1)] for n in range(3)]
            index = slot * 3 + head
            do = merged_grad[:, index * HEAD : (index + 1) * HEAD]
            probs = saved.probs[index]
            pieces[2].append(tn(probs.astype(BF16), do).astype(BF16))
            dp = nt(do, v)
            ds = (probs * (dp - jnp.sum(dp * probs, axis=1, keepdims=True))).astype(BF16)
            pieces[0].append((nn(ds, k) * SCALE).astype(BF16))
            pieces[1].append((tn(ds, q) * SCALE).astype(BF16))
        mixed = jnp.concatenate([piece for group in pieces for piece in group] + [jnp.zeros((VP, 64), BF16)], axis=1)
        mixed_grad[slot] = mixed
        value = nt(mixed[:, :576], wq[slot])
        total = value if total is None else total + value
    swaps[1, 0] = total.astype(BF16)
    second = remote(swaps.at[1, 0], swaps.at[1, 1], 3, ydev)
    second.start()
    for away in (True, False):
        slot = 1 - c if away else c
        here = mixed_grad[slot]
        stage[0, :, 0:640] = tn(saved.normed_a[...], here)
        qkv_in(wide, SROW.enc_qkv[0], pair_buf, stage.at[0])
        sums = jnp.sum(here.astype(F32), axis=0, keepdims=True)
        row_in(wide, SROW.enc_qkv_bias[0], jnp.concatenate([sums[:, :192], sums[:, 384:576]], axis=1))
        wide[SPLIT_LATE:SPLIT_EARLY, :] = held[slot]
        mine = jnp.where(slot == 0, saved.merged[:, :192], saved.merged[:, 192:])
        value_in(wide, SROW.enc_proj[0], 6, tn(mine, branch))
        narrow_part(wide, 0, gs.at[slot], 0, SPLIT_EARLY)
        (hooks.late_away if away else hooks.late_own)()
    base = COMMON_LATE
    jobs = []
    at = 0
    for start, count in SMALLS[1:]:
        jobs.append(small_rows(small.at[pl.ds(at, count)], start - base))
        at += round_up(count, 8)
    for name in CMATS[2:]:
        rows, width_all = vars(OUTS)[name]
        for col in range(0, width_all, 768):
            width = min(768, width_all - col)
            jobs.append(matrix(vars(grad)[name].at[:, pl.ds(col, width)], rows, width, width_all // LANES, vars(CROW)[name][0] - base, col // LANES))
    value_in(wide, CROW.to_decoder[0] - base, 3, tn(saved.final_low[...], lowered_grad) * first_y)
    clear(wide, COMMON_ROWS - base, C_WIDE - base)
    run_jobs(jobs, stage, stage_sem)
    held[0] = wide[0:TILE, :]
    narrow_part(wide, COMMON_EARLY - base, gc, COMMON_EARLY, C_WIDE - COMMON_EARLY)
    hooks.common_early()
    second.wait_recv()
    back, eg0, eg1 = norm_rows_back(saved.embedded[...], norm(0), swaps[1, 0].astype(F32) + swaps[1, 1].astype(F32))
    low = (deep[0] + back).astype(BF16)
    half = CROW.embedding[1] // 2

    def zero(index, _):
        wide[pl.ds((1 - y) * half + index * 64, 64), :] = jnp.zeros((64, LANES), F32)
        return 0

    lax.fori_loop(0, half // 64, zero, 0)
    value_in(wide, y * half, 6, tn(seen[...], low))
    wide[COMMON_LATE:COMMON_EARLY, :] = held[0]
    for n, vector in enumerate((jnp.sum(low.astype(F32), axis=0, keepdims=True), eg0, eg1, eg2, eg3, eg4, eg5, eb0, eb1)):
        row_in(wide, CROW.embedding_bias[0] + 6 * n, vector * first_y)
    narrow_part(wide, 0, gc, 0, COMMON_EARLY)
    hooks.common_late()

    @pl.when(y != c)
    def _():
        to_near.wait_send()

    @pl.when(y == c)
    def _():
        to_far.wait_send()

    swap.wait_send()
    second.wait_send()


def run_jobs(jobs, stage, stage_sem):
    loads = [job for job in jobs if len(job) > 1]
    copies = [
        pltpu.make_async_copy(job[1], stage.at[n % SLOTS, pl.ds(0, job[2]), pl.ds(0, job[3])], stage_sem.at[n % SLOTS]) for n, job in enumerate(loads)]
    for copy in copies[: SLOTS - 1]:
        copy.start()
    index = 0
    for job in jobs:
        if len(job) == 1:
            job[0]()
            continue
        if index + SLOTS - 1 < len(copies):
            copies[index + SLOTS - 1].start()
        copies[index].wait()
        job[0](stage.at[index % SLOTS])
        index += 1


def back_refs(refs):
    grads, (part, seen, norms, small, dbias, loss) = refs[: len(LATE_NAMES)], refs[len(LATE_NAMES) : len(LATE_NAMES) + 6]
    refs = refs[len(LATE_NAMES) + 6 :]
    weights, kept, outs = refs[:5], refs[5 : 5 + len(KEPT)], refs[5 + len(KEPT) : 8 + len(KEPT)]
    refs = refs[8 + len(KEPT) :]
    saved = Namespace(**dict(zip(KEPT, kept)))
    return (grads, part, seen, norms, small, dbias, weights, saved) + tuple(refs[:22]), loss, outs, refs[22:]


def back_scratch(gs_rows, gc_rows):
    return [
        pltpu.VMEM((WIDE_ROWS, LANES), F32), pltpu.VMEM((5, 64, LANES), F32), pltpu.VMEM((SLOTS, 768, 768), F32), pltpu.SemaphoreType.DMA((SLOTS,)),
        pltpu.VMEM((2, gs_rows, LANES), BF16), pltpu.VMEM((2, D_WIDE, LANES), BF16), pltpu.VMEM((gc_rows, LANES), BF16),
        pltpu.VMEM((2, TILE, LANES), F32),
    ] + [pltpu.VMEM(vars(OUTS)[name], BF16) for name in BACK_WEIGHTS] + [
        pltpu.SemaphoreType.DMA((5,)), pltpu.VMEM((VP, 1536), BF16), pltpu.VMEM((2, VP, 640), BF16), pltpu.VMEM((1, VP, D), F32),
        pltpu.VMEM((2, 2, VP, D), BF16), pltpu.VMEM((VP, DD), BF16), pltpu.VMEM((VP, DD), BF16), pltpu.SemaphoreType.DMA((4,)), pltpu.SemaphoreType.DMA((4,))]


ZORDER = (2, 3, 0, 1)
SUBS = 4


def reduce_kernel(cplan, splan, *refs):
    back, loss, (g_split, g_common, sums), refs = back_refs(refs)
    wide, gs, gd, gc = back[8], back[12], back[13], back[14]
    (ks, xs, zs, kc, yc, xc, zc, kd, yd, cq, part, send, recv) = refs
    me, t = lax.axis_index(DP), lax.axis_index(TENSOR)
    z, x, y, c = me // 2, me % 2, t // 2, t % 2
    rank = me * 4 + t
    srows, quarter = splan.rows, cplan.rows // 4
    sub = srows // SUBS
    updev, downdev = {DP: (z + 1) % 4 * 2 + x, TENSOR: t}, {DP: (z + 3) % 4 * 2 + x, TENSOR: t}
    xdev, ydev, kdev = {DP: z * 2 + (1 - x), TENSOR: t}, {DP: me, TENSOR: (1 - y) * 2 + c}, {DP: me, TENSOR: y * 2 + (1 - c)}
    others = [(rank + k) % 32 for k in range(1, 32)]
    devices = [{DP: other // 4, TENSOR: other % 4} for other in others]
    barrier = pltpu.get_barrier_semaphore()
    for device in devices:
        pl.semaphore_signal(barrier, inc=1, device_id=device, device_id_type=MESH)

    def remote(source, target, slot, device):
        return pltpu.make_async_remote_copy(
            src_ref=source, dst_ref=target, send_sem=send.at[slot], recv_sem=recv.at[slot], device_id=device, device_id_type=MESH)

    def s_at(i):
        return pl.multiple_of(i * splan.share // BLOCK * TILE, TILE)

    def c_at(i, tt):
        return pl.multiple_of(i * cplan.share // BLOCK * TILE + tt * quarter, TILE)

    def piece(q):
        return pl.ds(pl.multiple_of(q * sub, TILE), sub)

    def kd_copy():
        return remote(gd.at[1 - c], kd, 0, kdev)

    def ks_copy(i):
        return remote(gs.at[1 - c, pl.ds(s_at(i), srows)], ks.at[i], 1 + i, kdev)

    def kc_copy(i, yy):
        return remote(gc.at[pl.ds(c_at(i, 2 * yy + 1 - c), quarter)], kc.at[i, yy], 9 + i * 2 + yy, kdev)

    def yd_copy():
        return remote(kd, yd, 25, ydev)

    def yc_copy(i):
        return remote(kc.at[i, 1 - y], yc.at[i], 26 + i, ydev)

    def xs_copy(zz, q):
        return remote(ks.at[zz * 2 + (1 - x), piece(q)], xs.at[zz, piece(q)], 34 + zz * 4 + q, xdev)

    def xc_copy(zz):
        return remote(yc.at[zz * 2 + (1 - x)], xc.at[zz], 50 + zz, xdev)

    def zs_copy(down, zz, q):
        return remote(xs.at[zz, piece(q)], zs.at[down, zz, piece(q)], 54 + down * 16 + zz * 4 + q, downdev if down else updev)

    def zc_copy(down, zz):
        return remote(xc.at[zz], zc.at[down, zz], 86 + down * 4 + zz, downdev if down else updev)

    def along_z(zz, copy_of, add):
        for down in (0, 1):
            passes = z > zz if down else z < zz
            first = z == 3 if down else z == 0

            @pl.when(jnp.logical_and(passes, first))
            def _():
                add(None)

            @pl.when(jnp.logical_and(passes, jnp.logical_not(first)))
            def _(down=down):
                copy_of(down).wait_recv()
                add(down)

            @pl.when(passes)
            def _(down=down):
                copy_of(down).start()

    def across_x(zz):
        i = zz * 2 + (1 - x)
        ks_copy(i).wait_recv()

        def body(q, _):
            add_rows(ks.at[i, piece(q)], [(ks.at[i, piece(q)], 0), (gs.at[c], s_at(i) + q * sub)], sub)
            xs_copy(zz, q).start()
            return 0

        lax.fori_loop(0, SUBS, body, 0)

    def first():
        pl.semaphore_wait(barrier, 31)
        kd_copy().start()

    def early_away():
        for zz in ZORDER[:2]:
            ks_copy(zz * 2 + (1 - x)).start()
        for zz in ZORDER[:2]:
            ks_copy(zz * 2 + x).start()
        kd_copy().wait_recv()
        add_rows(kd, [(gd.at[c], 0), (kd, 0)], D_WIDE)
        yd_copy().start()

    def early_own():
        across_x(ZORDER[0])
        yd_copy().wait_recv()
        dec_rows = gs.at[c, pl.ds(DEC_FIRST, D_WIDE)]
        add_rows(dec_rows, [(dec_rows, 0), (yd, 0)], D_WIDE)
        across_x(ZORDER[1])

    def late_away():
        for zz in ZORDER[2:]:
            ks_copy(zz * 2 + (1 - x)).start()
        for zz in ZORDER[2:]:
            ks_copy(zz * 2 + x).start()

    def late_own():
        for zz in ZORDER[2:]:
            across_x(zz)

    def common_core_sends(zzs):
        for zz in zzs:
            for xx in (0, 1):
                for yy in (0, 1):
                    kc_copy(zz * 2 + xx, yy).start()

    back_and_pack(back, Namespace(
        first=first, early_away=early_away, early_own=early_own, late_away=late_away, late_own=late_own,
        common_early=lambda: common_core_sends(ZORDER[:2]), common_late=lambda: common_core_sends(ZORDER[2:])))
    fin, finc = wide.at[pl.ds(0, srows + 64)], wide.at[pl.ds(srows + 64, cplan.rows + 64)]
    for zz in ZORDER:
        for xx in (0, 1):
            i = zz * 2 + xx
            for yy in (0, 1):
                kc_copy(i, yy).wait_recv()
            add_rows(kc.at[i, 1 - y], [(gc, c_at(i, 2 * (1 - y) + c)), (kc.at[i, 1 - y], 0)], quarter)
            yc_copy(i).start()
    for zz in ZORDER:
        i = zz * 2 + (1 - x)
        yc_copy(i).wait_recv()
        add_rows(yc.at[i], [(gc, c_at(i, t)), (kc.at[i, y], 0), (yc.at[i], 0)], quarter)
        xc_copy(zz).start()
        i = zz * 2 + x
        ks_copy(i).wait_recv()

        def body(q, _, zz=zz, i=i):
            xs_copy(zz, q).wait_recv()

            def add(flow):
                parts = [(xs.at[zz, piece(q)], 0), (gs.at[c], s_at(i) + q * sub), (ks.at[i, piece(q)], 0)]
                add_rows(xs.at[zz, piece(q)], parts + ([] if flow is None else [(zs.at[flow, zz, piece(q)], 0)]), sub)

            along_z(zz, lambda down: zs_copy(down, zz, q), add)
            return 0

        lax.fori_loop(0, SUBS, body, 0)
    for zz in ZORDER:
        i = zz * 2 + x
        yc_copy(i).wait_recv()
        xc_copy(zz).wait_recv()

        def add_common(flow, zz=zz, i=i):
            parts = [(xc.at[zz], 0), (gc, c_at(i, t)), (kc.at[i, y], 0), (yc.at[i], 0)]
            add_rows(xc.at[zz], parts + ([] if flow is None else [(zc.at[flow, zz], 0)]), quarter)

        along_z(zz, lambda down, zz=zz: zc_copy(down, zz), add_common)

    def ends(copy_of, action):
        for low, high in ((0, 1), (1, 1), (1, 0)):
            here = jnp.logical_and((z > 0) == bool(low), (z < 3) == bool(high))

            @pl.when(here)
            def _(low=low, high=high):
                flows = [0] * low + [1] * high
                for flow in flows:
                    copy_of(flow)
                action(flows)

    mine = pl.ds(pl.multiple_of(t * quarter, TILE), quarter)
    ends(
        lambda flow: zc_copy(flow, z).wait_recv(),
        lambda flows: add_rows(
            cq.at[mine], [(xc.at[z], 0), (gc, c_at(me, t)), (kc.at[me, y], 0), (yc.at[me], 0)] + [(zc.at[flow, z], 0) for flow in flows], quarter))
    far = pl.ds(pl.multiple_of(((1 - y) * 2 + c) * quarter, TILE), quarter)
    across_t, beside_t, beside_far = remote(cq.at[mine], cq.at[mine], 94, ydev), remote(cq.at[mine], cq.at[mine], 95, kdev), remote(cq.at[far], cq.at[far], 96, kdev)
    across_t.start()
    beside_t.start()

    def wait_split(flow):
        for q in range(SUBS):
            zs_copy(flow, z, q).wait_recv()

    ends(
        wait_split,
        lambda flows: add_rows(fin, [(xs.at[z], 0), (gs.at[c], s_at(me)), (ks.at[me], 0)] + [(zs.at[flow, z], 0) for flow in flows], srows))
    across_t.wait_recv()
    beside_far.start()
    squares = unalign(fin, g_split, splan.share, me * splan.share % BLOCK)
    beside_t.wait_recv()
    beside_far.wait_recv()
    add_rows(finc, [(cq, 0)], cplan.rows)
    squares += unalign(finc, g_common, cplan.share, me * cplan.share % BLOCK) * 0.25
    part[rank, 0:8, :] = squares
    part[rank, 8:16, :] = loss[...]
    shared = [remote(part.at[rank], part.at[rank], 97 + k, device) for k, device in enumerate(devices)]
    for copy in shared:
        copy.start()
    kd_copy().wait_send()
    yd_copy().wait_send()
    for i in range(8):
        ks_copy(i).wait_send()
        yc_copy(i).wait_send()
        for yy in range(2):
            kc_copy(i, yy).wait_send()
    for zz in range(4):
        xc_copy(zz).wait_send()
        for q in range(SUBS):
            xs_copy(zz, q).wait_send()
        for down in (0, 1):
            @pl.when(z > zz if down else z < zz)
            def _(down=down, zz=zz):
                zc_copy(down, zz).wait_send()
                for q in range(SUBS):
                    zs_copy(down, zz, q).wait_send()
    for copy in (across_t, beside_t, beside_far):
        copy.wait_send()
    for copy in shared:
        copy.wait_recv()

    def total(index, value):
        return value + part[index]

    sums[...] = lax.fori_loop(0, 32, total, jnp.zeros((16, LANES), F32))
    for copy in shared:
        copy.wait_send()


def pack_kernel(*refs):
    back, _, outs, (out_sem,) = back_refs(refs)
    t = lax.axis_index(TENSOR)
    barrier = pltpu.get_barrier_semaphore()
    for other in (t // 2 * 2 + 1 - t % 2, (1 - t // 2) * 2 + t % 2):
        pl.semaphore_signal(barrier, inc=1, device_id={DP: lax.axis_index(DP), TENSOR: other}, device_id_type=MESH)

    def nothing():
        pass

    back_and_pack(back, Namespace(
        first=lambda: pl.semaphore_wait(barrier, 2), early_away=nothing, early_own=nothing, late_away=nothing, late_own=nothing,
        common_early=nothing, common_late=nothing))
    copies = [pltpu.make_async_copy(a, b, out_sem.at[k]) for k, (a, b) in enumerate(zip(back[12:15], outs))]
    for copy in copies:
        copy.start()
    for copy in copies:
        copy.wait()


def unalign_kernel(share_s, share_c, scalars, s_in, c_in, s_out, c_out, sums):
    sums[...] = unalign(s_in, s_out, share_s, scalars[0]) + unalign(c_in, c_out, share_c, scalars[1]) * 0.25


def reduce_grads(grads, part, seen, norms, small, dbias, loss, w, saved, cplan, splan):
    any_spec, vmem = pl.BlockSpec(memory_space=pl.ANY), pl.BlockSpec(memory_space=pltpu.VMEM)
    srows, quarter = splan.rows, cplan.rows // 4
    gs_rows, gc_rows = buffer_rows(splan, S_WIDE), buffer_rows(cplan, C_WIDE)
    flat = (jax.ShapeDtypeStruct((flat_rows(splan.share), LANES), F32), jax.ShapeDtypeStruct((flat_rows(cplan.share), LANES), F32))
    operands = [vars(grads)[name] for name in LATE_NAMES] + [part, seen, norms, small, dbias, loss]
    operands += [vars(w)[name] for name in BACK_WEIGHTS] + [vars(saved)[name] for name in KEPT]
    in_specs = [any_spec] * len(LATE_NAMES) + [vmem] * 6 + [any_spec] * 5 + [vmem] * len(KEPT)
    scratch = back_scratch(gs_rows, gc_rows)
    params = pltpu.CompilerParams(collective_id=1, has_side_effects=True, vmem_limit_bytes=67_000_000)
    if cplan.parts == 8 and splan.parts == 8:
        def rows(*shape, kind=BF16):
            return pltpu.VMEM(shape + (LANES,), kind)

        return pl.pallas_call(
            functools.partial(reduce_kernel, cplan, splan),
            out_shape=flat + (jax.ShapeDtypeStruct((16, LANES), F32),), in_specs=in_specs, out_specs=[vmem] * 3,
            scratch_shapes=scratch + [
                rows(8, srows), rows(4, srows), rows(2, 4, srows), rows(8, 2, quarter), rows(8, quarter), rows(4, quarter), rows(2, 4, quarter),
                rows(D_WIDE), rows(D_WIDE), rows(cplan.rows), rows(32, 16, kind=F32), pltpu.SemaphoreType.DMA((128,)), pltpu.SemaphoreType.DMA((128,))],
            compiler_params=params, name="reduce",
        )(*operands)
    shapes = [jax.ShapeDtypeStruct((2, gs_rows, LANES), BF16), jax.ShapeDtypeStruct((2, D_WIDE, LANES), BF16), jax.ShapeDtypeStruct((gc_rows, LANES), BF16)]
    gs, gd, gc = pl.pallas_call(
        pack_kernel, out_shape=shapes, in_specs=in_specs, out_specs=[any_spec] * 3,
        scratch_shapes=scratch + [pltpu.SemaphoreType.DMA((3,))], compiler_params=params, name="pack",
    )(*operands)
    me, t = lax.axis_index(DP), lax.axis_index(TENSOR)
    c = t % 2

    def swap(value, bit):
        return lax.ppermute(value, TENSOR, [(i, i ^ bit) for i in range(4)])

    def mine(value):
        keep = lax.dynamic_index_in_dim(value, c, 0, False).astype(F32)
        return keep + swap(lax.dynamic_index_in_dim(value, 1 - c, 0, False), 1).astype(F32)

    far = swap(mine(gd).astype(BF16), 2)
    split_sum = mine(gs).at[DEC_FIRST : DEC_FIRST + D_WIDE].add(far.astype(F32))
    common_sum = lax.psum(gc, TENSOR).astype(F32)

    def scattered(value, plan):
        frames = jnp.stack([value[base : base + plan.rows] for base in plan.base])
        return lax.psum_scatter(frames.astype(BF16), DP, scatter_dimension=0, tiled=True)[0].astype(F32)

    s_frame, c_frame = scattered(split_sum, splan), scattered(common_sum, cplan)
    pad = ((0, 64), (0, 0))
    g_split, g_common, squares = pl.pallas_call(
        functools.partial(unalign_kernel, splan.share, cplan.share), out_shape=flat + (jax.ShapeDtypeStruct((8, LANES), F32),),
        in_specs=[pl.BlockSpec(memory_space=pltpu.SMEM), vmem, vmem], out_specs=[vmem] * 3, name="unalign",
    )(jnp.stack([me * splan.share % BLOCK, me * cplan.share % BLOCK]).astype(jnp.int32), jnp.pad(s_frame, pad), jnp.pad(c_frame, pad))
    return g_split, g_common, lax.psum(jnp.concatenate([squares, loss]), (DP, TENSOR))


OWN = TUBES // 2
KEYS = 392


def head_masks(rows):
    lane = lax.broadcasted_iota(jnp.int32, (rows, LANES), 1)
    return lane < HEAD, lane >= HEAD


def attend_kernel(q_ref, k_ref, v_ref, o_ref, lse_ref, vt_ref, shifted_ref):
    q = q_ref[...]
    vt_ref[...] = v_ref[...].T
    pieces = []
    for head, mask in enumerate(head_masks(OWN)):
        qm = jnp.where(mask, q * SCALE, jnp.zeros_like(q))
        top = None
        for first in range(0, TUBES, KEYS):
            most = jnp.max(nt(k_ref[first : first + KEYS, :], qm), axis=0, keepdims=True)
            top = most if top is None else jnp.maximum(top, most)
        total = None
        qm = jnp.where(mask, q, jnp.zeros_like(q))
        for first in range(0, TUBES, KEYS):
            shifted = jnp.exp(nt(k_ref[first : first + KEYS, :], qm) * SCALE - top)
            part = jnp.sum(shifted, axis=0, keepdims=True)
            total = part if total is None else total + part
            shifted_ref[first : first + KEYS, :] = shifted.astype(BF16)
        pieces.append(nn(vt_ref[head * HEAD : (head + 1) * HEAD, :], shifted_ref[...]) / total)
        lse_ref[0, head : head + 1, :] = top + jnp.log(total)
    o_ref[...] = jnp.concatenate(pieces, axis=0).T


def attend(q, k, v):
    block, whole = pl.BlockSpec((OWN, LANES), lambda h: (0, h)), pl.BlockSpec((TUBES, LANES), lambda h: (0, h))
    return pl.pallas_call(
        attend_kernel, grid=(3,),
        out_shape=(jax.ShapeDtypeStruct((OWN, DD), F32), jax.ShapeDtypeStruct((3, 8, OWN), F32)),
        in_specs=[block, whole, whole], out_specs=[block, pl.BlockSpec((1, 8, OWN), lambda h: (h, 0, 0))],
        scratch_shapes=[pltpu.VMEM((LANES, TUBES), BF16), pltpu.VMEM((TUBES, OWN), BF16)], name="attend",
    )(q, k, v)


def attend_back_kernel(q_ref, k_ref, v_ref, do_ref, o_ref, lse_ref, dq_ref, dk_ref, dv_ref, kt_ref, ds_ref):
    q, do = q_ref[...], do_ref[...]
    kt_ref[...] = k_ref[...].T
    along = (do.astype(F32) * o_ref[...]).T
    pieces = []
    for head, mask in enumerate(head_masks(OWN)):
        qm, dom = jnp.where(mask, q * SCALE, jnp.zeros_like(q)), jnp.where(mask, do, jnp.zeros_like(do))
        delta = jnp.sum(along[head * HEAD : (head + 1) * HEAD], axis=0, keepdims=True)
        lse = lse_ref[0, head : head + 1, :]
        for first in range(0, TUBES, KEYS):
            rows = slice(first, first + KEYS)
            probs = jnp.exp(nt(k_ref[rows, :], qm) - lse)
            dv = nn(probs.astype(BF16), dom)
            ds = (probs * (nt(v_ref[rows, :], dom) - delta)).astype(BF16)
            ds_ref[rows, :] = ds
            dk = nn(ds, qm)
            if head:
                dk_ref[rows, :] += dk
                dv_ref[rows, :] += dv
            else:
                dk_ref[rows, :] = dk
                dv_ref[rows, :] = dv
        pieces.append(nn(kt_ref[head * HEAD : (head + 1) * HEAD, :], ds_ref[...]))
    dq_ref[...] = (jnp.concatenate(pieces, axis=0) * SCALE).T.astype(BF16)


def attend_back(q, k, v, do, o, lse):
    block, whole = pl.BlockSpec((OWN, LANES), lambda h: (0, h)), pl.BlockSpec((TUBES, LANES), lambda h: (0, h))
    return pl.pallas_call(
        attend_back_kernel, grid=(3,),
        out_shape=(jax.ShapeDtypeStruct((OWN, DD), BF16), jax.ShapeDtypeStruct((TUBES, DD), F32), jax.ShapeDtypeStruct((TUBES, DD), F32)),
        in_specs=[block, whole, whole, block, block, pl.BlockSpec((1, 8, OWN), lambda h: (h, 0, 0))], out_specs=[block, whole, whole],
        scratch_shapes=[pltpu.VMEM((LANES, TUBES), BF16), pltpu.VMEM((TUBES, OWN), BF16)], name="attend_back",
    )(q, k, v, do, o, lse)


NORM_EPS = 1e-06
PIXEL_EPS = 1e-06
CLIP_RATIO = 1.5
BETA_FIRST = 0.9
BETA_SECOND = 0.95
LEARN_RATE = 0.05
DECAY_RATE = 0.05
ADAM_EPS = 1e-08


def layer_norm(inputs, gain, shift):
    centered = inputs - jnp.mean(inputs, axis=-1, keepdims=True)
    spread = jnp.mean(centered * centered, axis=-1, keepdims=True)
    return centered * lax.rsqrt(spread + NORM_EPS) * gain + shift


def norm_back(inputs, gain, grad):
    centered = inputs - jnp.mean(inputs, axis=-1, keepdims=True)
    scale = lax.rsqrt(jnp.mean(centered * centered, axis=-1, keepdims=True) + NORM_EPS)
    unit = centered * scale
    inner = grad * gain
    back = scale * (inner - jnp.mean(inner, axis=-1, keepdims=True) - unit * jnp.mean(inner * unit, axis=-1, keepdims=True))
    return back, jnp.sum(grad * unit, axis=0), jnp.sum(grad, axis=0)


def gelu(inputs):
    return jax.nn.gelu(inputs, approximate=False)


def gelu_slope(inputs):
    return 0.5 * (1.0 + lax.erf(inputs * math.sqrt(0.5))) + inputs * jnp.exp(-0.5 * inputs * inputs) * (1.0 / math.sqrt(2.0 * math.pi))


def sine_rows(position, width):
    column = jnp.arange(width)
    exponent = (2 * (column // 2)).astype(F32) / width
    angles = position.astype(F32)[:, None] / jnp.power(10000.0, exponent)[None, :]
    return jnp.where((column % 2 == 0)[None, :], jnp.sin(angles), jnp.cos(angles))


def sine_table(width, step=32):
    column = np.arange(width)
    rate = 10000.0 ** (-(2 * (column // 2)) / width)
    high, low = np.arange(0, TUBES, step)[:, None] * rate, np.arange(step)[:, None] * rate
    even = column % 2 == 0
    a = np.where(even, np.sin(high), np.cos(high)).astype(np.float32)
    b = np.where(even, np.cos(high), -np.sin(high)).astype(np.float32)
    c, s = np.cos(low).astype(np.float32), np.sin(low).astype(np.float32)
    table = a[:, None] * jnp.asarray(c)[None] + b[:, None] * jnp.asarray(s)[None]
    return table.reshape(TUBES, width)


def beside(value):
    return lax.ppermute(value, TENSOR, [(i, i ^ 1) for i in range(4)])


def seen_inputs(pixels, order):
    c = lax.axis_index(TENSOR) % 2
    seen = jnp.pad(lax.dynamic_index_in_dim(order, c, 0, False)[:VIS], (0, VP - VIS))
    return jnp.take(pixels.reshape(2 * TUBES, PATCH), c * TUBES + seen, axis=0), sine_rows(seen, D)


def step_grads(pixels, order, w, saved, scale_back):
    t = lax.axis_index(TENSOR)
    y, c = t // 2, t % 2
    seen_y = jnp.pad(lax.dynamic_index_in_dim(order, y, 0, False)[:VIS], (0, VP - VIS), constant_values=-1)
    rows = pixels.reshape(2 * TUBES, PATCH)
    lowered = saved.lowered
    select = seen_y[None, :] == jnp.arange(TUBES, dtype=jnp.int32)[:, None]
    visible = jnp.any(select, axis=1, keepdims=True)
    placed = lax.dot_general(select.astype(F32), lowered, (((1,), (0,)), ((), ())), precision=lax.Precision.HIGHEST, preferred_element_type=F32)
    dec_in = placed + jnp.where(visible, 0.0, w.mask_token) + sine_table(DD)
    start = c * OWN

    def own(value):
        return lax.dynamic_slice_in_dim(value, start, OWN, 0)

    dnorms, dbiases = w.dec_norms, w.dec_biases
    normed_all = layer_norm(dec_in, dnorms[0], dnorms[1]).astype(BF16)
    normed_q = own(normed_all)
    dec_own = own(dec_in)
    query = (nn(normed_q, w.dec_qkv[:, :DD]) + w.dec_qkv_bias[0]).astype(BF16)
    key = nn(normed_all, w.dec_qkv[:, DD : 2 * DD]).astype(BF16)
    value = (nn(normed_all, w.dec_qkv[:, 2 * DD :]) + w.dec_qkv_bias[1]).astype(BF16)
    attended, lse = attend(query, key, value)
    attended_low = attended.astype(BF16)
    mid = dec_own + (nn(attended_low, w.dec_proj) + dbiases[0])
    normed_d = layer_norm(mid, dnorms[2], dnorms[3]).astype(BF16)
    draised = nn(normed_d, w.dec_up) + w.dec_up_bias
    dactive = gelu(draised).astype(BF16)
    decoded = mid + (nn(dactive, w.dec_down) + dbiases[1])
    head_low = layer_norm(decoded, dnorms[4], dnorms[5]).astype(BF16)
    predicted = nn(head_low, w.pixel_head) + w.head_bias
    target = lax.dynamic_slice_in_dim(rows, y * TUBES + start, OWN, 0).astype(F32)
    target = target - jnp.mean(target, axis=-1, keepdims=True)
    target = target * lax.rsqrt(jnp.mean(target * target, axis=-1, keepdims=True) + PIXEL_EPS)
    hidden = 1.0 - own(visible.astype(F32))
    missing = (predicted - target) * hidden
    loss = jnp.sum((missing * missing).reshape(-1, 8, PATCH // LANES, LANES), axis=(0, 2))
    pred_grad = (2.0 * scale_back * missing).astype(BF16)
    grads, small = Namespace(), Namespace()
    grads.pixel_head = tn(head_low, pred_grad)
    small.head_bias = jnp.sum(pred_grad, axis=0, dtype=F32)
    decoded_grad, dg4, dg5 = norm_back(decoded, dnorms[4], nt(pred_grad, w.pixel_head))
    branch = decoded_grad.astype(BF16)
    grads.dec_down = tn(dactive, branch)
    db1 = jnp.sum(branch, axis=0, dtype=F32)
    draised_grad = (nt(branch, w.dec_down) * gelu_slope(draised)).astype(BF16)
    grads.dec_up = tn(normed_d, draised_grad)
    dec_up_bias = jnp.sum(draised_grad, axis=0, dtype=F32)
    back, dg2, dg3 = norm_back(mid, dnorms[2], nt(draised_grad, w.dec_up))
    mid_grad = decoded_grad + back
    branch = mid_grad.astype(BF16)
    grads.dec_proj = tn(attended_low, branch)
    db0 = jnp.sum(branch, axis=0, dtype=F32)
    attended_grad = nt(branch, w.dec_proj).astype(BF16)
    query_grad, key_grad, value_grad = attend_back(query, key, value, attended_grad, attended, lse)

    def shared(total):
        keep = lax.dynamic_slice_in_dim(total, start, OWN, 0)
        give = lax.dynamic_slice_in_dim(total, OWN - start, OWN, 0).astype(BF16)
        return (keep + beside(give).astype(F32)).astype(BF16)

    mixed = jnp.concatenate([query_grad, shared(key_grad), shared(value_grad)], axis=1)
    grads.dec_qkv = tn(normed_q, mixed)
    dqb = jnp.sum(mixed, axis=0, dtype=F32)
    small.dec_qkv_bias = jnp.concatenate([dqb[:DD], dqb[2 * DD :]])
    back, dg0, dg1 = norm_back(dec_own, dnorms[0], nt(mixed, w.dec_qkv))
    in_grad = mid_grad + back
    small.mask_token = jnp.sum(in_grad * hidden, axis=0)
    part = tn(own(select).astype(BF16), in_grad.astype(BF16)).astype(BF16)
    small_b = jnp.concatenate([small.mask_token, dg0, dg1, dg2, dg3, dg4, dg5, db0, db1])
    tiles = []
    for piece in (small_b, small.dec_qkv_bias, small.head_bias):
        count = piece.shape[0] // LANES
        tiles.append(jnp.pad(piece.reshape(count, LANES), ((0, -count % 8), (0, 0))))
    dbias = jnp.pad(dec_up_bias.reshape(4, 3, LANES), ((0, 0), (0, 5), (0, 0)))
    return loss, grads, part, jnp.concatenate(tiles), dbias


def adamw(master, first, second, gradient):
    first_new = BETA_FIRST * first + (1.0 - BETA_FIRST) * gradient
    second_new = BETA_SECOND * second + (1.0 - BETA_SECOND) * gradient * gradient
    first_hat = first_new / (1.0 - BETA_FIRST**STEP)
    second_hat = second_new / (1.0 - BETA_SECOND**STEP)
    master_new = master - LEARN_RATE * (first_hat / (jnp.sqrt(second_hat) + ADAM_EPS) + DECAY_RATE * master)
    return (master_new, first_new, second_new, master_new.astype(BF16))


def shards(tubes, tube_order, common_master, common_first, common_second, split_master, split_first, split_second):
    groups = lax.axis_size(DP)
    cplan = Plan(groups, common_master.shape[0], 64)
    splan = Plan(groups, split_master.shape[1], TILE)
    masked_total = tubes.shape[0] * groups * (TUBES - VIS)
    pixel_count = masked_total * PATCH
    seen_pixels, places = seen_inputs(tubes, tube_order)
    w, saved = gather_weights(common_master, split_master, seen_pixels, places, cplan, splan)
    loss, grads, part, small, dbias = step_grads(tubes, tube_order, w, saved, 1.0 / pixel_count)
    half = lax.dynamic_slice_in_dim(seen_pixels, lax.axis_index(TENSOR) // 2 * 768, 768, 1)
    g_split, g_common, sums = reduce_grads(grads, part, half, w.enc_norms.reshape(36, LANES), small, dbias, loss, w, saved, cplan, splan)
    loss_mean = jnp.sum(sums[8:]) / pixel_count
    grad_norm = jnp.sqrt(jnp.sum(sums[:8]))
    factor = jnp.minimum(1.0, CLIP_RATIO / math.sqrt(masked_total) / (grad_norm + 1e-06))
    common = adamw(common_master, common_first, common_second, g_common.reshape(-1)[: common_master.shape[0]] * factor)
    split = adamw(split_master, split_first, split_second, g_split.reshape(1, -1)[:, : split_master.shape[1]] * factor)
    return (loss_mean.reshape(1), grad_norm.reshape(1)) + common + split


def solution(mesh):
    in_specs = (P(DP, None, None), P(DP, None), P(DP), P(DP), P(DP), P(TENSOR, DP), P(TENSOR, DP), P(TENSOR, DP))
    out_specs = (P(), P()) + (P(DP),) * 4 + (P(TENSOR, DP),) * 4
    return jax.shard_map(shards, mesh=mesh, in_specs=in_specs, out_specs=out_specs, check_vma=False)
```

```python
import functools
import math
from types import SimpleNamespace as Namespace

import jax
import jax.numpy as jnp
import numpy as np
from jax import lax
from jax.experimental import pallas as pl
from jax.experimental.pallas import tpu as pltpu
from jax.sharding import PartitionSpec as P

DP = "dp"
TENSOR = "tensor"
D = 768
HEAD = 64
FF = 3072
DD = 384
DFF = 1536
PATCH = 1536
TUBES = 1568
VIS = 157
STEP = 10
LANES = 128
TILE = 16
BLOCK = TILE * LANES
FRONT = 24
MESH = pl.DeviceIdType.MESH
F32 = jnp.float32
BF16 = jnp.bfloat16


def round_up(value, step):
    return -(-value // step) * step


COMMON = dict(
    embedding=(PATCH, D), embedding_bias=(D,), enc_norms=(6, D), enc_biases=(2, D), to_decoder=(D, DD), mask_token=(DD,),
    dec_norms=(6, DD), dec_biases=(2, DD), dec_qkv=(DD, 3 * DD), dec_qkv_bias=(2, DD), dec_proj=(DD, DD), pixel_head=(DD, PATCH),
    head_bias=(PATCH,))
SPLIT = dict(
    enc_qkv=(D, 576), enc_qkv_bias=(2, 192), enc_proj=(192, D), enc_up=(D, 768), enc_up_bias=(768,), enc_down=(768, D),
    dec_up=(DD, 384), dec_up_bias=(384,), dec_down=(384, DD))


def row_table(layout):
    table, at = {}, 0
    for name, shape in layout.items():
        count = math.prod(shape) // LANES
        table[name] = (at, count)
        at += count
    return Namespace(**table)


CROW = row_table(COMMON)
SROW = row_table(SPLIT)
DEC_ROW = SROW.dec_up[0]
SPLIT_ROWS = SROW.dec_down[0] + SROW.dec_down[1]
COMMON_ROWS = CROW.head_bias[0] + CROW.head_bias[1]


class Plan:
    def __init__(self, parts, share, rows_step):
        self.parts, self.share = parts, share
        self.base = [i * share // BLOCK * TILE for i in range(parts)]
        self.rows = round_up(-(-(share + BLOCK - 1) // LANES), rows_step)

    def pieces(self, first, last):
        out = []
        for i in range(self.parts):
            start = self.base[i] + (TILE if i else 0)
            stop = self.base[i + 1] if i + 1 < self.parts else self.base[i] + self.rows
            low, high = max(start, first), min(stop, last)
            if i and first <= self.base[i] < last:
                out.append(("edge", i, self.base[i] - self.base[i - 1], self.base[i], TILE))
            if low < high:
                out.append(("body", i, low - self.base[i], low, high - low))
        return out

    def owners(self, first, last):
        return sorted({i for kind, i, *_ in self.pieces(first, last)} | {i - 1 for kind, i, *_ in self.pieces(first, last) if kind == "edge"})


def align_kernel(scalars, split_in, common_in, split_out, common_out):
    def move(source, target, lanes, rows_down, skip, step):
        def part(row, step):
            lane = lax.broadcasted_iota(jnp.int32, (step, LANES), 1)
            here = source[pl.ds(FRONT - rows_down + skip + row, step), :]
            before = source[pl.ds(FRONT - 1 - rows_down + skip + row, step), :]
            value = jnp.where(lane >= lanes, pltpu.roll(here, lanes, 1), pltpu.roll(before, lanes, 1))
            target[pl.ds(pl.multiple_of(row, TILE), step), :] = value.astype(BF16)

        def body(index, _):
            part(index * step, step)
            return 0

        whole = target.shape[0] // step
        lax.fori_loop(0, whole, body, 0)
        if target.shape[0] % step:
            part(whole * step, target.shape[0] % step)

    move(split_in, split_out, scalars[0], scalars[1], 0, 256)
    move(common_in, common_out, scalars[2], scalars[3], scalars[4], 256)


def aligned(master, plan):
    tail = (plan.rows + 8) * LANES - master.shape[-1]
    return jnp.pad(master, ((0, 0),) * (master.ndim - 1) + ((FRONT * LANES, tail),)).reshape(-1, LANES)


def align(common_master, split_master, cplan, splan):
    me, t = lax.axis_index(DP), lax.axis_index(TENSOR)
    soff = me * splan.share % BLOCK
    coff = me * cplan.share % BLOCK
    quarter = cplan.rows // 4
    scalars = jnp.stack([soff % LANES, soff // LANES, coff % LANES, coff // LANES, t * quarter]).astype(jnp.int32)
    return pl.pallas_call(
        align_kernel,
        out_shape=(jax.ShapeDtypeStruct((splan.rows, LANES), BF16), jax.ShapeDtypeStruct((quarter, LANES), BF16)),
        in_specs=[pl.BlockSpec(memory_space=pltpu.SMEM), pl.BlockSpec(memory_space=pltpu.VMEM), pl.BlockSpec(memory_space=pltpu.VMEM)],
        out_specs=[pl.BlockSpec(memory_space=pltpu.VMEM)] * 2,
        name="align",
    )(scalars, aligned(split_master, splan), aligned(common_master, cplan))


OUTS = Namespace(
    embedding=(PATCH, D), to_decoder=(D, DD), dec_qkv=(DD, 3 * DD), dec_proj=(DD, DD), pixel_head=(DD, PATCH),
    enc_qkv=(2, D, 576), enc_proj=(384, D), enc_up=(D, 1536), enc_down=(1536, D), dec_up=(DD, 1536), dec_down=(1536, DD))
OUT_NAMES = tuple(vars(OUTS))
CMATS = OUT_NAMES[:5]
SMALLS = ((CROW.embedding_bias[0], 54), (CROW.mask_token[0], 27), (CROW.dec_qkv_bias[0], 6), (CROW.head_bias[0], 12))


def copy_rows(pieces, frame, wide, first, chunk=64):
    for kind, part, row, at, count in pieces:
        if kind == "edge":
            wide[pl.ds(at - first, TILE), :] = frame(part)[pl.ds(0, TILE), :].astype(F32) + frame(part - 1)[pl.ds(row, TILE), :].astype(F32)
            continue
        source, whole = frame(part), count // chunk

        def body(index, _, source=source, row=row, at=at):
            wide[pl.ds(pl.multiple_of(at - first + index * chunk, TILE), chunk), :] = source[
                pl.ds(pl.multiple_of(row + index * chunk, TILE), chunk), :
            ].astype(F32)
            return 0

        if whole:
            lax.fori_loop(0, whole, body, 0)
        for rest in range(whole * chunk, count, TILE):
            wide[pl.ds(at - first + rest, TILE), :] = source[pl.ds(row + rest, TILE), :].astype(F32)


def matrix_out(wide, start, rows, width, target, row0, col0, step=64):
    per_row = width // LANES

    def body(index, _):
        at = index * step
        for j in range(per_row):
            value = wide[pl.ds(start + j + at * per_row, step, stride=per_row), :]
            target[pl.ds(pl.multiple_of(row0 + at, TILE), step), col0 + j * LANES : col0 + (j + 1) * LANES] = value.astype(BF16)
        return 0

    lax.fori_loop(0, rows // step, body, 0)


def qkv_out(wide, start, pair_buf, target):
    step = 32
    lane = lax.broadcasted_iota(jnp.int32, (step, LANES), 1)

    def body(index, _):
        at = start + index * step * 9
        for j in range(5):
            even = wide[pl.ds(at + j, step, stride=9), :]
            low = pltpu.roll(wide[pl.ds(at + 4 + j, step, stride=9), :], 64, 1)
            if j < 4:
                high = pltpu.roll(wide[pl.ds(at + 5 + j, step, stride=9), :], 64, 1)
                odd = jnp.where(lane < 64, low, high)
            else:
                odd = low
            pair_buf[j, pl.ds(0, step, stride=2), :] = even
            pair_buf[j, pl.ds(1, step, stride=2), :] = odd
            both = pair_buf[j].astype(BF16)
            rows = pl.ds(pl.multiple_of(index * 64, 64), 64)
            if j < 4:
                target[rows, j * LANES : (j + 1) * LANES] = both
            else:
                target[rows, 512:576] = both[:, :64]
        return 0

    lax.fori_loop(0, 12, body, 0)


def floor16(value):
    return value // TILE * TILE


SCALE = HEAD ** (-0.5)


def nt(a, b):
    return lax.dot_general(a, b, (((1,), (1,)), ((), ())), preferred_element_type=F32)


def nn(a, b):
    return lax.dot_general(a, b, (((1,), (0,)), ((), ())), preferred_element_type=F32)


def tn(a, b):
    return lax.dot_general(a, b, (((0,), (0,)), ((), ())), preferred_element_type=F32)


VP = 160
SAVED = Namespace(
    embedded=((VP, D), F32), normed_a=((VP, D), BF16), mixed=((2, VP, 576), BF16), probs=((6, VP, VP), F32), merged=((VP, 384), BF16),
    after=((VP, D), F32), normed_m=((VP, D), BF16), raised=((VP, 1536), F32), active=((VP, 1536), BF16), encoded=((VP, D), F32),
    final_low=((VP, D), BF16), lowered=((VP, DD), F32), seen=((VP, PATCH), BF16))
NSAVED = len(vars(SAVED))
SMALL_AT = []
for _, _count in SMALLS:
    SMALL_AT.append(sum(round_up(count, 8) for _, count in SMALLS[: len(SMALL_AT)]))


def norm_rows(inputs, gain, shift):
    centered = inputs - jnp.mean(inputs, axis=-1, keepdims=True)
    spread = jnp.mean(centered * centered, axis=-1, keepdims=True)
    return centered * lax.rsqrt(spread + 1e-06) * gain + shift


def unpacker(cplan, splan, common_frame, split_frame, dec_frame, stage, small_ref, bias_ref, dbias_ref, wide, pair_buf, done):
    def load(plan, frame, start, count):
        first, last = floor16(start), round_up(start + count, TILE)
        copy_rows(plan.pieces(first, last), frame, wide, first)
        return start - first

    def split(c):
        frame = functools.partial(split_frame, c)
        start, count = SROW.enc_qkv
        qkv_out(wide, load(splan, frame, start, count), pair_buf, stage.enc_qkv.at[c])
        at = load(splan, frame, *SROW.enc_qkv_bias)
        bias_ref[c, 0:8, :] = wide[pl.ds(at, 8), :]
        at = load(splan, frame, *SROW.enc_proj)
        matrix_out(wide, at, 192, D, stage.enc_proj, c * 192, 0)
        at = load(splan, frame, *SROW.enc_up)
        matrix_out(wide, at, D, 768, stage.enc_up, 0, c * 768)
        at = load(splan, frame, *SROW.enc_up_bias)
        bias_ref[c, 8:16, :] = wide[pl.ds(at, 8), :]
        at = load(splan, frame, *SROW.enc_down)
        matrix_out(wide, at, 768, D, stage.enc_down, c * 768, 0)
        if c:
            for whole in (stage.enc_qkv, stage.enc_proj, stage.enc_up, stage.enc_down):
                done(whole)

    def common(name):
        at = load(cplan, common_frame, *vars(CROW)[name])
        rows, width = vars(OUTS)[name]
        matrix_out(wide, at, rows, width, vars(stage)[name], 0, 0)
        if name != CMATS[0]:
            done(vars(stage)[name])

    def smalls():
        for small_at, (start, count) in zip(SMALL_AT, SMALLS):
            at = load(cplan, common_frame, start, count)
            small_ref[pl.ds(small_at, round_up(count, 8)), :] = wide[pl.ds(at, round_up(count, 8)), :]

    def dec():
        for slot in range(4):
            frame = functools.partial(split_frame, slot) if slot < 2 else functools.partial(dec_frame, slot - 2)
            at = load(splan, frame, DEC_ROW, SPLIT_ROWS - DEC_ROW)
            matrix_out(wide, at, DD, 384, stage.dec_up, 0, slot * 384)
            bias = at + SROW.dec_up_bias[0] - DEC_ROW
            dbias_ref[slot, :, :] = wide[pl.ds(bias, 8), :]
            matrix_out(wide, bias + 3, 384, DD, stage.dec_down, slot * 384, 0)
        done(stage.dec_up)
        done(stage.dec_down)

    return split, common, smalls, dec


def row_of(ref, at, count):
    return jnp.concatenate([ref[at + k : at + k + 1, :] for k in range(count)], axis=1)


def sines(width, step=32):
    column = np.arange(width)
    rate = 10000.0 ** (-(2 * (column // 2)) / width)
    high, low = np.arange(0, TUBES, step)[:, None] * rate, np.arange(step)[:, None] * rate
    even = column % 2 == 0
    return (
        np.where(even, np.sin(high), np.cos(high)).astype(np.float32), np.where(even, np.cos(high), -np.sin(high)).astype(np.float32),
        np.cos(low).astype(np.float32), np.sin(low).astype(np.float32))


def exact(a, b):
    return lax.dot_general(a, b, (((1,), (0,)), ((), ())), precision=lax.Precision.HIGHEST, preferred_element_type=F32)


def pick_rows(order_ref, pixel_buf, high_ref, low_ref, saved):
    order = order_ref[...]
    chosen = order == lax.broadcasted_iota(jnp.int32, (VP, TUBES), 1)
    saved.seen[...] = nn(jnp.where(chosen, 1.0, 0.0).astype(BF16), pixel_buf[...]).astype(BF16)
    high = jnp.where(lax.shift_right_logical(order, 5) == lax.broadcasted_iota(jnp.int32, (VP, 56), 1), 1.0, 0.0)
    low = jnp.where(lax.bitwise_and(order, 31) == lax.broadcasted_iota(jnp.int32, (VP, 32), 1), 1.0, 0.0)
    saved.embedded[...] = exact(high, high_ref[:, :D]) * exact(low, low_ref[:, :D]) + exact(high, high_ref[:, D:]) * exact(low, low_ref[:, D:])


def embed(stage, small_ref, saved):
    saved.embedded[...] = nn(saved.seen[...], stage.embedding[...]) + row_of(small_ref, 0, 6) + saved.embedded[...]


def encode(stage, small_ref, bias_ref, saved, swap, while_first, while_second):
    def norm(k):
        return row_of(small_ref, 6 + 6 * k, 6)

    embedded = saved.embedded[...]
    normed = norm_rows(embedded, norm(0), norm(1)).astype(BF16)
    saved.normed_a[...] = normed
    keys = lax.broadcasted_iota(jnp.int32, (VP, VP), 1) < VIS
    outs = []
    for slot in range(2):
        flat = row_of(bias_ref.at[slot], 0, 3)
        bias = jnp.concatenate([flat[:, :192], jnp.zeros((1, 192), F32), flat[:, 192:]], axis=1)
        saved.mixed[slot] = (nn(normed, stage.enc_qkv[slot]) + bias).astype(BF16)
        for head in range(3):
            q, k, v = [saved.mixed[slot, :, 192 * n + HEAD * head : 192 * n + HEAD * (head + 1)] for n in range(3)]
            scores = jnp.where(keys, nt(q, k) * SCALE, -1e30)
            shifted = jnp.exp(scores - jnp.max(scores, axis=1, keepdims=True))
            probs = shifted / jnp.sum(shifted, axis=1, keepdims=True)
            saved.probs[slot * 3 + head] = probs
            outs.append(nn(probs.astype(BF16), v).astype(BF16))
    merged = jnp.concatenate(outs, axis=1)
    saved.merged[...] = merged
    mine, copy, other = swap(0)
    mine[...] = nn(merged, stage.enc_proj[...]).astype(BF16)
    copy.start()
    while_first()
    copy.wait_recv()
    after = embedded + (mine[...].astype(F32) + other[...].astype(F32) + row_of(small_ref, 42, 6))
    saved.after[...] = after
    normed = norm_rows(after, norm(2), norm(3)).astype(BF16)
    saved.normed_m[...] = normed
    up_bias = jnp.concatenate([row_of(bias_ref.at[slot], 8, 6) for slot in range(2)], axis=1)
    for col in range(0, 1536, 384):
        raised = nn(normed, stage.enc_up[:, col : col + 384]) + up_bias[:, col : col + 384]
        saved.raised[:, col : col + 384] = raised
        saved.active[:, col : col + 384] = (0.5 * raised * (1.0 + lax.erf(raised * math.sqrt(0.5)))).astype(BF16)
    mine, second, other = swap(1)
    mine[...] = nn(saved.active[...], stage.enc_down[...]).astype(BF16)
    second.start()
    while_second()
    second.wait_recv()
    encoded = saved.after[...] + (mine[...].astype(F32) + other[...].astype(F32) + row_of(small_ref, 48, 6))
    saved.encoded[...] = encoded
    saved.final_low[...] = norm_rows(encoded, norm(4), norm(5)).astype(BF16)
    copy.wait_send()
    second.wait_send()


def unpack_and_encode(cplan, splan, refs, ready):
    (order, pixels, high, low), outs, smalls, saved, (sbuf, dbuf, cbuf, wide, pair_buf), stages, out_sem, (swaps, moved, send, recv, pixel_buf, pixel_sem) = refs
    t = lax.axis_index(TENSOR)
    y, c = t // 2, t % 2
    me = lax.axis_index(DP)
    fd = first_dec(splan)
    stage = Namespace(**dict(zip(OUT_NAMES, stages)))
    copies = []
    pltpu.make_async_copy(pixels.at[c], pixel_buf, pixel_sem).wait()
    pick_rows(order, pixel_buf, high, low, saved)

    def done(whole):
        index = [ref is whole for ref in stages].index(True)
        copy = pltpu.make_async_copy(whole, outs[index], out_sem.at[index])
        copy.start()
        copies.append(copy)

    split, common, common_smalls, dec = unpacker(
        cplan, splan, lambda i: cbuf.at[i], lambda c, i: sbuf.at[c, i], lambda c, i: dbuf.at[c, i - fd],
        stage, smalls[0], smalls[1], smalls[2], wide, pair_buf, done)

    def swap(n):
        copy = pltpu.make_async_remote_copy(
            src_ref=swaps.at[n, 0], dst_ref=swaps.at[n, 1], send_sem=send.at[n], recv_sem=recv.at[n],
            device_id={DP: me, TENSOR: (1 - y) * 2 + c}, device_id_type=MESH)
        return swaps.at[n, 0], copy, swaps.at[n, 1]

    ready(0)
    common(CMATS[0])
    common_smalls()
    embed(stage, smalls[0], saved)
    ready(1)
    split(0)
    split(1)

    def first():
        common(CMATS[1])
        common(CMATS[2])

    def second():
        common(CMATS[3])
        common(CMATS[4])

    encode(stage, smalls[0], smalls[1], saved, swap, first, second)
    move = pltpu.make_async_remote_copy(
        src_ref=saved.final_low, dst_ref=moved, send_sem=send.at[2], recv_sem=recv.at[2],
        device_id={DP: me, TENSOR: y * 2 + (1 - c)}, device_id_type=MESH)

    @pl.when(y == c)
    def _():
        move.start()

    ready(2)
    dec()

    @pl.when(y == c)
    def _():
        saved.lowered[...] = nn(saved.final_low[...], stage.to_decoder[...])
        move.wait_send()

    @pl.when(y != c)
    def _():
        move.wait_recv()
        saved.lowered[...] = nn(moved[...], stage.to_decoder[...])

    for copy in copies:
        copy.wait()


SMALL_ROWS = sum(round_up(count, 8) for _, count in SMALLS)
GATHERED = tuple(jax.ShapeDtypeStruct(vars(OUTS)[name], BF16) for name in OUT_NAMES) + (
    jax.ShapeDtypeStruct((SMALL_ROWS, LANES), F32), jax.ShapeDtypeStruct((2, 16, LANES), F32), jax.ShapeDtypeStruct((4, 8, LANES), F32),
) + tuple(jax.ShapeDtypeStruct(*pair) for pair in vars(SAVED).values())


def first_dec(splan):
    return splan.owners(floor16(DEC_ROW), round_up(SPLIT_ROWS, TILE))[0]


def unpack_scratch(cplan, splan):
    fd = first_dec(splan)
    return [
        pltpu.VMEM((2, splan.parts, splan.rows, LANES), BF16),
        pltpu.VMEM((2, splan.parts - fd, splan.rows, LANES), BF16),
        pltpu.VMEM((cplan.parts, cplan.rows, LANES), BF16),
        pltpu.VMEM((CROW.embedding[1] + 32, LANES), F32),
        pltpu.VMEM((5, 64, LANES), F32),
    ] + [pltpu.VMEM(vars(OUTS)[name], BF16) for name in OUT_NAMES] + [
        pltpu.SemaphoreType.DMA((len(OUT_NAMES),)), pltpu.VMEM((2, 2, VP, D), BF16), pltpu.VMEM((VP, D), BF16),
        pltpu.SemaphoreType.DMA((3,)), pltpu.SemaphoreType.DMA((3,)), pltpu.VMEM((TUBES, PATCH), BF16), pltpu.SemaphoreType.DMA]


def shared_refs(refs):
    nout = len(OUT_NAMES)
    outs, smalls = refs[4 : nout + 4], refs[nout + 4 : nout + 7]
    saved = Namespace(**dict(zip(vars(SAVED), refs[nout + 7 : nout + 7 + NSAVED])))
    rest = refs[nout + 7 + NSAVED :]
    pltpu.make_async_copy(refs[1].at[lax.axis_index(TENSOR) % 2], rest[10 + nout], rest[11 + nout]).start()
    return (refs[:4], outs, smalls, saved, rest[:5], rest[5 : 5 + nout], rest[5 + nout], rest[6 + nout : 12 + nout]), rest[12 + nout :]


def gather_kernel(cplan, splan, s_own, c_own, *refs):
    shared, (send, recv, local) = shared_refs(refs)
    sbuf, dbuf, cbuf = shared[4][:3]
    me, t = lax.axis_index(DP), lax.axis_index(TENSOR)
    z, x, y, c = me // 2, me % 2, t // 2, t % 2
    ty = (1 - y) * 2 + c
    fd = first_dec(splan)
    quarter = cplan.rows // 4

    def cblock(i, tt):
        return cbuf.at[i, pl.ds(pl.multiple_of(tt * quarter, TILE), quarter)]

    def sblock(i):
        return sbuf.at[c, i]

    zdev = [{DP: (z + k) % 4 * 2 + x, TENSOR: t} for k in range(4)]
    xdev, ydev, kdev = {DP: z * 2 + (1 - x), TENSOR: t}, {DP: me, TENSOR: ty}, {DP: me, TENSOR: y * 2 + (1 - c)}
    barrier = pltpu.get_barrier_semaphore()
    for device in zdev[1:] + [xdev, ydev, kdev]:
        pl.semaphore_signal(barrier, inc=1, device_id=device, device_id_type=MESH)
    own = [pltpu.make_async_copy(s_own, sblock(me), local.at[0]), pltpu.make_async_copy(c_own, cblock(me, t), local.at[1])]
    for copy in own:
        copy.start()
    pl.semaphore_wait(barrier, 6)
    for copy in own:
        copy.wait()

    def remote(source, target, slot, device):
        return pltpu.make_async_remote_copy(
            src_ref=source, dst_ref=target, send_sem=send.at[slot], recv_sem=recv.at[slot], device_id=device, device_id_type=MESH)

    def z_copy(common, down, hop, i):
        block = cblock(i, t) if common else sblock(i)
        return remote(block, block, common * 6 + down * 3 + hop - 1, zdev[3 if down else 1])

    def x_copy(common, i):
        block = cblock(i, t) if common else sblock(i)
        return remote(block, block, 12 + common * 4 + i // 2, xdev)

    def y_copy(i):
        return remote(cblock(i, t), cblock(i, t), 20 + i, ydev)

    def k_copy(i):
        return remote(sblock(i), sblock(i), 28 + i, kdev)

    def k_common(i):
        return remote(cblock(i, t), cblock(i, t), 36 + i, kdev)

    def k_far(i):
        return remote(cblock(i, ty), cblock(i, ty), 44 + i, kdev)

    def dec_rows(i):
        return pl.ds(max(0, DEC_FIRST - splan.base[i]), min(splan.rows, S_WIDE - splan.base[i]) - max(0, DEC_FIRST - splan.base[i]))

    def d_copy(i):
        return remote(sbuf.at[c, i, dec_rows(i)], dbuf.at[c, i - fd, dec_rows(i)], 52 + i - fd, ydev)

    def d_beside(i):
        return remote(dbuf.at[c, i - fd, dec_rows(i)], dbuf.at[c, i - fd, dec_rows(i)], 54 + i - fd, kdev)

    def send_z(common, down, hop):
        i = (z + (hop - 1 if down else 1 - hop)) * 2 + x
        able = jnp.logical_and(z > 0, z + hop - 1 <= 3) if down else jnp.logical_and(z < 3, z - hop + 1 >= 0)
        return i, able

    def pass_on(common, down, hop, action):
        i, able = send_z(common, down, hop)

        @pl.when(able)
        def _():
            action(z_copy(common, down, hop, i))

    def share_c(i):
        x_copy(1, i).start()
        y_copy(i).start()
        k_common(i).start()

    def share_s(i):
        x_copy(0, i).start()
        k_copy(i).start()
        dec_start(i)

    def dec_start(i):
        for known in range(fd, splan.parts):
            @pl.when(i == known)
            def _(known=known):
                d_copy(known).start()

    for common in (1, 0):
        for down in (0, 1):
            pass_on(common, down, 1, lambda copy: copy.start())
    share_c(me)
    share_s(me)
    for hop in (1, 2, 3):
        for common in (1, 0):
            for down in (0, 1):
                i = (z + (hop if down else -hop)) * 2 + x
                here = z + hop <= 3 if down else z >= hop

                @pl.when(here)
                def _(common=common, down=down, hop=hop, i=i):
                    z_copy(common, down, hop, i).wait_recv()
                    if hop < 3:
                        pass_on(common, down, hop + 1, lambda copy: copy.start())
                    if common:
                        share_c(i)
                    else:
                        share_s(i)

    def split_here(zz):
        i = zz * 2 + (1 - x)
        x_copy(0, i).wait_recv()
        k_copy(i).start()
        dec_start(i)

    def ready(stage):
        if stage == 0:
            for zz in range(4):
                i = zz * 2 + (1 - x)
                x_copy(1, i).wait_recv()
                y_copy(i).start()
                k_common(i).start()
            for i in range(8):
                y_copy(i).wait_recv()
                k_far(i).start()
            for i in range(8):
                k_common(i).wait_recv()
                k_far(i).wait_recv()
        if stage == 1:
            for zz in range(4):
                split_here(zz)
            for i in range(8):
                k_copy(i).wait_recv()
        if stage == 2:
            for i in range(fd, splan.parts):
                d_copy(i).wait_recv()
                d_beside(i).start()
            for i in range(fd, splan.parts):
                d_beside(i).wait_recv()

    unpack_and_encode(cplan, splan, shared, ready)
    for hop in (1, 2, 3):
        for common in (1, 0):
            for down in (0, 1):
                pass_on(common, down, hop, lambda copy: copy.wait_send())
    for zz in range(4):
        for common in (1, 0):
            x_copy(common, zz * 2 + x).wait_send()
    for i in range(8):
        for copy in (y_copy(i), k_copy(i), k_common(i), k_far(i)):
            copy.wait_send()
    for i in range(fd, splan.parts):
        d_copy(i).wait_send()
        d_beside(i).wait_send()


def local_unpack_kernel(cplan, splan, s_all, d_all, c_all, *refs):
    shared, (local,) = shared_refs(refs)
    t = lax.axis_index(TENSOR)
    barrier = pltpu.get_barrier_semaphore()
    for other in (t // 2 * 2 + 1 - t % 2, (1 - t // 2) * 2 + t % 2):
        pl.semaphore_signal(barrier, inc=1, device_id={DP: lax.axis_index(DP), TENSOR: other}, device_id_type=MESH)
    copies = [pltpu.make_async_copy(source, target, local.at[k]) for k, (source, target) in enumerate(zip((s_all, d_all, c_all), shared[4][:3]))]
    for copy in copies:
        copy.start()
    for copy in copies:
        copy.wait()
    pl.semaphore_wait(barrier, 2)
    unpack_and_encode(cplan, splan, shared, lambda stage: None)


def gather_weights(common_master, split_master, order, pixels, cplan, splan):
    s_own, c_own = align(common_master, split_master, cplan, splan)
    seen = lax.dynamic_index_in_dim(order, lax.axis_index(TENSOR) % 2, 0, False)[:VIS]
    first, second, third, fourth = sines(D)
    high = np.pad(np.concatenate([first, second], axis=1), ((0, 7), (0, 0)))
    inputs = (jnp.pad(seen, (0, VP - VIS))[:, None], pixels, jnp.asarray(high), jnp.asarray(np.concatenate([third, fourth], axis=1)))
    any_spec = pl.BlockSpec(memory_space=pl.ANY)
    vmem = pl.BlockSpec(memory_space=pltpu.VMEM)
    scratch = unpack_scratch(cplan, splan)
    fd = first_dec(splan)
    out_specs = [any_spec] * len(OUT_NAMES) + [vmem] * (3 + NSAVED)
    params = pltpu.CompilerParams(collective_id=0, has_side_effects=True, vmem_limit_bytes=64000 * 1024)
    if cplan.parts == 8 and splan.parts == 8:
        results = pl.pallas_call(
            functools.partial(gather_kernel, cplan, splan),
            out_shape=GATHERED, in_specs=[vmem] * 3 + [any_spec] + [vmem] * 2, out_specs=out_specs,
            scratch_shapes=scratch + [pltpu.SemaphoreType.DMA((56,)), pltpu.SemaphoreType.DMA((56,)), pltpu.SemaphoreType.DMA((2,))],
            compiler_params=params, name="gather",
        )(s_own, c_own, *inputs)
    else:
        y = lax.axis_index(TENSOR) // 2
        s_all = lax.all_gather(lax.all_gather(s_own, DP), TENSOR).reshape(2, 2, splan.parts, splan.rows, LANES)
        c_all = jnp.moveaxis(lax.all_gather(lax.all_gather(c_own, DP), TENSOR), 0, 1).reshape(cplan.parts, cplan.rows, LANES)
        s_mine = lax.dynamic_index_in_dim(s_all, y, 0, False)
        d_other = lax.dynamic_index_in_dim(s_all, 1 - y, 0, False)[:, fd:]
        results = pl.pallas_call(
            functools.partial(local_unpack_kernel, cplan, splan),
            out_shape=GATHERED, in_specs=[any_spec] * 3 + [vmem, any_spec] + [vmem] * 2, out_specs=out_specs,
            scratch_shapes=scratch + [pltpu.SemaphoreType.DMA((3,))], compiler_params=params, name="unpack",
        )(s_mine, d_other, c_all, *inputs)
    weights = Namespace(**dict(zip(OUT_NAMES, results)))
    small, bias, dbias = results[len(OUT_NAMES) : len(OUT_NAMES) + 3]
    at = 0
    rows = []
    for _, count in SMALLS:
        rows.append(small[at : at + count])
        at += round_up(count, 8)
    a, b, qkv_rows, head_rows = rows
    weights.embedding_bias = a[:6].reshape(1, D)
    weights.enc_norms = a[6:42].reshape(6, D)
    weights.enc_biases = a[42:54].reshape(2, D)
    weights.mask_token = b[:3].reshape(1, DD)
    weights.dec_norms = b[3:21].reshape(6, DD)
    weights.dec_biases = b[21:27].reshape(2, DD)
    weights.dec_qkv_bias = qkv_rows.reshape(2, DD)
    weights.head_bias = head_rows.reshape(1, PATCH)
    weights.enc_qkv_bias = bias[:, :3].reshape(2, 2, 192)
    weights.enc_up_bias = bias[:, 8:14].reshape(1, 1536)
    weights.dec_up_bias = dbias[:, :3].reshape(1, 1536)
    return weights, Namespace(**dict(zip(vars(SAVED), results[len(OUT_NAMES) + 3 :])))


DEC_FIRST = floor16(DEC_ROW)
S_WIDE = round_up(SPLIT_ROWS, TILE)
C_WIDE = round_up(COMMON_ROWS, TILE)
D_WIDE = S_WIDE - DEC_FIRST
SLOTS = 2


def buffer_rows(plan, wide):
    return max(wide, plan.base[-1] + plan.rows)


def clear(wide, first, last, chunk=64):
    def body(index, _):
        wide[pl.ds(first + index * chunk, chunk), :] = jnp.zeros((chunk, LANES), F32)
        return 0

    whole = (last - first) // chunk
    lax.fori_loop(0, whole, body, 0)
    rest = (last - first) % chunk
    if rest:
        wide[pl.ds(first + whole * chunk, rest), :] = jnp.zeros((rest, LANES), F32)


def matrix_in(wide, start, per_row, stage, rows, width, j0, step=64):
    def body(index, _):
        at = index * step
        for j in range(width // LANES):
            wide[pl.ds(start + j0 + j + at * per_row, step, stride=per_row), :] = stage[
                pl.ds(pl.multiple_of(at, 8), step), j * LANES : (j + 1) * LANES
            ]
        return 0

    lax.fori_loop(0, rows // step, body, 0)


def qkv_in(wide, start, pair_buf, stage):
    step = 32
    lane = lax.broadcasted_iota(jnp.int32, (step, LANES), 1)

    def body(index, _):
        at = start + index * step * 9
        even, odd = [], []
        base = pl.multiple_of(index * 64, 8)
        for j in range(5):
            lanes = slice(j * LANES, (j + 1) * LANES) if j < 4 else slice(512, 640)
            pair_buf[j] = stage[pl.ds(base, 64), lanes]
            even.append(pair_buf[j, pl.ds(0, step, stride=2), :])
            odd.append(pltpu.roll(pair_buf[j, pl.ds(1, step, stride=2), :], 64, 1))
        for j in range(4):
            wide[pl.ds(at + j, step, stride=9), :] = even[j]
        wide[pl.ds(at + 4, step, stride=9), :] = jnp.where(lane < 64, even[4], odd[0])
        for j in range(4):
            wide[pl.ds(at + 5 + j, step, stride=9), :] = jnp.where(lane < 64, odd[j], odd[j + 1])
        return 0

    lax.fori_loop(0, 12, body, 0)


def add_rows(target, parts, count, chunk=None):
    chunk = chunk or max(c for c in (128, 64, 48, 32, 16) if count % c == 0)

    def body(index, _):
        at = index * chunk
        total = None
        for ref, start in parts:
            value = ref[pl.ds(pl.multiple_of(start + at, TILE), chunk), :].astype(F32)
            total = value if total is None else total + value
        target[pl.ds(pl.multiple_of(at, TILE), chunk), :] = total.astype(target.dtype)
        return 0

    lax.fori_loop(0, count // chunk, body, 0)


def unalign(source, target, share, offset):
    down, lanes = offset // LANES, offset % LANES
    step = 64
    lane = lax.broadcasted_iota(jnp.int32, (step, LANES), 1)
    row = lax.broadcasted_iota(jnp.int32, (step, LANES), 0)

    def body(index, total):
        at = index * step
        here = pltpu.roll(source[pl.ds(down + at, step), :], LANES - lanes, 1)
        after = pltpu.roll(source[pl.ds(down + at + 1, step), :], LANES - lanes, 1)
        value = jnp.where(lane < LANES - lanes, here, after)
        value = jnp.where((row + at) * LANES + lane < share, value, 0.0)
        target[pl.ds(pl.multiple_of(at, 8), step), :] = value
        square = (value * value).reshape(step // 8, 8, LANES)
        return total + jnp.sum(square, axis=0)

    return lax.fori_loop(0, target.shape[0] // step, body, jnp.zeros((8, LANES), F32))


def flat_rows(share):
    return round_up(-(-share // LANES), 64)


SPLIT_EARLY = round_up(SROW.enc_up[0], TILE)
SPLIT_LATE = floor16(SROW.enc_up[0])
COMMON_EARLY = round_up(CROW.to_decoder[0], TILE)
COMMON_LATE = floor16(CROW.to_decoder[0])
WIDE_ROWS = max(S_WIDE - SPLIT_LATE, C_WIDE - COMMON_LATE)
BACK_WEIGHTS = OUT_NAMES[5:9] + OUT_NAMES[1:2]
LATE_NAMES = OUT_NAMES[2:5] + OUT_NAMES[9:]
KEPT = tuple(vars(SAVED))[:-2]


def norm_rows_back(inputs, gain, grad):
    centered = inputs - jnp.mean(inputs, axis=-1, keepdims=True)
    scale = lax.rsqrt(jnp.mean(centered * centered, axis=-1, keepdims=True) + 1e-06)
    unit = centered * scale
    inner = grad * gain
    back = scale * (inner - jnp.mean(inner, axis=-1, keepdims=True) - unit * jnp.mean(inner * unit, axis=-1, keepdims=True))
    return back, jnp.sum(grad * unit, axis=0, keepdims=True), jnp.sum(grad, axis=0, keepdims=True)


def value_in(wide, start, per_row, value, j0=0):
    rows = value.shape[0]
    for j in range(value.shape[1] // LANES):
        wide[pl.ds(start + j0 + j, rows, stride=per_row), :] = value[:, j * LANES : (j + 1) * LANES]


def row_in(wide, start, value):
    for j in range(value.shape[1] // LANES):
        wide[start + j : start + j + 1, :] = value[:, j * LANES : (j + 1) * LANES]


def narrow_part(wide, at, target, row, count, chunk=128):
    def body(index, _):
        target[pl.ds(pl.multiple_of(row + index * chunk, TILE), chunk), :] = wide[pl.ds(pl.multiple_of(at + index * chunk, TILE), chunk), :].astype(BF16)
        return 0

    whole = count // chunk
    lax.fori_loop(0, whole, body, 0)
    rest = count % chunk
    if rest:
        target[row + whole * chunk : row + count, :] = wide[at + whole * chunk : at + count, :].astype(BF16)


def back_and_pack(refs, hooks):
    (grads, part, seen, norms, small, dbias, weights, saved, wide, pair_buf, stage, stage_sem, gs, gd, gc, held,
     wq, wp, wu, wd, wt, weight_sem, raised_grad, mixed_grad, deep, swaps, joined, near, send, recv) = refs
    t = lax.axis_index(TENSOR)
    me = lax.axis_index(DP)
    y, c = t // 2, t % 2
    first_y = jnp.where(y == 0, 1.0, 0.0)
    ydev, kdev = {DP: me, TENSOR: (1 - y) * 2 + c}, {DP: me, TENSOR: y * 2 + (1 - c)}
    grad = Namespace(**dict(zip(LATE_NAMES, grads)))
    loads = [pltpu.make_async_copy(source, target, weight_sem.at[n]) for n, (source, target) in enumerate(zip(weights, (wq, wp, wu, wd, wt)))]
    for copy in loads:
        copy.start()

    def matrix(source, rows, width, per_row, start, j0=0):
        return (lambda here: matrix_in(wide, start, per_row, here, rows, width, j0), source, rows, width)

    def small_rows(source, start):
        def action():
            wide[pl.ds(start, source.shape[0]), :] = source[...]

        return (action,)

    def columns(slot, width):
        return pl.ds(pl.multiple_of(slot * width, LANES), width)

    def rows_of(slot, count):
        return pl.ds(pl.multiple_of(slot * count, 8), count)

    def dec_part(slot, first):
        return [
            matrix(grad.dec_up.at[:, columns(slot, 384)], DD, 384, 3, SROW.dec_up[0] - first),
            small_rows(dbias.at[slot, pl.ds(0, 3)], SROW.dec_up_bias[0] - first),
            matrix(grad.dec_down.at[rows_of(slot, 384)], 384, DD, 3, SROW.dec_down[0] - first),
            (functools.partial(clear, wide, SPLIT_ROWS - first, S_WIDE - first),)]

    def dec_jobs(slot):
        return [(lambda: clear(wide, 0, DEC_ROW - DEC_FIRST),)] + dec_part(slot + 2, DEC_FIRST) + [(lambda: narrow_part(wide, 0, gd.at[slot], 0, D_WIDE),)]

    def remote(source, target, slot, device):
        return pltpu.make_async_remote_copy(
            src_ref=source, dst_ref=target, send_sem=send.at[slot], recv_sem=recv.at[slot], device_id=device, device_id_type=MESH)

    def norm(k):
        return jnp.concatenate([norms[6 * k + n : 6 * k + n + 1, :] for n in range(6)], axis=1)

    run_jobs(dec_jobs(1 - c), stage, stage_sem)
    hooks.first()
    to_near, to_far = remote(part, near, 0, kdev), remote(joined, joined, 1, ydev)

    @pl.when(y != c)
    def _():
        to_near.start()

    run_jobs(dec_jobs(c), stage, stage_sem)

    @pl.when(y == c)
    def _():
        to_near.wait_recv()
        joined[...] = part[...] + near[...]
        to_far.start()

    for copy in loads:
        copy.wait()

    @pl.when(y != c)
    def _():
        to_far.wait_recv()

    lowered_grad = joined[...]
    encoded_grad, eg4, eg5 = norm_rows_back(saved.encoded[...], norm(4), nt(lowered_grad, wt[...]))
    deep[0] = encoded_grad
    branch = encoded_grad.astype(BF16)
    eb1 = jnp.sum(branch.astype(F32), axis=0, keepdims=True)
    for col in range(0, 1536, 384):
        raised = saved.raised[:, col : col + 384]
        slope = 0.5 * (1.0 + lax.erf(raised * math.sqrt(0.5))) + raised * jnp.exp(-0.5 * raised * raised) * (1.0 / math.sqrt(2.0 * math.pi))
        raised_grad[:, col : col + 384] = (nt(branch, wd[col : col + 384, :]) * slope).astype(BF16)
    swaps[0, 0] = nt(raised_grad[...], wu[...]).astype(BF16)
    swap = remote(swaps.at[0, 0], swaps.at[0, 1], 2, ydev)
    swap.start()
    base = SPLIT_LATE
    for away in (True, False):
        slot = 1 - c if away else c
        cols = columns(slot, 768)
        value_in(wide, SROW.enc_down[0] - base, 6, tn(saved.active[:, cols], branch))
        here = raised_grad[:, cols]
        value_in(wide, SROW.enc_up[0] - base, 6, tn(saved.normed_m[...], here))
        row_in(wide, SROW.enc_up_bias[0] - base, jnp.sum(here.astype(F32), axis=0, keepdims=True))
        run_jobs(dec_part(slot, base), stage, stage_sem)
        held[slot] = wide[0:TILE, :]
        narrow_part(wide, SPLIT_EARLY - base, gs.at[slot], SPLIT_EARLY, S_WIDE - SPLIT_EARLY)
        (hooks.early_away if away else hooks.early_own)()
    swap.wait_recv()
    back, eg2, eg3 = norm_rows_back(saved.after[...], norm(2), swaps[0, 0].astype(F32) + swaps[0, 1].astype(F32))
    after_grad = deep[0] + back
    deep[0] = after_grad
    branch = after_grad.astype(BF16)
    eb0 = jnp.sum(branch.astype(F32), axis=0, keepdims=True)
    merged_grad = nt(branch, wp[...]).astype(BF16)
    total = None
    for slot in range(2):
        pieces = [[], [], []]
        for head in range(3):
            q, k, v = [saved.mixed[slot, :, 192 * n + HEAD * head : 192 * n + HEAD * (head + 1)] for n in range(3)]
            index = slot * 3 + head
            do = merged_grad[:, index * HEAD : (index + 1) * HEAD]
            probs = saved.probs[index]
            pieces[2].append(tn(probs.astype(BF16), do).astype(BF16))
            dp = nt(do, v)
            ds = (probs * (dp - jnp.sum(dp * probs, axis=1, keepdims=True))).astype(BF16)
            pieces[0].append((nn(ds, k) * SCALE).astype(BF16))
            pieces[1].append((tn(ds, q) * SCALE).astype(BF16))
        mixed = jnp.concatenate([piece for group in pieces for piece in group] + [jnp.zeros((VP, 64), BF16)], axis=1)
        mixed_grad[slot] = mixed
        value = nt(mixed[:, :576], wq[slot])
        total = value if total is None else total + value
    swaps[1, 0] = total.astype(BF16)
    second = remote(swaps.at[1, 0], swaps.at[1, 1], 3, ydev)
    second.start()
    for away in (True, False):
        slot = 1 - c if away else c
        here = mixed_grad[slot]
        stage[0, :, 0:640] = tn(saved.normed_a[...], here)
        qkv_in(wide, SROW.enc_qkv[0], pair_buf, stage.at[0])
        sums = jnp.sum(here.astype(F32), axis=0, keepdims=True)
        row_in(wide, SROW.enc_qkv_bias[0], jnp.concatenate([sums[:, :192], sums[:, 384:576]], axis=1))
        wide[SPLIT_LATE:SPLIT_EARLY, :] = held[slot]
        mine = jnp.where(slot == 0, saved.merged[:, :192], saved.merged[:, 192:])
        value_in(wide, SROW.enc_proj[0], 6, tn(mine, branch))
        narrow_part(wide, 0, gs.at[slot], 0, SPLIT_EARLY)
        (hooks.late_away if away else hooks.late_own)()
    base = COMMON_LATE
    jobs = []
    at = 0
    for start, count in SMALLS[1:]:
        jobs.append(small_rows(small.at[pl.ds(at, count)], start - base))
        at += round_up(count, 8)
    for name in CMATS[2:]:
        rows, width_all = vars(OUTS)[name]
        for col in range(0, width_all, 768):
            width = min(768, width_all - col)
            jobs.append(matrix(vars(grad)[name].at[:, pl.ds(col, width)], rows, width, width_all // LANES, vars(CROW)[name][0] - base, col // LANES))
    value_in(wide, CROW.to_decoder[0] - base, 3, tn(saved.final_low[...], lowered_grad) * first_y)
    clear(wide, COMMON_ROWS - base, C_WIDE - base)
    run_jobs(jobs, stage, stage_sem)
    held[0] = wide[0:TILE, :]
    narrow_part(wide, COMMON_EARLY - base, gc, COMMON_EARLY, C_WIDE - COMMON_EARLY)
    hooks.common_early()
    second.wait_recv()
    back, eg0, eg1 = norm_rows_back(saved.embedded[...], norm(0), swaps[1, 0].astype(F32) + swaps[1, 1].astype(F32))
    low = (deep[0] + back).astype(BF16)
    half = CROW.embedding[1] // 2

    def zero(index, _):
        wide[pl.ds((1 - y) * half + index * 64, 64), :] = jnp.zeros((64, LANES), F32)
        return 0

    lax.fori_loop(0, half // 64, zero, 0)
    value_in(wide, y * half, 6, tn(seen[...], low))
    wide[COMMON_LATE:COMMON_EARLY, :] = held[0]
    for n, vector in enumerate((jnp.sum(low.astype(F32), axis=0, keepdims=True), eg0, eg1, eg2, eg3, eg4, eg5, eb0, eb1)):
        row_in(wide, CROW.embedding_bias[0] + 6 * n, vector * first_y)
    narrow_part(wide, 0, gc, 0, COMMON_EARLY)
    hooks.common_late()

    @pl.when(y != c)
    def _():
        to_near.wait_send()

    @pl.when(y == c)
    def _():
        to_far.wait_send()

    swap.wait_send()
    second.wait_send()


def run_jobs(jobs, stage, stage_sem):
    loads = [job for job in jobs if len(job) > 1]
    copies = [
        pltpu.make_async_copy(job[1], stage.at[n % SLOTS, pl.ds(0, job[2]), pl.ds(0, job[3])], stage_sem.at[n % SLOTS]) for n, job in enumerate(loads)]
    for copy in copies[: SLOTS - 1]:
        copy.start()
    index = 0
    for job in jobs:
        if len(job) == 1:
            job[0]()
            continue
        if index + SLOTS - 1 < len(copies):
            copies[index + SLOTS - 1].start()
        copies[index].wait()
        job[0](stage.at[index % SLOTS])
        index += 1


def back_refs(refs):
    grads, (part, seen, norms, small, dbias, loss) = refs[: len(LATE_NAMES)], refs[len(LATE_NAMES) : len(LATE_NAMES) + 6]
    refs = refs[len(LATE_NAMES) + 6 :]
    weights, kept, outs = refs[:5], refs[5 : 5 + len(KEPT)], refs[5 + len(KEPT) : 8 + len(KEPT)]
    refs = refs[8 + len(KEPT) :]
    saved = Namespace(**dict(zip(KEPT, kept)))
    return (grads, part, seen, norms, small, dbias, weights, saved) + tuple(refs[:22]), loss, outs, refs[22:]


def back_scratch(gs_rows, gc_rows):
    return [
        pltpu.VMEM((WIDE_ROWS, LANES), F32), pltpu.VMEM((5, 64, LANES), F32), pltpu.VMEM((SLOTS, 768, 768), F32), pltpu.SemaphoreType.DMA((SLOTS,)),
        pltpu.VMEM((2, gs_rows, LANES), BF16), pltpu.VMEM((2, D_WIDE, LANES), BF16), pltpu.VMEM((gc_rows, LANES), BF16),
        pltpu.VMEM((2, TILE, LANES), F32),
    ] + [pltpu.VMEM(vars(OUTS)[name], BF16) for name in BACK_WEIGHTS] + [
        pltpu.SemaphoreType.DMA((5,)), pltpu.VMEM((VP, 1536), BF16), pltpu.VMEM((2, VP, 640), BF16), pltpu.VMEM((1, VP, D), F32),
        pltpu.VMEM((2, 2, VP, D), BF16), pltpu.VMEM((VP, DD), BF16), pltpu.VMEM((VP, DD), BF16), pltpu.SemaphoreType.DMA((4,)), pltpu.SemaphoreType.DMA((4,))]


ZORDER = (2, 3, 0, 1)
SUBS = 4


def reduce_kernel(cplan, splan, *refs):
    back, loss, (g_split, g_common, sums), refs = back_refs(refs)
    wide, gs, gd, gc = back[8], back[12], back[13], back[14]
    (ks, xs, zs, kc, yc, xc, zc, kd, yd, cq, part, send, recv) = refs
    me, t = lax.axis_index(DP), lax.axis_index(TENSOR)
    z, x, y, c = me // 2, me % 2, t // 2, t % 2
    rank = me * 4 + t
    srows, quarter = splan.rows, cplan.rows // 4
    sub = srows // SUBS
    updev, downdev = {DP: (z + 1) % 4 * 2 + x, TENSOR: t}, {DP: (z + 3) % 4 * 2 + x, TENSOR: t}
    xdev, ydev, kdev = {DP: z * 2 + (1 - x), TENSOR: t}, {DP: me, TENSOR: (1 - y) * 2 + c}, {DP: me, TENSOR: y * 2 + (1 - c)}
    others = [(rank + k) % 32 for k in range(1, 32)]
    devices = [{DP: other // 4, TENSOR: other % 4} for other in others]
    barrier = pltpu.get_barrier_semaphore()
    for device in devices:
        pl.semaphore_signal(barrier, inc=1, device_id=device, device_id_type=MESH)

    def remote(source, target, slot, device):
        return pltpu.make_async_remote_copy(
            src_ref=source, dst_ref=target, send_sem=send.at[slot], recv_sem=recv.at[slot], device_id=device, device_id_type=MESH)

    def s_at(i):
        return pl.multiple_of(i * splan.share // BLOCK * TILE, TILE)

    def c_at(i, tt):
        return pl.multiple_of(i * cplan.share // BLOCK * TILE + tt * quarter, TILE)

    def piece(q):
        return pl.ds(pl.multiple_of(q * sub, TILE), sub)

    def kd_copy():
        return remote(gd.at[1 - c], kd, 0, kdev)

    def ks_copy(i):
        return remote(gs.at[1 - c, pl.ds(s_at(i), srows)], ks.at[i], 1 + i, kdev)

    def kc_copy(i, yy):
        return remote(gc.at[pl.ds(c_at(i, 2 * yy + 1 - c), quarter)], kc.at[i, yy], 9 + i * 2 + yy, kdev)

    def yd_copy():
        return remote(kd, yd, 25, ydev)

    def yc_copy(i):
        return remote(kc.at[i, 1 - y], yc.at[i], 26 + i, ydev)

    def xs_copy(zz, q):
        return remote(ks.at[zz * 2 + (1 - x), piece(q)], xs.at[zz, piece(q)], 34 + zz * 4 + q, xdev)

    def xc_copy(zz):
        return remote(yc.at[zz * 2 + (1 - x)], xc.at[zz], 50 + zz, xdev)

    def zs_copy(down, zz, q):
        return remote(xs.at[zz, piece(q)], zs.at[down, zz, piece(q)], 54 + down * 16 + zz * 4 + q, downdev if down else updev)

    def zc_copy(down, zz):
        return remote(xc.at[zz], zc.at[down, zz], 86 + down * 4 + zz, downdev if down else updev)

    def along_z(zz, copy_of, add):
        for down in (0, 1):
            passes = z > zz if down else z < zz
            first = z == 3 if down else z == 0

            @pl.when(jnp.logical_and(passes, first))
            def _():
                add(None)

            @pl.when(jnp.logical_and(passes, jnp.logical_not(first)))
            def _(down=down):
                copy_of(down).wait_recv()
                add(down)

            @pl.when(passes)
            def _(down=down):
                copy_of(down).start()

    def across_x(zz):
        i = zz * 2 + (1 - x)
        ks_copy(i).wait_recv()

        def body(q, _):
            add_rows(ks.at[i, piece(q)], [(ks.at[i, piece(q)], 0), (gs.at[c], s_at(i) + q * sub)], sub)
            xs_copy(zz, q).start()
            return 0

        lax.fori_loop(0, SUBS, body, 0)

    def first():
        pl.semaphore_wait(barrier, 31)
        kd_copy().start()

    def early_away():
        for zz in ZORDER[:2]:
            ks_copy(zz * 2 + (1 - x)).start()
        for zz in ZORDER[:2]:
            ks_copy(zz * 2 + x).start()
        kd_copy().wait_recv()
        add_rows(kd, [(gd.at[c], 0), (kd, 0)], D_WIDE)
        yd_copy().start()

    def early_own():
        across_x(ZORDER[0])
        yd_copy().wait_recv()
        dec_rows = gs.at[c, pl.ds(DEC_FIRST, D_WIDE)]
        add_rows(dec_rows, [(dec_rows, 0), (yd, 0)], D_WIDE)
        across_x(ZORDER[1])

    def late_away():
        for zz in ZORDER[2:]:
            ks_copy(zz * 2 + (1 - x)).start()
        for zz in ZORDER[2:]:
            ks_copy(zz * 2 + x).start()

    def late_own():
        for zz in ZORDER[2:]:
            across_x(zz)

    def common_core_sends(zzs):
        for zz in zzs:
            for xx in (0, 1):
                for yy in (0, 1):
                    kc_copy(zz * 2 + xx, yy).start()

    back_and_pack(back, Namespace(
        first=first, early_away=early_away, early_own=early_own, late_away=late_away, late_own=late_own,
        common_early=lambda: common_core_sends(ZORDER[:2]), common_late=lambda: common_core_sends(ZORDER[2:])))
    fin, finc = wide.at[pl.ds(0, srows + 64)], wide.at[pl.ds(srows + 64, cplan.rows + 64)]
    for zz in ZORDER:
        for xx in (0, 1):
            i = zz * 2 + xx
            for yy in (0, 1):
                kc_copy(i, yy).wait_recv()
            add_rows(kc.at[i, 1 - y], [(gc, c_at(i, 2 * (1 - y) + c)), (kc.at[i, 1 - y], 0)], quarter)
            yc_copy(i).start()
    for zz in ZORDER:
        i = zz * 2 + (1 - x)
        yc_copy(i).wait_recv()
        add_rows(yc.at[i], [(gc, c_at(i, t)), (kc.at[i, y], 0), (yc.at[i], 0)], quarter)
        xc_copy(zz).start()
        i = zz * 2 + x
        ks_copy(i).wait_recv()

        def body(q, _, zz=zz, i=i):
            xs_copy(zz, q).wait_recv()

            def add(flow):
                parts = [(xs.at[zz, piece(q)], 0), (gs.at[c], s_at(i) + q * sub), (ks.at[i, piece(q)], 0)]
                add_rows(xs.at[zz, piece(q)], parts + ([] if flow is None else [(zs.at[flow, zz, piece(q)], 0)]), sub)

            along_z(zz, lambda down: zs_copy(down, zz, q), add)
            return 0

        lax.fori_loop(0, SUBS, body, 0)
    for zz in ZORDER:
        i = zz * 2 + x
        yc_copy(i).wait_recv()
        xc_copy(zz).wait_recv()

        def add_common(flow, zz=zz, i=i):
            parts = [(xc.at[zz], 0), (gc, c_at(i, t)), (kc.at[i, y], 0), (yc.at[i], 0)]
            add_rows(xc.at[zz], parts + ([] if flow is None else [(zc.at[flow, zz], 0)]), quarter)

        along_z(zz, lambda down, zz=zz: zc_copy(down, zz), add_common)

    def ends(copy_of, action):
        for low, high in ((0, 1), (1, 1), (1, 0)):
            here = jnp.logical_and((z > 0) == bool(low), (z < 3) == bool(high))

            @pl.when(here)
            def _(low=low, high=high):
                flows = [0] * low + [1] * high
                for flow in flows:
                    copy_of(flow)
                action(flows)

    mine = pl.ds(pl.multiple_of(t * quarter, TILE), quarter)
    ends(
        lambda flow: zc_copy(flow, z).wait_recv(),
        lambda flows: add_rows(
            cq.at[mine], [(xc.at[z], 0), (gc, c_at(me, t)), (kc.at[me, y], 0), (yc.at[me], 0)] + [(zc.at[flow, z], 0) for flow in flows], quarter))
    far = pl.ds(pl.multiple_of(((1 - y) * 2 + c) * quarter, TILE), quarter)
    across_t, beside_t, beside_far = remote(cq.at[mine], cq.at[mine], 94, ydev), remote(cq.at[mine], cq.at[mine], 95, kdev), remote(cq.at[far], cq.at[far], 96, kdev)
    across_t.start()
    beside_t.start()

    def wait_split(flow):
        for q in range(SUBS):
            zs_copy(flow, z, q).wait_recv()

    ends(
        wait_split,
        lambda flows: add_rows(fin, [(xs.at[z], 0), (gs.at[c], s_at(me)), (ks.at[me], 0)] + [(zs.at[flow, z], 0) for flow in flows], srows))
    across_t.wait_recv()
    beside_far.start()
    squares = unalign(fin, g_split, splan.share, me * splan.share % BLOCK)
    beside_t.wait_recv()
    beside_far.wait_recv()
    add_rows(finc, [(cq, 0)], cplan.rows)
    squares += unalign(finc, g_common, cplan.share, me * cplan.share % BLOCK) * 0.25
    part[rank, 0:8, :] = squares
    part[rank, 8:16, :] = loss[...]
    shared = [remote(part.at[rank], part.at[rank], 97 + k, device) for k, device in enumerate(devices)]
    for copy in shared:
        copy.start()
    kd_copy().wait_send()
    yd_copy().wait_send()
    for i in range(8):
        ks_copy(i).wait_send()
        yc_copy(i).wait_send()
        for yy in range(2):
            kc_copy(i, yy).wait_send()
    for zz in range(4):
        xc_copy(zz).wait_send()
        for q in range(SUBS):
            xs_copy(zz, q).wait_send()
        for down in (0, 1):
            @pl.when(z > zz if down else z < zz)
            def _(down=down, zz=zz):
                zc_copy(down, zz).wait_send()
                for q in range(SUBS):
                    zs_copy(down, zz, q).wait_send()
    for copy in (across_t, beside_t, beside_far):
        copy.wait_send()
    for copy in shared:
        copy.wait_recv()

    def total(index, value):
        return value + part[index]

    sums[...] = lax.fori_loop(0, 32, total, jnp.zeros((16, LANES), F32))
    for copy in shared:
        copy.wait_send()


def pack_kernel(*refs):
    back, _, outs, (out_sem,) = back_refs(refs)
    t = lax.axis_index(TENSOR)
    barrier = pltpu.get_barrier_semaphore()
    for other in (t // 2 * 2 + 1 - t % 2, (1 - t // 2) * 2 + t % 2):
        pl.semaphore_signal(barrier, inc=1, device_id={DP: lax.axis_index(DP), TENSOR: other}, device_id_type=MESH)

    def nothing():
        pass

    back_and_pack(back, Namespace(
        first=lambda: pl.semaphore_wait(barrier, 2), early_away=nothing, early_own=nothing, late_away=nothing, late_own=nothing,
        common_early=nothing, common_late=nothing))
    copies = [pltpu.make_async_copy(a, b, out_sem.at[k]) for k, (a, b) in enumerate(zip(back[12:15], outs))]
    for copy in copies:
        copy.start()
    for copy in copies:
        copy.wait()


def unalign_kernel(share_s, share_c, scalars, s_in, c_in, s_out, c_out, sums):
    sums[...] = unalign(s_in, s_out, share_s, scalars[0]) + unalign(c_in, c_out, share_c, scalars[1]) * 0.25


def reduce_grads(grads, part, seen, norms, small, dbias, loss, w, saved, cplan, splan):
    any_spec, vmem = pl.BlockSpec(memory_space=pl.ANY), pl.BlockSpec(memory_space=pltpu.VMEM)
    srows, quarter = splan.rows, cplan.rows // 4
    gs_rows, gc_rows = buffer_rows(splan, S_WIDE), buffer_rows(cplan, C_WIDE)
    flat = (jax.ShapeDtypeStruct((flat_rows(splan.share), LANES), F32), jax.ShapeDtypeStruct((flat_rows(cplan.share), LANES), F32))
    operands = [vars(grads)[name] for name in LATE_NAMES] + [part, seen, norms, small, dbias, loss]
    operands += [vars(w)[name] for name in BACK_WEIGHTS] + [vars(saved)[name] for name in KEPT]
    in_specs = [any_spec] * len(LATE_NAMES) + [vmem] * 6 + [any_spec] * 5 + [vmem] * len(KEPT)
    scratch = back_scratch(gs_rows, gc_rows)
    params = pltpu.CompilerParams(collective_id=1, has_side_effects=True, vmem_limit_bytes=67_000_000)
    if cplan.parts == 8 and splan.parts == 8:
        def rows(*shape, kind=BF16):
            return pltpu.VMEM(shape + (LANES,), kind)

        return pl.pallas_call(
            functools.partial(reduce_kernel, cplan, splan),
            out_shape=flat + (jax.ShapeDtypeStruct((16, LANES), F32),), in_specs=in_specs, out_specs=[vmem] * 3,
            scratch_shapes=scratch + [
                rows(8, srows), rows(4, srows), rows(2, 4, srows), rows(8, 2, quarter), rows(8, quarter), rows(4, quarter), rows(2, 4, quarter),
                rows(D_WIDE), rows(D_WIDE), rows(cplan.rows), rows(32, 16, kind=F32), pltpu.SemaphoreType.DMA((128,)), pltpu.SemaphoreType.DMA((128,))],
            compiler_params=params, name="reduce",
        )(*operands)
    shapes = [jax.ShapeDtypeStruct((2, gs_rows, LANES), BF16), jax.ShapeDtypeStruct((2, D_WIDE, LANES), BF16), jax.ShapeDtypeStruct((gc_rows, LANES), BF16)]
    gs, gd, gc = pl.pallas_call(
        pack_kernel, out_shape=shapes, in_specs=in_specs, out_specs=[any_spec] * 3,
        scratch_shapes=scratch + [pltpu.SemaphoreType.DMA((3,))], compiler_params=params, name="pack",
    )(*operands)
    me, t = lax.axis_index(DP), lax.axis_index(TENSOR)
    c = t % 2

    def swap(value, bit):
        return lax.ppermute(value, TENSOR, [(i, i ^ bit) for i in range(4)])

    def mine(value):
        keep = lax.dynamic_index_in_dim(value, c, 0, False).astype(F32)
        return keep + swap(lax.dynamic_index_in_dim(value, 1 - c, 0, False), 1).astype(F32)

    far = swap(mine(gd).astype(BF16), 2)
    split_sum = mine(gs).at[DEC_FIRST : DEC_FIRST + D_WIDE].add(far.astype(F32))
    common_sum = lax.psum(gc, TENSOR).astype(F32)

    def scattered(value, plan):
        frames = jnp.stack([value[base : base + plan.rows] for base in plan.base])
        return lax.psum_scatter(frames.astype(BF16), DP, scatter_dimension=0, tiled=True)[0].astype(F32)

    s_frame, c_frame = scattered(split_sum, splan), scattered(common_sum, cplan)
    pad = ((0, 64), (0, 0))
    g_split, g_common, squares = pl.pallas_call(
        functools.partial(unalign_kernel, splan.share, cplan.share), out_shape=flat + (jax.ShapeDtypeStruct((8, LANES), F32),),
        in_specs=[pl.BlockSpec(memory_space=pltpu.SMEM), vmem, vmem], out_specs=[vmem] * 3, name="unalign",
    )(jnp.stack([me * splan.share % BLOCK, me * cplan.share % BLOCK]).astype(jnp.int32), jnp.pad(s_frame, pad), jnp.pad(c_frame, pad))
    return g_split, g_common, lax.psum(jnp.concatenate([squares, loss]), (DP, TENSOR))


OWN = TUBES // 2
KEYS = 392


def head_masks(rows):
    lane = lax.broadcasted_iota(jnp.int32, (rows, LANES), 1)
    return lane < HEAD, lane >= HEAD


def attend_kernel(q_ref, k_ref, v_ref, o_ref, lse_ref, vt_ref, shifted_ref):
    q = q_ref[...]
    vt_ref[...] = v_ref[...].T
    pieces = []
    for head, mask in enumerate(head_masks(OWN)):
        qm = jnp.where(mask, q * SCALE, jnp.zeros_like(q))
        top = None
        for first in range(0, TUBES, KEYS):
            most = jnp.max(nt(k_ref[first : first + KEYS, :], qm), axis=0, keepdims=True)
            top = most if top is None else jnp.maximum(top, most)
        total = None
        qm = jnp.where(mask, q, jnp.zeros_like(q))
        for first in range(0, TUBES, KEYS):
            shifted = jnp.exp(nt(k_ref[first : first + KEYS, :], qm) * SCALE - top)
            part = jnp.sum(shifted, axis=0, keepdims=True)
            total = part if total is None else total + part
            shifted_ref[first : first + KEYS, :] = shifted.astype(BF16)
        pieces.append(nn(vt_ref[head * HEAD : (head + 1) * HEAD, :], shifted_ref[...]) / total)
        lse_ref[0, head : head + 1, :] = top + jnp.log(total)
    o_ref[...] = jnp.concatenate(pieces, axis=0).T


def attend(q, k, v):
    block, whole = pl.BlockSpec((OWN, LANES), lambda h: (0, h)), pl.BlockSpec((TUBES, LANES), lambda h: (0, h))
    return pl.pallas_call(
        attend_kernel, grid=(3,),
        out_shape=(jax.ShapeDtypeStruct((OWN, DD), F32), jax.ShapeDtypeStruct((3, 8, OWN), F32)),
        in_specs=[block, whole, whole], out_specs=[block, pl.BlockSpec((1, 8, OWN), lambda h: (h, 0, 0))],
        scratch_shapes=[pltpu.VMEM((LANES, TUBES), BF16), pltpu.VMEM((TUBES, OWN), BF16)], name="attend",
    )(q, k, v)


def attend_back_kernel(q_ref, k_ref, v_ref, do_ref, o_ref, lse_ref, dq_ref, dk_ref, dv_ref, kt_ref, ds_ref):
    q, do = q_ref[...], do_ref[...]
    kt_ref[...] = k_ref[...].T
    along = (do.astype(F32) * o_ref[...]).T
    pieces = []
    for head, mask in enumerate(head_masks(OWN)):
        qm, dom = jnp.where(mask, q * SCALE, jnp.zeros_like(q)), jnp.where(mask, do, jnp.zeros_like(do))
        delta = jnp.sum(along[head * HEAD : (head + 1) * HEAD], axis=0, keepdims=True)
        lse = lse_ref[0, head : head + 1, :]
        for first in range(0, TUBES, KEYS):
            rows = slice(first, first + KEYS)
            probs = jnp.exp(nt(k_ref[rows, :], qm) - lse)
            dv = nn(probs.astype(BF16), dom)
            ds = (probs * (nt(v_ref[rows, :], dom) - delta)).astype(BF16)
            ds_ref[rows, :] = ds
            dk = nn(ds, qm)
            if head:
                dk_ref[rows, :] += dk
                dv_ref[rows, :] += dv
            else:
                dk_ref[rows, :] = dk
                dv_ref[rows, :] = dv
        pieces.append(nn(kt_ref[head * HEAD : (head + 1) * HEAD, :], ds_ref[...]))
    dq_ref[...] = (jnp.concatenate(pieces, axis=0) * SCALE).T.astype(BF16)


def attend_back(q, k, v, do, o, lse):
    block, whole = pl.BlockSpec((OWN, LANES), lambda h: (0, h)), pl.BlockSpec((TUBES, LANES), lambda h: (0, h))
    return pl.pallas_call(
        attend_back_kernel, grid=(3,),
        out_shape=(jax.ShapeDtypeStruct((OWN, DD), BF16), jax.ShapeDtypeStruct((TUBES, DD), F32), jax.ShapeDtypeStruct((TUBES, DD), F32)),
        in_specs=[block, whole, whole, block, block, pl.BlockSpec((1, 8, OWN), lambda h: (h, 0, 0))], out_specs=[block, whole, whole],
        scratch_shapes=[pltpu.VMEM((LANES, TUBES), BF16), pltpu.VMEM((TUBES, OWN), BF16)], name="attend_back",
    )(q, k, v, do, o, lse)


NORM_EPS = 1e-06
PIXEL_EPS = 1e-06
CLIP_RATIO = 1.5
BETA_FIRST = 0.9
BETA_SECOND = 0.95
LEARN_RATE = 0.05
DECAY_RATE = 0.05
ADAM_EPS = 1e-08


def layer_norm(inputs, gain, shift):
    centered = inputs - jnp.mean(inputs, axis=-1, keepdims=True)
    spread = jnp.mean(centered * centered, axis=-1, keepdims=True)
    return centered * lax.rsqrt(spread + NORM_EPS) * gain + shift


def norm_back(inputs, gain, grad):
    centered = inputs - jnp.mean(inputs, axis=-1, keepdims=True)
    scale = lax.rsqrt(jnp.mean(centered * centered, axis=-1, keepdims=True) + NORM_EPS)
    unit = centered * scale
    inner = grad * gain
    back = scale * (inner - jnp.mean(inner, axis=-1, keepdims=True) - unit * jnp.mean(inner * unit, axis=-1, keepdims=True))
    return back, jnp.sum(grad * unit, axis=0), jnp.sum(grad, axis=0)


def gelu(inputs):
    return jax.nn.gelu(inputs, approximate=False)


def gelu_slope(inputs):
    return 0.5 * (1.0 + lax.erf(inputs * math.sqrt(0.5))) + inputs * jnp.exp(-0.5 * inputs * inputs) * (1.0 / math.sqrt(2.0 * math.pi))


def sine_table(width, step=32):
    first, second, third, fourth = sines(width, step)
    table = first[:, None] * jnp.asarray(third)[None] + second[:, None] * jnp.asarray(fourth)[None]
    return table.reshape(TUBES, width)


def beside(value):
    return lax.ppermute(value, TENSOR, [(i, i ^ 1) for i in range(4)])


def step_grads(pixels, order, w, saved, scale_back):
    t = lax.axis_index(TENSOR)
    y, c = t // 2, t % 2
    seen_y = jnp.pad(lax.dynamic_index_in_dim(order, y, 0, False)[:VIS], (0, VP - VIS), constant_values=-1)
    rows = pixels.reshape(2 * TUBES, PATCH)
    lowered = saved.lowered
    select = seen_y[None, :] == jnp.arange(TUBES, dtype=jnp.int32)[:, None]
    visible = jnp.any(select, axis=1, keepdims=True)
    placed = lax.dot_general(select.astype(F32), lowered, (((1,), (0,)), ((), ())), precision=lax.Precision.HIGHEST, preferred_element_type=F32)
    dec_in = placed + jnp.where(visible, 0.0, w.mask_token) + sine_table(DD)
    start = c * OWN

    def own(value):
        return lax.dynamic_slice_in_dim(value, start, OWN, 0)

    dnorms, dbiases = w.dec_norms, w.dec_biases
    normed_all = layer_norm(dec_in, dnorms[0], dnorms[1]).astype(BF16)
    normed_q = own(normed_all)
    dec_own = own(dec_in)
    query = (nn(normed_q, w.dec_qkv[:, :DD]) + w.dec_qkv_bias[0]).astype(BF16)
    key = nn(normed_all, w.dec_qkv[:, DD : 2 * DD]).astype(BF16)
    value = (nn(normed_all, w.dec_qkv[:, 2 * DD :]) + w.dec_qkv_bias[1]).astype(BF16)
    attended, lse = attend(query, key, value)
    attended_low = attended.astype(BF16)
    mid = dec_own + (nn(attended_low, w.dec_proj) + dbiases[0])
    normed_d = layer_norm(mid, dnorms[2], dnorms[3]).astype(BF16)
    draised = nn(normed_d, w.dec_up) + w.dec_up_bias
    dactive = gelu(draised).astype(BF16)
    decoded = mid + (nn(dactive, w.dec_down) + dbiases[1])
    head_low = layer_norm(decoded, dnorms[4], dnorms[5]).astype(BF16)
    predicted = nn(head_low, w.pixel_head) + w.head_bias
    target = lax.dynamic_slice_in_dim(rows, y * TUBES + start, OWN, 0).astype(F32)
    target = target - jnp.mean(target, axis=-1, keepdims=True)
    target = target * lax.rsqrt(jnp.mean(target * target, axis=-1, keepdims=True) + PIXEL_EPS)
    hidden = 1.0 - own(visible.astype(F32))
    missing = (predicted - target) * hidden
    loss = jnp.sum((missing * missing).reshape(-1, 8, PATCH // LANES, LANES), axis=(0, 2))
    pred_grad = (2.0 * scale_back * missing).astype(BF16)
    grads, small = Namespace(), Namespace()
    grads.pixel_head = tn(head_low, pred_grad)
    small.head_bias = jnp.sum(pred_grad, axis=0, dtype=F32)
    decoded_grad, dg4, dg5 = norm_back(decoded, dnorms[4], nt(pred_grad, w.pixel_head))
    branch = decoded_grad.astype(BF16)
    grads.dec_down = tn(dactive, branch)
    db1 = jnp.sum(branch, axis=0, dtype=F32)
    draised_grad = (nt(branch, w.dec_down) * gelu_slope(draised)).astype(BF16)
    grads.dec_up = tn(normed_d, draised_grad)
    dec_up_bias = jnp.sum(draised_grad, axis=0, dtype=F32)
    back, dg2, dg3 = norm_back(mid, dnorms[2], nt(draised_grad, w.dec_up))
    mid_grad = decoded_grad + back
    branch = mid_grad.astype(BF16)
    grads.dec_proj = tn(attended_low, branch)
    db0 = jnp.sum(branch, axis=0, dtype=F32)
    attended_grad = nt(branch, w.dec_proj).astype(BF16)
    query_grad, key_grad, value_grad = attend_back(query, key, value, attended_grad, attended, lse)

    def shared(total):
        keep = lax.dynamic_slice_in_dim(total, start, OWN, 0)
        give = lax.dynamic_slice_in_dim(total, OWN - start, OWN, 0).astype(BF16)
        return (keep + beside(give).astype(F32)).astype(BF16)

    mixed = jnp.concatenate([query_grad, shared(key_grad), shared(value_grad)], axis=1)
    grads.dec_qkv = tn(normed_q, mixed)
    dqb = jnp.sum(mixed, axis=0, dtype=F32)
    small.dec_qkv_bias = jnp.concatenate([dqb[:DD], dqb[2 * DD :]])
    back, dg0, dg1 = norm_back(dec_own, dnorms[0], nt(mixed, w.dec_qkv))
    in_grad = mid_grad + back
    small.mask_token = jnp.sum(in_grad * hidden, axis=0)
    part = tn(own(select).astype(BF16), in_grad.astype(BF16)).astype(BF16)
    small_b = jnp.concatenate([small.mask_token, dg0, dg1, dg2, dg3, dg4, dg5, db0, db1])
    tiles = []
    for piece in (small_b, small.dec_qkv_bias, small.head_bias):
        count = piece.shape[0] // LANES
        tiles.append(jnp.pad(piece.reshape(count, LANES), ((0, -count % 8), (0, 0))))
    dbias = jnp.pad(dec_up_bias.reshape(4, 3, LANES), ((0, 0), (0, 5), (0, 0)))
    return loss, grads, part, jnp.concatenate(tiles), dbias


def adamw(master, first, second, gradient):
    first_new = BETA_FIRST * first + (1.0 - BETA_FIRST) * gradient
    second_new = BETA_SECOND * second + (1.0 - BETA_SECOND) * gradient * gradient
    first_hat = first_new / (1.0 - BETA_FIRST**STEP)
    second_hat = second_new / (1.0 - BETA_SECOND**STEP)
    master_new = master - LEARN_RATE * (first_hat / (jnp.sqrt(second_hat) + ADAM_EPS) + DECAY_RATE * master)
    return (master_new, first_new, second_new, master_new.astype(BF16))


def shards(tubes, tube_order, common_master, common_first, common_second, split_master, split_first, split_second):
    groups = lax.axis_size(DP)
    cplan = Plan(groups, common_master.shape[0], 64)
    splan = Plan(groups, split_master.shape[1], TILE)
    masked_total = tubes.shape[0] * groups * (TUBES - VIS)
    pixel_count = masked_total * PATCH
    w, saved = gather_weights(common_master, split_master, tube_order, tubes, cplan, splan)
    loss, grads, part, small, dbias = step_grads(tubes, tube_order, w, saved, 1.0 / pixel_count)
    half = lax.dynamic_slice_in_dim(saved.seen, lax.axis_index(TENSOR) // 2 * 768, 768, 1)
    g_split, g_common, sums = reduce_grads(grads, part, half, w.enc_norms.reshape(36, LANES), small, dbias, loss, w, saved, cplan, splan)
    loss_mean = jnp.sum(sums[8:]) / pixel_count
    grad_norm = jnp.sqrt(jnp.sum(sums[:8]))
    factor = jnp.minimum(1.0, CLIP_RATIO / math.sqrt(masked_total) / (grad_norm + 1e-06))
    common = adamw(common_master, common_first, common_second, g_common.reshape(-1)[: common_master.shape[0]] * factor)
    split = adamw(split_master, split_first, split_second, g_split.reshape(1, -1)[:, : split_master.shape[1]] * factor)
    return (loss_mean.reshape(1), grad_norm.reshape(1)) + common + split


def solution(mesh):
    in_specs = (P(DP, None, None), P(DP, None), P(DP), P(DP), P(DP), P(TENSOR, DP), P(TENSOR, DP), P(TENSOR, DP))
    out_specs = (P(), P()) + (P(DP),) * 4 + (P(TENSOR, DP),) * 4
    return jax.shard_map(shards, mesh=mesh, in_specs=in_specs, out_specs=out_specs, check_vma=False)
```
